32 devices in a mesh: gx: 4 (over y, x), gy: 4 (over z), gz: 2 (over core).
Axes of the slice: x: 2, y: 2, z: 4, core: 2. Of those that a mesh axis runs over, the one named last changes fastest.
Arguments:
- displacement: float32 [4, 4, 9216], P('gx', 'gy', 'gz'), may hold values from -0.1 to 0.1
- species: int32 [4, 4, 3072], P('gx', 'gy', 'gz'), may hold values from 0 to 1
- centres: int32 [4, 4, 32], P('gx', 'gy', 'gz'), may hold values from 0 to 1535, as said below
- neighbours: int32 [4, 4, 1024], P('gx', 'gy', 'gz'), may hold values from 0 to 5183, as said below
- neighbour_count: int32 [4, 4, 32], P('gx', 'gy', 'gz'), may hold values from 1 to 32, as said below
- live_centres: int32 [4, 4, 2], P('gx', 'gy', 'gz'), may hold values from 8 to 16, as said below
- w_two: float32 [12, 64], replicated, may hold values from -1.75 to 1.75
- w_lat: float32 [64, 64], replicated, may hold values from -0.75 to 0.75
- w_env: float32 [64, 64], replicated, may hold values from -0.75 to 0.75
- w_out: float32 [256, 64], replicated, may hold values from -0.375 to 0.375
- readout: float32 [64], replicated, may hold values from -0.75 to 0.75
Outputs:
- centre_energy: float32 [4, 4, 32], P('gx', 'gy', 'gz')
- forces: float32 [4, 4, 9216], P('gx', 'gy', 'gz')
The draws below stay inside these ranges and needn't reach their ends.
Inputs may be any that keep to these rules, and one draw needn't show every extreme that they name: `centres`: local atom index of an owned atom; entries may repeat. `neighbours`: extended index of an atom whose cell lies within two cells of the centre's cell in each dimension, with squared cell distance at most 4; never the centre itself. `neighbour_count`: in every domain some centre has all 32 slots live. `live_centres`: some domain has all 16 centres live; the live centres are the first ones.
All inputs are finite; a program needn't handle non-finite values.
Results may differ from the reference program's by a relative error of at most 0.0003.
Values sent between devices are 32-bit elements; how exact they have to be, the bound alone decides.
A program may use at most 64 MiB of HBM per device.

```python
import math
import jax
import jax.numpy as jnp
import numpy as np
from jax import lax

CELLS = 8
CENTRES = 16
NEIGH = 32
LATENT = 64
NBASIS = 8
SPECIES = 2
NX = 32
NY = 32
NZ = 16
N_GX = 4
N_GY = 4
N_GZ = 2


offset_rows = np.array([[0, 0, 0]] + [[a, b, c] for a in range(-2, 3) for b in range(-2, 3) for c in range(-2, 3) if 0 < a * a + b * b + c * c <= 4], np.int32)


def pair_lists(key):
    grid_x = NX // CELLS
    grid_y = NY // CELLS
    grid_z = NZ // CELLS
    extent = CELLS + 4
    base = jax.random.fold_in(key, 7)
    key_centre, key_offset, key_atom = jax.random.split(base, 3)
    centre = jax.random.randint(key_centre, (grid_x, grid_y, grid_z, CENTRES), 0, 3 * CELLS ** 3)
    atom_first = centre % 3
    cell_first = centre // 3
    loc_z = cell_first % CELLS
    loc_y = cell_first // CELLS % CELLS
    loc_x = cell_first // (CELLS * CELLS)
    choice_offset = jax.random.randint(key_offset, (grid_x, grid_y, grid_z, CENTRES, NEIGH), 0, offset_rows.shape[0])
    table = jnp.array(offset_rows)
    offsets = table[choice_offset]
    atom_second = jax.random.randint(key_atom, (grid_x, grid_y, grid_z, CENTRES, NEIGH), 0, 3)
    clash = (choice_offset == 0) & (atom_second == atom_first[..., None])
    atom_second = jnp.where(clash, (atom_first[..., None] + 1) % 3, atom_second)
    ext_x = loc_x[..., None] + 2 + offsets[..., 0]
    ext_y = loc_y[..., None] + 2 + offsets[..., 1]
    ext_z = loc_z[..., None] + 2 + offsets[..., 2]
    second = ((ext_x * extent + ext_y) * extent + ext_z) * 3 + atom_second
    return (centre.reshape(grid_x, grid_y, grid_z * CENTRES), second.reshape(grid_x, grid_y, grid_z * CENTRES * NEIGH))


def draw_centres(key, part):
    return pair_lists(key)[0].astype(jnp.int32)


def draw_neighbours(key, part):
    return pair_lists(key)[1].astype(jnp.int32)


def draw_neighbour_count(key, part):
    grid_x = NX // CELLS
    grid_y = NY // CELLS
    grid_z = NZ // CELLS
    key_level, key_count, key_pick = jax.random.split(jax.random.fold_in(key, 11), 3)
    level = jax.random.randint(key_level, (grid_x, grid_y, grid_z), 1, 5)
    ceiling = jnp.maximum(NEIGH * level // 4, 1)
    floor_count = jnp.maximum(ceiling // 2, 1)
    counts = jax.random.randint(key_count, (grid_x, grid_y, grid_z, CENTRES), floor_count[..., None], ceiling[..., None] + 1)
    pick = jax.random.randint(key_pick, (grid_x, grid_y, grid_z, 1), 0, CENTRES)
    ranks = jnp.arange(CENTRES, dtype=jnp.int32)
    counts = jnp.where(ranks == pick, NEIGH, counts)
    return counts.reshape(grid_x, grid_y, grid_z * CENTRES).astype(jnp.int32)


def draw_live_centres(key, part):
    grid_x = NX // CELLS
    grid_y = NY // CELLS
    grid_z = NZ // CELLS
    key_live, key_pick = jax.random.split(jax.random.fold_in(key, 13), 2)
    total = grid_x * grid_y * grid_z
    live = jax.random.randint(key_live, (total,), CENTRES // 2, CENTRES + 1)
    pick = jax.random.randint(key_pick, (), 0, total)
    live = jnp.where(jnp.arange(total, dtype=jnp.int32) == pick, CENTRES, live)
    return live.reshape(grid_x, grid_y, grid_z).astype(jnp.int32)


def set_ends(values, own_key, smallest, largest):
    spot = [jax.random.randint(jax.random.fold_in(own_key, axis), (), 0, length) for axis, length in enumerate(values.shape)]
    widest = values.shape.index(max(values.shape))
    neighbour = spot[:widest] + [(spot[widest] + 1) % values.shape[widest]] + spot[widest + 1:]
    return values.at[tuple(spot)].set(smallest).at[tuple(neighbour)].set(largest)


def shard_levels(key, shape, cuts, low, top_value):
    loudness, own = 1.0, jax.random.fold_in(key, 6)
    for axis_at, parts in cuts:
        draws = jnp.exp(jax.random.uniform(jax.random.fold_in(own, axis_at), (parts,), jnp.float32, low / len(cuts), top_value / len(cuts)))
        loudness = loudness * jnp.repeat(draws, shape[axis_at] // parts).reshape([-1 if axis == axis_at else 1 for axis in range(len(shape))])
    return loudness


def normal_values(stream_key, shape, spread, reach, kind=jnp.bfloat16):
    result = jax.random.normal(stream_key, shape, jnp.float32) * spread
    return jnp.minimum(jnp.maximum(result, -reach), reach).astype(kind)


def setup_inputs(seed: int = 0) -> dict:
    seeds = jax.random.split(jax.random.key(seed), 12)
    return {
        "displacement": jnp.clip(jax.random.uniform(seeds[0], (N_GX, N_GY, N_GZ * CELLS**3 * 9), jnp.float32, -0.1, 0.1) * shard_levels(seeds[0], (N_GX, N_GY, N_GZ * CELLS**3 * 9), ((0, 4), (1, 4), (2, 2)), -0.4, 0.0), -0.1, 0.1),
        "species": set_ends(jax.random.randint(seeds[1], (N_GX, N_GY, N_GZ * CELLS**3 * 3), 0, SPECIES), jax.random.fold_in(seeds[1], 1), 0, SPECIES - 1).astype(jnp.int32),
        "centres": draw_centres(jax.random.fold_in(seeds[11], 71), 0),
        "neighbours": draw_neighbours(jax.random.fold_in(seeds[11], 71), 0),
        "neighbour_count": draw_neighbour_count(jax.random.fold_in(seeds[11], 71), 0),
        "live_centres": draw_live_centres(jax.random.fold_in(seeds[11], 71), 0),
        "w_two": normal_values(seeds[6], (2 * SPECIES + NBASIS, LATENT), (2 * SPECIES + NBASIS) ** -0.5, 1.75, jnp.float32),
        "w_lat": normal_values(seeds[7], (LATENT, LATENT), LATENT ** -0.5, 0.75, jnp.float32),
        "w_env": normal_values(seeds[8], (LATENT, LATENT), LATENT ** -0.5, 0.75, jnp.float32),
        "w_out": normal_values(seeds[9], (4 * LATENT, LATENT), (4 * LATENT) ** -0.5, 0.375, jnp.float32),
        "readout": normal_values(seeds[10], (LATENT,), LATENT ** -0.5, 0.75, jnp.float32),
    }


cutoff = 6.0
cell_side = 3.1
env_scale = 0.2
site_rows = np.array([[0.25, 0.25, 0.25], [0.75, 0.75, 0.25], [0.25, 0.75, 0.75]], np.float32)

def mixing(weight, data):
    return jnp.dot(weight.T, data, precision=lax.Precision.HIGHEST, preferred_element_type=jnp.float32)

def harmonics(unit):
    ux, uy, uz = (unit[0], unit[1], unit[2])
    root3 = math.sqrt(3.0)
    root5 = math.sqrt(5.0)
    root15 = math.sqrt(15.0)
    return jnp.stack([jnp.ones_like(ux), root3 * ux, root3 * uy, root3 * uz, root15 * ux * uy, root15 * uy * uz, 0.5 * root5 * (3.0 * uz * uz - 1.0), root15 * ux * uz, 0.5 * root15 * (ux * ux - uy * uy)], 0)

def block_energy(rvec, kind_first, kind_second, live, w_two, w_lat, w_env, w_out, readout, slots):
    dist = jnp.sqrt(lax.optimization_barrier(jnp.sum(rvec * rvec, axis=0)))
    unit = rvec / dist
    ratio = dist / cutoff
    envelope = jnp.where(ratio < 1.0, 1.0 - 28.0 * ratio ** 6 + 48.0 * ratio ** 7 - 21.0 * ratio ** 8, 0.0)
    orders = jnp.arange(1, NBASIS + 1, dtype=jnp.float32)[:, None]
    basis = math.sqrt(2.0 / cutoff) * jnp.sin(orders * math.pi * dist[None, :] / cutoff) / dist[None, :] * envelope[None, :]
    kinds = jnp.arange(SPECIES, dtype=jnp.float32)[:, None]
    first_hot = (kind_first[None, :] == kinds).astype(jnp.float32)
    second_hot = (kind_second[None, :] == kinds).astype(jnp.float32)
    inputs = jnp.concatenate([first_hot, second_hot, basis], 0)
    hidden = jax.nn.silu(mixing(w_two, inputs))
    latent = jax.nn.silu(mixing(w_lat, hidden))
    weights = mixing(w_env, latent) * (envelope * live)[None, :]
    harm = harmonics(unit)
    width = latent.shape[0]
    centre_total = rvec.shape[1] // slots
    edge = (harm[:, None, :] * weights[None, :, :]).reshape(9, width, centre_total, slots)
    environ = env_scale * lax.optimization_barrier(jnp.sum(edge, axis=3))
    product = edge * environ[:, :, :, None]
    scalars = jnp.stack([product[0], lax.optimization_barrier(jnp.sum(product[1:4], axis=0)), lax.optimization_barrier(jnp.sum(product[4:9], axis=0))], 0)
    joined = jnp.concatenate([latent, scalars.reshape(3 * width, centre_total * slots)], 0)
    updated = jax.nn.silu(mixing(w_out, joined))
    pair_energy = jnp.dot(readout, updated, precision=lax.Precision.HIGHEST) * envelope * live
    return lax.optimization_barrier(jnp.sum(pair_energy.reshape(centre_total, slots), axis=1))

def to_grid(blocks, width):
    cube = blocks.reshape(N_GX, N_GY, N_GZ, CELLS, CELLS, CELLS, width)
    return jnp.transpose(cube, (0, 3, 1, 4, 2, 5, 6)).reshape(NX, NY, NZ, width)

def reference(displacement, species, centres, neighbours, neighbour_count, live_centres, w_two, w_lat, w_env, w_out, readout):
    side = CELLS
    extent = CELLS + 4
    domains = N_GX * N_GY * N_GZ
    shifts = to_grid(displacement, 9).reshape(NX, NY, NZ, 3, 3)
    kinds = to_grid(species, 3).astype(jnp.float32)
    centre_rows = centres.reshape(domains, CENTRES)
    neighbour_rows = neighbours.reshape(domains, CENTRES * NEIGH)
    count_rows = neighbour_count.reshape(domains, CENTRES)
    alive = live_centres.reshape(domains)
    sites = jnp.array(site_rows, dtype=jnp.float32)
    slot_ids = jnp.arange(NEIGH, dtype=jnp.int32)
    centre_ids = jnp.arange(CENTRES, dtype=jnp.int32)

    def one_domain(forces, index):
        dom_x = index // (N_GY * N_GZ)
        dom_y = index // N_GZ % N_GY
        dom_z = index % N_GZ
        first = jnp.repeat(centre_rows[index], NEIGH)
        atom_first = first % 3
        cell_first = first // 3
        loc_z = cell_first % side
        loc_y = cell_first // side % side
        loc_x = cell_first // (side * side)
        glob_xi = dom_x * side + loc_x
        glob_yi = dom_y * side + loc_y
        glob_zi = dom_z * side + loc_z
        second = neighbour_rows[index]
        atom_second = second % 3
        cell_second = second // 3
        ext_z = cell_second % extent - 2
        ext_y = cell_second // extent % extent - 2
        ext_x = cell_second // (extent * extent) - 2
        glob_xj = (dom_x * side + ext_x) % NX
        glob_yj = (dom_y * side + ext_y) % NY
        glob_zj = (dom_z * side + ext_z) % NZ
        place_first = jnp.stack([loc_x, loc_y, loc_z], 0).astype(jnp.float32) + sites[atom_first].T + shifts[glob_xi, glob_yi, glob_zi, atom_first].T
        place_second = jnp.stack([ext_x, ext_y, ext_z], 0).astype(jnp.float32) + sites[atom_second].T + shifts[glob_xj, glob_yj, glob_zj, atom_second].T
        rvec = (place_second - place_first) * cell_side
        kind_first = kinds[glob_xi, glob_yi, glob_zi, atom_first]
        kind_second = kinds[glob_xj, glob_yj, glob_zj, atom_second]
        live = ((slot_ids[None, :] < count_rows[index][:, None]) & (centre_ids[:, None] < alive[index])).reshape(-1).astype(jnp.float32)

        def energy_of(vectors):
            return block_energy(vectors, kind_first, kind_second, live, w_two, w_lat, w_env, w_out, readout, NEIGH)
        energy, pullback = jax.vjp(energy_of, rvec)
        grad = pullback(jnp.ones_like(energy))[0]
        index_first = ((glob_xi * NY + glob_yi) * NZ + glob_zi) * 3 + atom_first
        index_second = ((glob_xj * NY + glob_yj) * NZ + glob_zj) * 3 + atom_second
        forces = forces.at[index_second].add(-grad.T)
        forces = forces.at[index_first].add(grad.T)
        return (forces, energy)
    start = jnp.zeros((NX * NY * NZ * 3, 3), jnp.float32)
    forces, energies = lax.scan(one_domain, start, jnp.arange(domains, dtype=jnp.int32))
    grid = forces.reshape(N_GX, CELLS, N_GY, CELLS, N_GZ, CELLS, 9)
    blocks = jnp.transpose(grid, (0, 2, 4, 1, 3, 5, 6)).reshape(N_GX, N_GY, N_GZ * CELLS * CELLS * CELLS * 9)
    return (energies.reshape(N_GX, N_GY, N_GZ * CENTRES), blocks)
```

```python
import math

import jax
import jax.numpy as jnp
from jax import lax
from jax.experimental import pallas as pl
from jax.experimental.pallas import tpu as pltpu
from jax.sharding import PartitionSpec as P

CELLS = 8
NBASIS = 8
CUTOFF = 6.0
SIDE = 3.1
ENV = 0.2
LANES = 128
ZROWS = CELLS * 9
KINDS = CELLS * 3
KEPT = 18
KIND_AT = ZROWS + KEPT
HALF = CELLS * CELLS // 2
AXES = ("gx", "gy", "gz")

NN = (((1,), (0,)), ((), ()))
NT = (((1,), (1,)), ((), ()))


def halves(x):
    hi = x.astype(jnp.bfloat16)
    lo = (x - hi.astype(jnp.float32)).astype(jnp.bfloat16)
    return hi, lo


def raw(a, b, dims):
    return lax.dot_general(a, b, dims, preferred_element_type=jnp.float32)


def mm(a, b, dims=NN):
    ah, al = a if isinstance(a, tuple) else halves(a)
    bh, bl = b if isinstance(b, tuple) else halves(b)
    if dims is NT:
        m, n = ah.shape[0], bh.shape[0]
        both = raw(jnp.concatenate([ah, al], axis=0), jnp.concatenate([bh, bl], axis=0), NT)
        return both[:m, :n] + (both[:m, n:] + both[m:, :n])
    if ah.shape[1] > 2 * LANES - 1:
        return raw(ah, bh, dims) + (raw(ah, bl, dims) + raw(al, bh, dims))
    return raw(
        jnp.concatenate([ah, ah, al], axis=1), jnp.concatenate([bh, bl, bh], axis=0), NN
    )


def mm_exact_b(a, b, dims=NN):
    ah, al = halves(a)
    return raw(ah, b, dims) + raw(al, b, dims)


def mm_exact_a(a, b):
    n = b.shape[0]
    both = raw(a, jnp.concatenate(halves(b), axis=0), NT)
    return both[:, :n] + both[:, n:]


def slot_plan(depth):
    sides = [1] if depth == 2 else [1, -1]
    ends = (-1, 1)
    groups = [
        [((0, 0, dz), HALF) for dz in sides],
        [((dx, 0, 0), 2 * CELLS) for dx in ends],
        [((0, dy, 0), 2 * CELLS) for dy in ends],
        [((dx, 0, dz), CELLS) for dz in sides for dx in ends],
        [((0, dy, dz), CELLS // 2) for dz in sides for dy in ends],
        [((dx, dy, 0), 1) for dx in ends for dy in ends],
        [((dx, dy, dz), 1) for dz in sides for dx in ends for dy in ends],
    ]
    plan, at = [], 0
    for step, rows in [entry for group in groups for entry in group]:
        plan.append((step, at, rows))
        at += rows
    return plan, at


def origin(step, tiles):
    return 0 if step >= 0 else CELLS - tiles


def own_corner(step):
    return step[2] == 0 and step[0] != 0 and step[1] != 0


def wave(turns):
    f = turns - jnp.floor(turns + 0.5)
    f = jnp.where(f > 0.25, 0.5 - f, jnp.where(f < -0.25, -0.5 - f, f))
    x = f * (2.0 * math.pi)
    s = x * x
    p = -1.0 / 39916800.0
    for c in (1.0 / 362880.0, -1.0 / 5040.0, 1.0 / 120.0, -1.0 / 6.0):
        p = p * s + c
    return x + x * s * p


def divided(value, by):
    return jnp.floor((value + 0.5) * (1.0 / by))


def silu_pair(x):
    s = 1.0 / (1.0 + jnp.exp(-x))
    return x * s, s * (1.0 + x * (1.0 - s))


def kernel_body(sizes, plan, disp_hbm, spec_hbm, cen_hbm, nbr_hbm, cnt_hbm, alive_hbm, two_hbm,
                lat_hbm, env_hbm, out_hbm, readout_hbm, result,
                disp, spec, cen, nbr, cnt, alive, w_two, w_lat, w_env, w_out_t, readout,
                table, pack, ztable, zpack, mail, inbox, back_mail, back_inbox, halo, part, got,
                send_a, recv_a, send_b, recv_b, load):
    loads = [
        pltpu.make_async_copy(src, dst, load.at[at])
        for at, (src, dst) in enumerate(
            (
                (disp_hbm, disp),
                (spec_hbm, spec),
                (cen_hbm, cen),
                (nbr_hbm, nbr),
                (cnt_hbm, cnt),
                (alive_hbm, alive),
                (two_hbm, w_two),
                (lat_hbm, w_lat),
                (env_hbm, w_env),
                (out_hbm, w_out_t),
                (readout_hbm, readout),
            )
        )
    ]
    for copy in loads:
        copy.start()
    disp, spec, cen, nbr, cnt, alive = (
        ref.at[0] for ref in (disp, spec, cen, nbr, cnt, alive)
    )
    total = result.at[pl.ds(0, CELLS * CELLS)]
    me = tuple(lax.axis_index(a) for a in AXES)
    odd = [lax.rem(i, 2) for i in me[:2]]
    swapped = tuple(i + 1 - 2 * o for i, o in zip(me, odd)) + me[2:]

    def moved(place, step, sign):
        return tuple(
            lax.rem(i + (sign * d + n), n) if d else i for i, d, n in zip(place, step, sizes)
        )

    def holder(step):
        return moved(swapped, step, 1)

    def worker(step):
        x, y, z = moved(me, step, -1)
        return x + 1 - 2 * lax.rem(x, 2), y + 1 - 2 * lax.rem(y, 2), z

    def mine_too(step):
        return (odd[0] == (1 if step[0] > 0 else 0)) & (odd[1] == (1 if step[1] > 0 else 0))

    barrier = pltpu.get_barrier_semaphore()

    def greet(device):
        pl.semaphore_signal(
            barrier, inc=1, device_id=device, device_id_type=pl.DeviceIdType.MESH
        )

    def unless_mine(step, action):
        if own_corner(step):
            pl.when(jnp.logical_not(mine_too(step)))(action)
        else:
            action()

    for step, at, rows in reversed(plan):
        unless_mine(step, lambda step=step: greet(holder(step)))
    greet(swapped)

    for copy in loads[:2]:
        copy.wait()
    dwide, swide = 16 * ZROWS, 16 * KINDS
    dline = jnp.concatenate([disp[:, dwide * q : dwide * (q + 1)] for q in range(4)], axis=0)
    sline = jnp.concatenate([spec[:, swide * q : swide * (q + 1)] for q in range(4)], axis=0)
    sline = sline.astype(jnp.float32)
    gap = jnp.zeros((4, KEPT), jnp.float32)
    blank = jnp.zeros((4, LANES - KIND_AT - KINDS), jnp.float32)
    for j in range(16):
        kinds = sline[:, KINDS * j : KINDS * (j + 1)]
        table[pl.ds(j, 4, stride=16), :] = jnp.concatenate(
            [
                dline[:, ZROWS * j : ZROWS * (j + 1)],
                gap,
                kinds[:, KINDS - 6 : KINDS],
                kinds[:, 0 : KINDS - 6],
                blank,
            ],
            axis=1,
        )
    lane_row = lax.broadcasted_iota(jnp.int32, (1, LANES), 1)

    def high(shape):
        ids = lax.broadcasted_iota(jnp.int32, shape, 1)
        return (
            ((ids >= KEPT) & (ids < 2 * KEPT))
            | ((ids >= ZROWS) & (ids < KIND_AT))
            | ((ids >= KIND_AT + KEPT) & (ids < KIND_AT + KEPT + 12))
        )

    ztable[...] = jnp.where(
        high((HALF, LANES)),
        pltpu.roll(table[pl.ds(HALF, HALF), :], KEPT, 1),
        table[pl.ds(0, HALF), :],
    )
    for t, y in enumerate((0, 1, CELLS - 2, CELLS - 1)):
        pack[pl.ds(8 * t, 8), :] = table[pl.ds(y, 8, stride=8), :]
    for t, y in enumerate((0, CELLS - 1)):
        zpack[pl.ds(4 * t, 4), :] = ztable[pl.ds(y, 4, stride=8), :]

    def source(step, rows):
        dx, dy, dz = step
        if dx and dy:
            if dz:
                return ztable.at[pl.ds((HALF - CELLS) * (dx < 0) + (CELLS - 1) * (dy < 0), 1)]
            return table.at[pl.ds(CELLS * (CELLS - 1) * (dx < 0) + (CELLS - 1) * (dy < 0), 1)]
        if dy:
            return (zpack if dz else pack).at[pl.ds(0 if dy > 0 else rows, rows)]
        if dz:
            return ztable.at[pl.ds(HALF - rows if dx < 0 else 0, rows)]
        return table.at[pl.ds(CELLS * origin(dx, 2), rows)]

    def remote(src, dst, send, recv, device):
        return pltpu.make_async_remote_copy(
            src_ref=src,
            dst_ref=dst,
            send_sem=send,
            recv_sem=recv,
            device_id=device,
            device_id_type=pl.DeviceIdType.MESH,
        )

    pl.semaphore_wait(barrier, len(plan))
    for step, at, rows in reversed(plan):
        copy = remote(
            source(step, rows), halo.at[pl.ds(at, rows)], send_a.at[0], recv_a.at[0], worker(step)
        )
        unless_mine(step, copy.start)

    for copy in loads[2:]:
        copy.wait()

    pairs = nbr.shape[1]
    centre_total = cen.shape[1]
    slots = pairs // centre_total
    lane = lax.broadcasted_iota(jnp.int32, (centre_total, pairs), 1)
    row = lax.broadcasted_iota(jnp.int32, (centre_total, pairs), 0)
    mine = ((lane >= row * slots) & (lane < (row + 1) * slots)).astype(jnp.float32)
    mine16 = mine.astype(jnp.bfloat16)
    own = CELLS * CELLS

    def site(atom):
        one, two = atom == 1.0, atom == 2.0
        return (
            jnp.where(one, 0.75, 0.25),
            jnp.where(one | two, 0.75, 0.25),
            jnp.where(two, 0.75, 0.25),
        )

    def kind_lane(z, atom):
        turned = jnp.where(z >= CELLS - 2, z - (CELLS - 2), z + 2.0)
        return KIND_AT + 3.0 * turned + atom

    first = cen[...].astype(jnp.float32)
    cell_i = divided(first, 3.0)
    atom_i = first - 3.0 * cell_i
    col_i = divided(cell_i, CELLS)
    z_i = cell_i - CELLS * col_i
    x_i = divided(col_i, CELLS)
    y_i = col_i - CELLS * x_i
    spot_i = [a + b for a, b in zip((x_i, y_i, z_i), site(atom_i))]
    alive_lane = lax.broadcasted_iota(jnp.int32, (1, centre_total), 1)
    count = jnp.where(alive_lane < alive[...], cnt[...], 0).astype(jnp.float32)
    spread = raw(
        jnp.concatenate(
            spot_i + [count, jnp.zeros((4, centre_total), jnp.float32)], axis=0
        ).astype(jnp.bfloat16),
        mine16,
        NN,
    )
    lanef = lax.broadcasted_iota(jnp.int32, (1, pairs), 1).astype(jnp.float32)
    slot_id = lanef - slots * divided(lanef, slots)
    live = jnp.where(slot_id < spread[3:4], 1.0, 0.0).astype(jnp.float32)

    second = nbr[...].astype(jnp.float32)
    ext = CELLS + 4
    cell_j = divided(second, 3.0)
    atom_j = second - 3.0 * cell_j
    col_j = divided(cell_j, ext)
    z_j = cell_j - ext * col_j - 2.0
    x_j = divided(col_j, ext)
    y_j = col_j - ext * x_j - 2.0
    x_j = x_j - 2.0

    def side(v):
        return jnp.where(v < 0.0, -1.0, jnp.where(v >= CELLS, 1.0, 0.0))

    sx, sy, sz = side(x_j), side(y_j), side(z_j)
    x_in, y_in, z_in = x_j - CELLS * sx, y_j - CELLS * sy, z_j - CELLS * sz
    if sizes[2] == 2:
        sz = jnp.abs(sz)
    code = sx * 9.0 + sy * 3.0 + sz
    upper = jnp.where(x_in >= CELLS // 2, 1.0, 0.0)
    across, along = x_in * CELLS + y_in, y_in * CELLS + x_in
    line = jnp.full_like(code, -1.0)
    for (dx, dy, dz), at, rows in plan:
        if dx and dy:
            value = float(at)
        elif dz and dy:
            value = x_in - (CELLS // 2) * upper + float(at)
        elif dz and dx:
            value = y_in + float(at)
        elif dz:
            value = across - HALF * upper + float(at)
        elif dy:
            value = along + float(at - CELLS * origin(dy, 2))
        else:
            value = across + float(at - CELLS * origin(dx, 2))
        line = jnp.where(code == float(dx * 9 + dy * 3 + dz), value, line)
    raised = jnp.where(sz != 0.0, KEPT * upper, 0.0)
    place_j = 9.0 * z_in + 3.0 * atom_j + raised
    kind_at_j = kind_lane(z_in, atom_j) + raised
    inner = jnp.where(code == 0.0, across, -1.0)

    tail = jnp.full((1, LANES - centre_total), -8.0, jnp.float32)
    column = jnp.concatenate([inner, col_i, tail], axis=1).astype(jnp.int32)
    place = jnp.concatenate(
        [jnp.where(code == 0.0, place_j, -8.0), 9.0 * z_i + 3.0 * atom_i, tail], axis=1
    ).astype(jnp.int32)
    kind_at = jnp.concatenate([kind_at_j, kind_lane(z_i, atom_i), tail], axis=1).astype(jnp.int32)

    def hot(index, length):
        ids = lax.broadcasted_iota(jnp.int32, (length, index.shape[1]), 0)
        return jnp.where(ids == index, 1.0, 0.0).astype(jnp.bfloat16)

    def picked(stack, at, kind_at):
        ids = lax.broadcasted_iota(jnp.int32, stack.shape, 0)
        body, body_ids = stack[0:96], ids[0:96]
        out = [
            jnp.sum(jnp.where(body_ids == at + c, body, 0.0), axis=0, keepdims=True)
            for c in range(3)
        ]
        kind = jnp.sum(
            jnp.where(ids[88:120] == kind_at, stack[88:120], 0.0), axis=0, keepdims=True
        )
        return out, kind

    def fetch(block, onehot):
        both = raw(jnp.concatenate(halves(block.T), axis=0), onehot, NN)
        return both[:LANES] + both[LANES:]

    hot_own = hot(column, own)
    shift, kind = picked(fetch(table[...], hot_own), place, kind_at)
    from_centre = mm_exact_b(
        jnp.concatenate(
            [v[:, pairs : pairs + centre_total] for v in shift + [kind]]
            + [jnp.zeros((4, centre_total), jnp.float32)],
            axis=0,
        ),
        mine16,
    )
    spot_j = [a + b for a, b in zip((x_j, y_j, z_j), site(atom_j))]
    mail[...] = jnp.concatenate(
        [
            ((spot_j[c] - spread[c : c + 1]) + (shift[c][:, 0:pairs] - from_centre[c : c + 1]))
            * SIDE
            for c in range(3)
        ]
        + [
            from_centre[3:4] + 2.0 * live,
            jnp.where(code == 0.0, kind[:, 0:pairs], 0.0),
            line,
            place_j,
            kind_at_j,
        ],
        axis=0,
    )
    post = remote(mail, inbox, send_a.at[1], recv_a.at[1], worker((0, 0, 0)))
    post.start()

    two = w_two[...]
    two = jnp.concatenate([two[4:12], two[0:4], jnp.zeros_like(two[0:4])], axis=0)
    two_t, lat_t, env_t, out_t = two.T, w_lat[...].T, w_env[...].T, w_out_t[...]

    crossing = plan[-1][1] + plan[-1][2] - 1
    halo_rows = halo.shape[0]

    def every(ref, send, recv):
        span = pl.ds(0, crossing)
        return remote(ref.at[span], ref.at[span], send, recv, swapped)

    post.wait_recv()
    arrivals = every(halo, send_a.at[0], recv_a.at[0])
    arrivals.wait_recv()

    ids = lax.broadcasted_iota(jnp.int32, (8, LANES), 0)

    def with_mine(block, row_of):
        pieces = block
        corner = [(step, at) for step, at, rows in plan if own_corner(step)]
        base = corner[0][1] // 8 * 8
        tile = block[base : base + 8]
        for step, at in corner:
            tile = jnp.where((ids == at - base) & mine_too(step), row_of(step, at), tile)
        pieces = [block[0:base], tile, block[base + 8 :]]
        return jnp.concatenate([p for p in pieces if p.shape[0]], axis=0)

    letter = inbox[...]
    block = with_mine(halo[...], lambda step, at: source(step, 1)[...])
    total_rows = plan[-1][1] + plan[-1][2]
    if total_rows < halo_rows:
        every_id = lax.broadcasted_iota(jnp.int32, (halo_rows, LANES), 0)
        block = jnp.where(every_id < total_rows, block, 0.0)
    hot_j = hot(letter[5:6].astype(jnp.int32), halo_rows)
    there = letter[6:7].astype(jnp.int32)
    shift_j, kind_j = picked(fetch(block, hot_j), there, letter[7:8].astype(jnp.int32))
    rx, ry, rz = [letter[c : c + 1] + SIDE * shift_j[c] for c in range(3)]
    live = jnp.where(letter[3:4] > 1.5, 1.0, 0.0)
    kind_i = letter[3:4] - 2.0 * live
    kind_j = letter[4:5] + kind_j
    dist = jnp.sqrt(rx * rx + ry * ry + rz * rz)
    inv = 1.0 / dist
    ux, uy, uz = rx * inv, ry * inv, rz * inv
    ratio = dist * (1.0 / CUTOFF)
    r2 = ratio * ratio
    r5 = r2 * r2 * ratio
    inside = ratio < 1.0
    bell = jnp.where(inside, 1.0 + r5 * ratio * (-28.0 + ratio * (48.0 - 21.0 * ratio)), 0.0)
    slope = jnp.where(
        inside, r5 * (1.0 - ratio) * (1.0 - ratio) * (-168.0 / CUTOFF), 0.0
    )
    order = (lax.broadcasted_iota(jnp.int32, (NBASIS, pairs), 0) + 1).astype(jnp.float32)
    turns = order * (dist * (0.5 / CUTOFF))
    sines, cosines = wave(turns), wave(turns + 0.25)
    norm = math.sqrt(2.0 / CUTOFF)
    basis = norm * sines * (inv * bell)
    basis_d = norm * (
        cosines * order * (inv * bell * (math.pi / CUTOFF))
        + sines * (inv * (slope - bell * inv))
    )
    kinds = [1.0 - kind_i, kind_i, 1.0 - kind_j, kind_j]
    inputs = jnp.concatenate([basis] + kinds + [jnp.zeros((4, pairs), jnp.float32)], axis=0)

    hidden, hidden_d = silu_pair(mm(two_t, inputs))
    latent, latent_d = silu_pair(mm(lat_t, hidden))
    latent_h = halves(latent)
    plain = mm(env_t, latent_h)
    scale = bell * live
    weight = plain * scale
    s3, s5, s15 = math.sqrt(3.0), math.sqrt(5.0), math.sqrt(15.0)
    harm = [
        jnp.ones_like(ux),
        s3 * ux,
        s3 * uy,
        s3 * uz,
        s15 * ux * uy,
        s15 * uy * uz,
        0.5 * s5 * (3.0 * uz * uz - 1.0),
        s15 * ux * uz,
        0.5 * s15 * (ux * ux - uy * uy),
    ]
    spread_y = halves(jnp.concatenate([h * mine for h in harm], axis=0))
    weight_h = halves(weight)
    bounds = [(0, 1), (1, 4), (4, 9)]
    cuts = [slice(a * centre_total, b * centre_total) for a, b in bounds]

    def cut(pair, s):
        return pair[0][s], pair[1][s]

    environ = ENV * mm(spread_y, weight_h, NT)
    mixed = [mm(environ[s].T, cut(spread_y, s)) for s in cuts]
    width = latent.shape[0]
    joined = jnp.concatenate([latent] + [weight * a for a in mixed], axis=0)
    updated, updated_d = silu_pair(mm(out_t, joined))
    gain = jnp.broadcast_to(readout[...], (8, width)).T[:, 0:1]
    score = jnp.sum(gain * updated, axis=0, keepdims=True)
    pair_energy = score * scale

    d_out = (gain * scale) * updated_d
    back = mm(out_t.T, d_out)
    d_mixed = [back[width * (k + 1) : width * (k + 2)] for k in range(3)]
    d_weight = d_mixed[0] * mixed[0] + d_mixed[1] * mixed[1] + d_mixed[2] * mixed[2]
    passing = [halves(q * weight) for q in d_mixed]
    d_environ = ENV * jnp.concatenate(
        [mm(cut(spread_y, s), p, NT) for s, p in zip(cuts, passing)], axis=0
    )
    d_weight = d_weight + mm(d_environ.T, spread_y)
    d_spread = jnp.concatenate(
        [mm(environ[s], p) for s, p in zip(cuts, passing)], axis=0
    ) + mm(d_environ, weight_h)
    d_harm = [
        jnp.sum(
            d_spread[m * centre_total : (m + 1) * centre_total] * mine, axis=0, keepdims=True
        )
        for m in range(9)
    ]
    d_scale = score + jnp.sum(d_weight * plain, axis=0, keepdims=True)
    d_latent = back[0:width] + mm(w_env[...], d_weight * scale)
    d_hidden = mm(w_lat[...], d_latent * latent_d)
    d_inputs = mm(two, d_hidden * hidden_d)
    d_dist = (
        jnp.sum(d_inputs[0:NBASIS] * basis_d, axis=0, keepdims=True) + d_scale * live * slope
    )
    dux = s3 * d_harm[1] + s15 * (uy * d_harm[4] + uz * d_harm[7] + ux * d_harm[8])
    duy = s3 * d_harm[2] + s15 * (ux * d_harm[4] + uz * d_harm[5] - uy * d_harm[8])
    duz = s3 * d_harm[3] + s15 * (uy * d_harm[5] + ux * d_harm[7]) + 3.0 * s5 * uz * d_harm[6]
    radial = d_dist - (ux * dux + uy * duy + uz * duz) * inv
    grad = [d * inv + u * radial for d, u in ((dux, ux), (duy, uy), (duz, uz))]


    back_mail[0:3, 0:pairs] = jnp.concatenate(grad, axis=0)
    sums = mm_exact_b(
        jnp.concatenate(grad + [pair_energy, jnp.zeros((4, pairs), jnp.float32)], axis=0),
        mine16,
        NT,
    )
    back_mail[:, pairs : pairs + centre_total] = sums[0:4]
    reply = remote(back_mail, back_inbox, send_b.at[1], recv_b.at[1], swapped)
    reply.start()

    def placed(at, values):
        ids = lax.broadcasted_iota(jnp.int32, (96, at.shape[1]), 0)
        out = jnp.zeros(ids.shape, jnp.float32)
        for c in range(3):
            out = jnp.where(ids == at + c, values[c], out)
        return jnp.concatenate(
            [out, jnp.zeros((LANES - 96, at.shape[1]), jnp.float32)], axis=0
        )

    part[...] = mm_exact_a(hot_j, placed(there, [-g for g in grad]))
    for step, at, rows in reversed(plan):
        span = pl.ds(at, rows)
        copy = remote(part.at[span], got.at[span], send_b.at[0], recv_b.at[0], holder(step))
        unless_mine(step, copy.start)

    reply.wait_recv()
    answer = back_inbox[...]
    signs = jnp.where(
        lax.broadcasted_iota(jnp.int32, (1, pairs + LANES), 1) < pairs, -1.0, 1.0
    )
    total[...] = mm_exact_a(
        hot_own, placed(place, [signs * answer[c : c + 1] for c in range(3)])
    )
    result[pl.ds(own, 8), 0:centre_total] = jnp.broadcast_to(
        answer[3:4, pairs : pairs + centre_total], (8, centre_total)
    )
    returns = every(got, send_b.at[0], recv_b.at[0])
    returns.wait_recv()

    def add(spot, value):
        total[spot, :] = total[spot, :] + value

    for (dx, dy, dz), at, rows in plan:
        value = got[pl.ds(at, rows), :]
        x, y = (CELLS - 1) * (dx < 0), (CELLS - 1) * (dy < 0)
        if own_corner((dx, dy, dz)):
            value = jnp.where(mine_too((dx, dy, dz)), part[pl.ds(at, 1), :], value)
            add(pl.ds(CELLS * x + y, 1), value)
        elif dz:
            top = high(value.shape)
            low = jnp.where(top, 0.0, value)
            lifted = pltpu.roll(jnp.where(top, value, 0.0), LANES - KEPT, 1)
            if dx:
                spot = pl.ds(CELLS * x + y, rows)
                add(spot, lifted if dx < 0 else low)
            elif dy:
                add(pl.ds(y, rows, stride=CELLS), low)
                add(pl.ds(HALF + y, rows, stride=CELLS), lifted)
            else:
                add(pl.ds(0, HALF), low)
                add(pl.ds(HALF, HALF), lifted)
        elif dy:
            for t in range(2):
                add(pl.ds(origin(dy, 2) + t, 8, stride=8), value[8 * t : 8 * t + 8])
        else:
            add(pl.ds(CELLS * origin(dx, 2), rows), value)
    for copy in (post, arrivals, reply, returns):
        copy.wait_send()


def unpack_body(result, energy, forces):
    energy[0] = result[pl.ds(CELLS * CELLS, 1), 0 : energy.shape[2]]
    final = jnp.concatenate(
        [result[pl.ds(j, 4, stride=16), :][:, 0:ZROWS] for j in range(16)], axis=1
    )
    wide = 16 * ZROWS
    for q in range(4):
        forces[0, :, wide * q : wide * (q + 1)] = final[q : q + 1, :]


def solution(mesh):
    sizes = tuple(mesh.shape[a] for a in AXES)
    plan, line_total = slot_plan(sizes[2])

    def local(displacement, species, centres, neighbours, neighbour_count, live_centres,
              w_two, w_lat, w_env, w_out, readout):
        pairs = neighbours.shape[2]
        vmem = pl.BlockSpec(memory_space=pltpu.VMEM)
        rows = -(-line_total // 8) * 8
        args = [
            displacement, species, centres, neighbours, neighbour_count, live_centres,
            w_two, w_lat, w_env, w_out.T, readout.reshape(1, -1),
        ]

        def body(*refs):
            kernel_body(sizes, plan, *refs)

        sizes_vmem = [
            (CELLS * CELLS, LANES), (4 * CELLS, LANES), (HALF, LANES), (CELLS, LANES),
            (8, pairs), (8, pairs), (4, pairs + LANES), (4, pairs + LANES),
            (rows, LANES), (rows, LANES), (rows, LANES),
        ]
        result = pl.pallas_call(
            body,
            out_shape=jax.ShapeDtypeStruct((CELLS * CELLS + 8, LANES), jnp.float32),
            in_specs=[pl.BlockSpec(memory_space=pltpu.HBM)] * len(args),
            out_specs=vmem,
            scratch_shapes=[pltpu.VMEM(x.shape, x.dtype) for x in args]
            + [pltpu.VMEM(shape, jnp.float32) for shape in sizes_vmem]
            + [pltpu.SemaphoreType.DMA((2,))] * 4
            + [pltpu.SemaphoreType.DMA((len(args),))],
            compiler_params=pltpu.CompilerParams(collective_id=0, has_side_effects=True),
        )(*args)
        return pl.pallas_call(
            unpack_body,
            out_shape=(
                jax.ShapeDtypeStruct(centres.shape, jnp.float32),
                jax.ShapeDtypeStruct(displacement.shape, jnp.float32),
            ),
            in_specs=[vmem],
            out_specs=(vmem, vmem),
        )(result)

    split = P(*AXES)
    return jax.shard_map(
        local,
        mesh=mesh,
        in_specs=(split,) * 6 + (P(),) * 5,
        out_specs=(split, split),
        check_vma=False,
    )
```

```python
import math

import jax
import jax.numpy as jnp
from jax import lax
from jax.experimental import pallas as pl
from jax.experimental.pallas import tpu as pltpu
from jax.sharding import PartitionSpec as P

CELLS = 8
NBASIS = 8
CUTOFF = 6.0
SIDE = 3.1
ENV = 0.2
LANES = 128
ZROWS = CELLS * 9
KINDS = CELLS * 3
KEPT = 18
KIND_AT = ZROWS + KEPT
HALF = CELLS * CELLS // 2
AXES = ("gx", "gy", "gz")

NN = (((1,), (0,)), ((), ()))
NT = (((1,), (1,)), ((), ()))


def halves(x):
    hi = x.astype(jnp.bfloat16)
    lo = (x - hi.astype(jnp.float32)).astype(jnp.bfloat16)
    return hi, lo


def raw(a, b, dims):
    return lax.dot_general(a, b, dims, preferred_element_type=jnp.float32)


def mm(a, b, dims=NN):
    ah, al = a if isinstance(a, tuple) else halves(a)
    bh, bl = b if isinstance(b, tuple) else halves(b)
    if dims is NT:
        m, n = ah.shape[0], bh.shape[0]
        both = raw(jnp.concatenate([ah, al], axis=0), jnp.concatenate([bh, bl], axis=0), NT)
        return both[:m, :n] + (both[:m, n:] + both[m:, :n])
    if ah.shape[1] > 2 * LANES - 1:
        return raw(ah, bh, dims) + (raw(ah, bl, dims) + raw(al, bh, dims))
    return raw(
        jnp.concatenate([ah, ah, al], axis=1), jnp.concatenate([bh, bl, bh], axis=0), NN
    )


def mm_exact_b(a, b, dims=NN):
    ah, al = halves(a)
    return raw(ah, b, dims) + raw(al, b, dims)


def mm_exact_a(a, b):
    n = b.shape[0]
    both = raw(a, jnp.concatenate(halves(b), axis=0), NT)
    return both[:, :n] + both[:, n:]


def slot_plan(depth):
    sides = [1] if depth == 2 else [1, -1]
    ends = (-1, 1)
    groups = [
        [((0, 0, dz), HALF) for dz in sides],
        [((dx, 0, 0), 2 * CELLS) for dx in ends],
        [((0, dy, 0), 2 * CELLS) for dy in ends],
        [((dx, 0, dz), CELLS) for dz in sides for dx in ends],
        [((0, dy, dz), CELLS // 2) for dz in sides for dy in ends],
        [((dx, dy, 0), 1) for dx in ends for dy in ends],
        [((dx, dy, dz), 1) for dz in sides for dx in ends for dy in ends],
    ]
    plan, at = [], 0
    for step, rows in [entry for group in groups for entry in group]:
        plan.append((step, at, rows))
        at += rows
    return plan, at


def origin(step, tiles):
    return 0 if step >= 0 else CELLS - tiles


def own_corner(step):
    return step[2] == 0 and step[0] != 0 and step[1] != 0


def wave(turns):
    f = turns - jnp.floor(turns + 0.5)
    f = jnp.where(f > 0.25, 0.5 - f, jnp.where(f < -0.25, -0.5 - f, f))
    x = f * (2.0 * math.pi)
    s = x * x
    p = -1.0 / 39916800.0
    for c in (1.0 / 362880.0, -1.0 / 5040.0, 1.0 / 120.0, -1.0 / 6.0):
        p = p * s + c
    return x + x * s * p


def divided(value, by):
    return jnp.floor((value + 0.5) * (1.0 / by))


def silu_pair(x):
    s = 1.0 / (1.0 + jnp.exp(-x))
    return x * s, s * (1.0 + x * (1.0 - s))


def kernel_body(sizes, plan, disp_hbm, spec_hbm, cen_hbm, nbr_hbm, cnt_hbm, alive_hbm, two_hbm,
                lat_hbm, env_hbm, out_hbm, readout_hbm, result,
                disp, spec, cen, nbr, cnt, alive, w_two, w_lat, w_env, w_out_t, readout,
                table, pack, ztable, zpack, mail, inbox, back_mail, back_inbox, halo, part, got,
                send_a, recv_a, send_b, recv_b, load):
    loads = [
        pltpu.make_async_copy(src, dst, load.at[at])
        for at, (src, dst) in enumerate(
            (
                (disp_hbm, disp),
                (spec_hbm, spec),
                (cen_hbm, cen),
                (nbr_hbm, nbr),
                (cnt_hbm, cnt),
                (alive_hbm, alive),
                (two_hbm, w_two),
                (lat_hbm, w_lat),
                (env_hbm, w_env),
                (out_hbm, w_out_t),
                (readout_hbm, readout),
            )
        )
    ]
    for copy in loads:
        copy.start()
    disp, spec, cen, nbr, cnt, alive = (
        ref.at[0] for ref in (disp, spec, cen, nbr, cnt, alive)
    )
    total = result.at[pl.ds(0, CELLS * CELLS)]
    me = tuple(lax.axis_index(a) for a in AXES)
    odd = [lax.rem(i, 2) for i in me[:2]]
    swapped = tuple(i + 1 - 2 * o for i, o in zip(me, odd)) + me[2:]

    def moved(place, step, sign):
        return tuple(
            lax.rem(i + (sign * d + n), n) if d else i for i, d, n in zip(place, step, sizes)
        )

    def holder(step):
        return moved(swapped, step, 1)

    def worker(step):
        x, y, z = moved(me, step, -1)
        return x + 1 - 2 * lax.rem(x, 2), y + 1 - 2 * lax.rem(y, 2), z

    def mine_too(step):
        return (odd[0] == (1 if step[0] > 0 else 0)) & (odd[1] == (1 if step[1] > 0 else 0))

    barrier = pltpu.get_barrier_semaphore()

    def greet(device):
        pl.semaphore_signal(
            barrier, inc=1, device_id=device, device_id_type=pl.DeviceIdType.MESH
        )

    def unless_mine(step, action):
        if own_corner(step):
            pl.when(jnp.logical_not(mine_too(step)))(action)
        else:
            action()

    for step, at, rows in reversed(plan):
        unless_mine(step, lambda step=step: greet(holder(step)))
    greet(swapped)

    for copy in loads[:2]:
        copy.wait()
    dwide, swide = 16 * ZROWS, 16 * KINDS
    dline = jnp.concatenate([disp[:, dwide * q : dwide * (q + 1)] for q in range(4)], axis=0)
    sline = jnp.concatenate([spec[:, swide * q : swide * (q + 1)] for q in range(4)], axis=0)
    sline = sline.astype(jnp.float32)
    gap = jnp.zeros((4, KEPT), jnp.float32)
    blank = jnp.zeros((4, LANES - KIND_AT - KINDS), jnp.float32)
    for j in range(16):
        kinds = sline[:, KINDS * j : KINDS * (j + 1)]
        table[pl.ds(j, 4, stride=16), :] = jnp.concatenate(
            [
                dline[:, ZROWS * j : ZROWS * (j + 1)],
                gap,
                kinds[:, KINDS - 6 : KINDS],
                kinds[:, 0 : KINDS - 6],
                blank,
            ],
            axis=1,
        )
    lane_row = lax.broadcasted_iota(jnp.int32, (1, LANES), 1)

    def high(shape):
        ids = lax.broadcasted_iota(jnp.int32, shape, 1)
        return (
            ((ids >= KEPT) & (ids < 2 * KEPT))
            | ((ids >= ZROWS) & (ids < KIND_AT))
            | ((ids >= KIND_AT + KEPT) & (ids < KIND_AT + KEPT + 12))
        )

    ztable[...] = jnp.where(
        high((HALF, LANES)),
        pltpu.roll(table[pl.ds(HALF, HALF), :], KEPT, 1),
        table[pl.ds(0, HALF), :],
    )
    for t, y in enumerate((0, 1, CELLS - 2, CELLS - 1)):
        pack[pl.ds(8 * t, 8), :] = table[pl.ds(y, 8, stride=8), :]
    for t, y in enumerate((0, CELLS - 1)):
        zpack[pl.ds(4 * t, 4), :] = ztable[pl.ds(y, 4, stride=8), :]

    def source(step, rows):
        dx, dy, dz = step
        if dx and dy:
            if dz:
                return ztable.at[pl.ds((HALF - CELLS) * (dx < 0) + (CELLS - 1) * (dy < 0), 1)]
            return table.at[pl.ds(CELLS * (CELLS - 1) * (dx < 0) + (CELLS - 1) * (dy < 0), 1)]
        if dy:
            return (zpack if dz else pack).at[pl.ds(0 if dy > 0 else rows, rows)]
        if dz:
            return ztable.at[pl.ds(HALF - rows if dx < 0 else 0, rows)]
        return table.at[pl.ds(CELLS * origin(dx, 2), rows)]

    def remote(src, dst, send, recv, device):
        return pltpu.make_async_remote_copy(
            src_ref=src,
            dst_ref=dst,
            send_sem=send,
            recv_sem=recv,
            device_id=device,
            device_id_type=pl.DeviceIdType.MESH,
        )

    pl.semaphore_wait(barrier, len(plan))
    for step, at, rows in reversed(plan):
        copy = remote(
            source(step, rows), halo.at[pl.ds(at, rows)], send_a.at[0], recv_a.at[0], worker(step)
        )
        unless_mine(step, copy.start)

    for copy in loads[2:]:
        copy.wait()

    pairs = nbr.shape[1]
    centre_total = cen.shape[1]
    slots = pairs // centre_total
    lane = lax.broadcasted_iota(jnp.int32, (centre_total, pairs), 1)
    row = lax.broadcasted_iota(jnp.int32, (centre_total, pairs), 0)
    mine = ((lane >= row * slots) & (lane < (row + 1) * slots)).astype(jnp.float32)
    mine16 = mine.astype(jnp.bfloat16)
    own = CELLS * CELLS

    def site(atom):
        one, two = atom == 1.0, atom == 2.0
        return (
            jnp.where(one, 0.75, 0.25),
            jnp.where(one | two, 0.75, 0.25),
            jnp.where(two, 0.75, 0.25),
        )

    def kind_lane(z, atom):
        turned = jnp.where(z >= CELLS - 2, z - (CELLS - 2), z + 2.0)
        return KIND_AT + 3.0 * turned + atom

    first = cen[...].astype(jnp.float32)
    cell_i = divided(first, 3.0)
    atom_i = first - 3.0 * cell_i
    col_i = divided(cell_i, CELLS)
    z_i = cell_i - CELLS * col_i
    x_i = divided(col_i, CELLS)
    y_i = col_i - CELLS * x_i
    spot_i = [a + b for a, b in zip((x_i, y_i, z_i), site(atom_i))]
    alive_lane = lax.broadcasted_iota(jnp.int32, (1, centre_total), 1)
    count = jnp.where(alive_lane < alive[...], cnt[...], 0).astype(jnp.float32)
    spread = raw(
        jnp.concatenate(
            spot_i + [count, jnp.zeros((4, centre_total), jnp.float32)], axis=0
        ).astype(jnp.bfloat16),
        mine16,
        NN,
    )
    lanef = lax.broadcasted_iota(jnp.int32, (1, pairs), 1).astype(jnp.float32)
    slot_id = lanef - slots * divided(lanef, slots)
    live = jnp.where(slot_id < spread[3:4], 1.0, 0.0).astype(jnp.float32)

    second = nbr[...].astype(jnp.float32)
    ext = CELLS + 4
    cell_j = divided(second, 3.0)
    atom_j = second - 3.0 * cell_j
    col_j = divided(cell_j, ext)
    z_j = cell_j - ext * col_j - 2.0
    x_j = divided(col_j, ext)
    y_j = col_j - ext * x_j - 2.0
    x_j = x_j - 2.0

    def side(v):
        return jnp.where(v < 0.0, -1.0, jnp.where(v >= CELLS, 1.0, 0.0))

    sx, sy, sz = side(x_j), side(y_j), side(z_j)
    x_in, y_in, z_in = x_j - CELLS * sx, y_j - CELLS * sy, z_j - CELLS * sz
    if sizes[2] == 2:
        sz = jnp.abs(sz)
    code = sx * 9.0 + sy * 3.0 + sz
    upper = jnp.where(x_in >= CELLS // 2, 1.0, 0.0)
    across, along = x_in * CELLS + y_in, y_in * CELLS + x_in
    line = jnp.full_like(code, -1.0)
    for (dx, dy, dz), at, rows in plan:
        if dx and dy:
            value = float(at)
        elif dz and dy:
            value = x_in - (CELLS // 2) * upper + float(at)
        elif dz and dx:
            value = y_in + float(at)
        elif dz:
            value = across - HALF * upper + float(at)
        elif dy:
            value = along + float(at - CELLS * origin(dy, 2))
        else:
            value = across + float(at - CELLS * origin(dx, 2))
        line = jnp.where(code == float(dx * 9 + dy * 3 + dz), value, line)
    raised = jnp.where(sz != 0.0, KEPT * upper, 0.0)
    place_j = 9.0 * z_in + 3.0 * atom_j + raised
    kind_at_j = kind_lane(z_in, atom_j) + raised
    inner = jnp.where(code == 0.0, across, -1.0)

    tail = jnp.full((1, LANES - centre_total), -8.0, jnp.float32)
    column = jnp.concatenate([inner, col_i, tail], axis=1).astype(jnp.int32)
    place = jnp.concatenate(
        [jnp.where(code == 0.0, place_j, -8.0), 9.0 * z_i + 3.0 * atom_i, tail], axis=1
    ).astype(jnp.int32)
    kind_at = jnp.concatenate([kind_at_j, kind_lane(z_i, atom_i), tail], axis=1).astype(jnp.int32)

    def hot(index, length):
        ids = lax.broadcasted_iota(jnp.int32, (length, index.shape[1]), 0)
        return jnp.where(ids == index, 1.0, 0.0).astype(jnp.bfloat16)

    def picked(stack, at, kind_at):
        ids = lax.broadcasted_iota(jnp.int32, stack.shape, 0)
        body, body_ids = stack[0:96], ids[0:96]
        out = [
            jnp.sum(jnp.where(body_ids == at + c, body, 0.0), axis=0, keepdims=True)
            for c in range(3)
        ]
        kind = jnp.sum(
            jnp.where(ids[88:120] == kind_at, stack[88:120], 0.0), axis=0, keepdims=True
        )
        return out, kind

    def fetch(block, onehot):
        both = raw(jnp.concatenate(halves(block.T), axis=0), onehot, NN)
        return both[:LANES] + both[LANES:]

    hot_own = hot(column, own)
    shift, kind = picked(fetch(table[...], hot_own), place, kind_at)
    from_centre = mm_exact_b(
        jnp.concatenate(
            [v[:, pairs : pairs + centre_total] for v in shift + [kind]]
            + [jnp.zeros((4, centre_total), jnp.float32)],
            axis=0,
        ),
        mine16,
    )
    spot_j = [a + b for a, b in zip((x_j, y_j, z_j), site(atom_j))]
    mail[...] = jnp.concatenate(
        [
            ((spot_j[c] - spread[c : c + 1]) + (shift[c][:, 0:pairs] - from_centre[c : c + 1]))
            * SIDE
            for c in range(3)
        ]
        + [
            from_centre[3:4] + 2.0 * live,
            jnp.where(code == 0.0, kind[:, 0:pairs], 0.0),
            line,
            place_j,
            kind_at_j,
        ],
        axis=0,
    )
    post = remote(mail, inbox, send_a.at[1], recv_a.at[1], worker((0, 0, 0)))
    post.start()

    two = w_two[...]
    two = jnp.concatenate([two[4:12], two[0:4], jnp.zeros_like(two[0:4])], axis=0)
    two_t, lat_t, env_t, out_t = two.T, w_lat[...].T, w_env[...].T, w_out_t[...]

    crossing = plan[-1][1] + plan[-1][2] - 1
    halo_rows = halo.shape[0]

    def every(ref, send, recv):
        span = pl.ds(0, crossing)
        return remote(ref.at[span], ref.at[span], send, recv, swapped)

    post.wait_recv()
    arrivals = every(halo, send_a.at[0], recv_a.at[0])
    arrivals.wait_recv()

    ids = lax.broadcasted_iota(jnp.int32, (8, LANES), 0)

    def with_mine(block, row_of):
        pieces = block
        corner = [(step, at) for step, at, rows in plan if own_corner(step)]
        base = corner[0][1] // 8 * 8
        tile = block[base : base + 8]
        for step, at in corner:
            tile = jnp.where((ids == at - base) & mine_too(step), row_of(step, at), tile)
        pieces = [block[0:base], tile, block[base + 8 :]]
        return jnp.concatenate([p for p in pieces if p.shape[0]], axis=0)

    letter = inbox[...]
    block = with_mine(halo[...], lambda step, at: source(step, 1)[...])
    total_rows = plan[-1][1] + plan[-1][2]
    if total_rows < halo_rows:
        every_id = lax.broadcasted_iota(jnp.int32, (halo_rows, LANES), 0)
        block = jnp.where(every_id < total_rows, block, 0.0)
    hot_j = hot(letter[5:6].astype(jnp.int32), halo_rows)
    there = letter[6:7].astype(jnp.int32)
    shift_j, kind_j = picked(fetch(block, hot_j), there, letter[7:8].astype(jnp.int32))
    rx, ry, rz = [letter[c : c + 1] + SIDE * shift_j[c] for c in range(3)]
    live = jnp.where(letter[3:4] > 1.5, 1.0, 0.0)
    kind_i = letter[3:4] - 2.0 * live
    kind_j = letter[4:5] + kind_j
    dist = jnp.sqrt(rx * rx + ry * ry + rz * rz)
    inv = 1.0 / dist
    ux, uy, uz = rx * inv, ry * inv, rz * inv
    ratio = dist * (1.0 / CUTOFF)
    r2 = ratio * ratio
    r5 = r2 * r2 * ratio
    inside = ratio < 1.0
    bell = jnp.where(inside, 1.0 + r5 * ratio * (-28.0 + ratio * (48.0 - 21.0 * ratio)), 0.0)
    slope = jnp.where(
        inside, r5 * (1.0 - ratio) * (1.0 - ratio) * (-168.0 / CUTOFF), 0.0
    )
    order = (lax.broadcasted_iota(jnp.int32, (NBASIS, pairs), 0) + 1).astype(jnp.float32)
    turns = order * (dist * (0.5 / CUTOFF))
    sines, cosines = wave(turns), wave(turns + 0.25)
    norm = math.sqrt(2.0 / CUTOFF)
    basis = norm * sines * (inv * bell)
    basis_d = norm * (
        cosines * order * (inv * bell * (math.pi / CUTOFF))
        + sines * (inv * (slope - bell * inv))
    )
    kinds = [1.0 - kind_i, kind_i, 1.0 - kind_j, kind_j]
    inputs = jnp.concatenate([basis] + kinds + [jnp.zeros((4, pairs), jnp.float32)], axis=0)

    hidden, hidden_d = silu_pair(mm(two_t, inputs))
    latent, latent_d = silu_pair(mm(lat_t, hidden))
    latent_h = halves(latent)
    plain = mm(env_t, latent_h)
    scale = bell * live
    weight = plain * scale
    s3, s5, s15 = math.sqrt(3.0), math.sqrt(5.0), math.sqrt(15.0)
    harm = [
        jnp.ones_like(ux),
        s3 * ux,
        s3 * uy,
        s3 * uz,
        s15 * ux * uy,
        s15 * uy * uz,
        0.5 * s5 * (3.0 * uz * uz - 1.0),
        s15 * ux * uz,
        0.5 * s15 * (ux * ux - uy * uy),
    ]
    spread_y = halves(jnp.concatenate([h * mine for h in harm], axis=0))
    weight_h = halves(weight)
    bounds = [(0, 1), (1, 4), (4, 9)]
    cuts = [slice(a * centre_total, b * centre_total) for a, b in bounds]

    def cut(pair, s):
        return pair[0][s], pair[1][s]

    environ = ENV * mm(spread_y, weight_h, NT)
    mixed = [mm(environ[s].T, cut(spread_y, s)) for s in cuts]
    width = latent.shape[0]
    joined = jnp.concatenate([latent] + [weight * a for a in mixed], axis=0)
    updated, updated_d = silu_pair(mm(out_t, joined))
    gain = jnp.broadcast_to(readout[...], (8, width)).T[:, 0:1]
    score = jnp.sum(gain * updated, axis=0, keepdims=True)
    pair_energy = score * scale

    d_out = (gain * scale) * updated_d
    back = mm(out_t.T, d_out)
    d_mixed = [back[width * (k + 1) : width * (k + 2)] for k in range(3)]
    d_weight = d_mixed[0] * mixed[0] + d_mixed[1] * mixed[1] + d_mixed[2] * mixed[2]
    passing = [halves(q * weight) for q in d_mixed]
    d_environ = ENV * jnp.concatenate(
        [mm(cut(spread_y, s), p, NT) for s, p in zip(cuts, passing)], axis=0
    )
    d_weight = d_weight + mm(d_environ.T, spread_y)
    d_spread = jnp.concatenate(
        [mm(environ[s], p) for s, p in zip(cuts, passing)], axis=0
    ) + mm(d_environ, weight_h)
    d_harm = [
        jnp.sum(
            d_spread[m * centre_total : (m + 1) * centre_total] * mine, axis=0, keepdims=True
        )
        for m in range(9)
    ]
    d_scale = score + jnp.sum(d_weight * plain, axis=0, keepdims=True)
    d_latent = back[0:width] + mm(w_env[...], d_weight * scale)
    d_hidden = mm(w_lat[...], d_latent * latent_d)
    d_inputs = mm(two, d_hidden * hidden_d)
    d_dist = (
        jnp.sum(d_inputs[0:NBASIS] * basis_d, axis=0, keepdims=True) + d_scale * live * slope
    )
    dux = s3 * d_harm[1] + s15 * (uy * d_harm[4] + uz * d_harm[7] + ux * d_harm[8])
    duy = s3 * d_harm[2] + s15 * (ux * d_harm[4] + uz * d_harm[5] - uy * d_harm[8])
    duz = s3 * d_harm[3] + s15 * (uy * d_harm[5] + ux * d_harm[7]) + 3.0 * s5 * uz * d_harm[6]
    radial = d_dist - (ux * dux + uy * duy + uz * duz) * inv
    grad = [d * inv + u * radial for d, u in ((dux, ux), (duy, uy), (duz, uz))]


    back_mail[0:3, 0:pairs] = jnp.concatenate(grad, axis=0)
    sums = mm_exact_b(
        jnp.concatenate(grad + [pair_energy, jnp.zeros((4, pairs), jnp.float32)], axis=0),
        mine16,
        NT,
    )
    back_mail[:, pairs : pairs + centre_total] = sums[0:4]
    reply = remote(back_mail, back_inbox, send_b.at[1], recv_b.at[1], swapped)
    reply.start()

    def placed(at, values):
        ids = lax.broadcasted_iota(jnp.int32, (96, at.shape[1]), 0)
        out = jnp.zeros(ids.shape, jnp.float32)
        for c in range(3):
            out = jnp.where(ids == at + c, values[c], out)
        return jnp.concatenate(
            [out, jnp.zeros((LANES - 96, at.shape[1]), jnp.float32)], axis=0
        )

    part[...] = mm_exact_a(hot_j, placed(there, [-g for g in grad]))
    for step, at, rows in reversed(plan):
        span = pl.ds(at, rows)
        copy = remote(part.at[span], got.at[span], send_b.at[0], recv_b.at[0], holder(step))
        unless_mine(step, copy.start)

    reply.wait_recv()
    answer = back_inbox[...]
    signs = jnp.where(
        lax.broadcasted_iota(jnp.int32, (1, pairs + LANES), 1) < pairs, -1.0, 1.0
    )
    total[...] = mm_exact_a(
        hot_own, placed(place, [signs * answer[c : c + 1] for c in range(3)])
    )
    result[pl.ds(own, 8), 0:centre_total] = jnp.broadcast_to(
        answer[3:4, pairs : pairs + centre_total], (8, centre_total)
    )
    returns = every(got, send_b.at[0], recv_b.at[0])
    returns.wait_recv()

    def add(spot, value):
        total[spot, :] = total[spot, :] + value

    for (dx, dy, dz), at, rows in plan:
        value = got[pl.ds(at, rows), :]
        x, y = (CELLS - 1) * (dx < 0), (CELLS - 1) * (dy < 0)
        if own_corner((dx, dy, dz)):
            value = jnp.where(mine_too((dx, dy, dz)), part[pl.ds(at, 1), :], value)
            add(pl.ds(CELLS * x + y, 1), value)
        elif dz:
            top = high(value.shape)
            low = jnp.where(top, 0.0, value)
            lifted = pltpu.roll(jnp.where(top, value, 0.0), LANES - KEPT, 1)
            if dx:
                spot = pl.ds(CELLS * x + y, rows)
                add(spot, lifted if dx < 0 else low)
            elif dy:
                add(pl.ds(y, rows, stride=CELLS), low)
                add(pl.ds(HALF + y, rows, stride=CELLS), lifted)
            else:
                add(pl.ds(0, HALF), low)
                add(pl.ds(HALF, HALF), lifted)
        elif dy:
            for t in range(2):
                add(pl.ds(origin(dy, 2) + t, 8, stride=8), value[8 * t : 8 * t + 8])
        else:
            add(pl.ds(CELLS * origin(dx, 2), rows), value)
    for copy in (post, arrivals, reply, returns):
        copy.wait_send()


def unpack_body(result, energy, forces):
    energy[0] = result[pl.ds(CELLS * CELLS, 1), 0 : energy.shape[2]]
    final = jnp.concatenate(
        [result[pl.ds(j, 4, stride=16), :][:, 0:ZROWS] for j in range(16)], axis=1
    )
    wide = 16 * ZROWS
    for q in range(4):
        forces[0, :, wide * q : wide * (q + 1)] = final[q : q + 1, :]


def solution(mesh):
    sizes = tuple(mesh.shape[a] for a in AXES)
    plan, line_total = slot_plan(sizes[2])

    def local(displacement, species, centres, neighbours, neighbour_count, live_centres,
              w_two, w_lat, w_env, w_out, readout):
        pairs = neighbours.shape[2]
        vmem = pl.BlockSpec(memory_space=pltpu.VMEM)
        rows = -(-line_total // 8) * 8
        args = [
            displacement, species, centres, neighbours, neighbour_count, live_centres,
            w_two, w_lat, w_env, w_out.T, readout.reshape(1, -1),
        ]

        def body(*refs):
            kernel_body(sizes, plan, *refs)

        sizes_vmem = [
            (CELLS * CELLS, LANES), (4 * CELLS, LANES), (HALF, LANES), (CELLS, LANES),
            (8, pairs), (8, pairs), (4, pairs + LANES), (4, pairs + LANES),
            (rows, LANES), (rows, LANES), (rows, LANES),
        ]
        result = pl.pallas_call(
            body,
            out_shape=pltpu.VMEM((CELLS * CELLS + 8, LANES), jnp.float32),
            in_specs=[pl.BlockSpec(memory_space=pltpu.HBM)] * len(args),
            out_specs=vmem,
            scratch_shapes=[pltpu.VMEM(x.shape, x.dtype) for x in args]
            + [pltpu.VMEM(shape, jnp.float32) for shape in sizes_vmem]
            + [pltpu.SemaphoreType.DMA((2,))] * 4
            + [pltpu.SemaphoreType.DMA((len(args),))],
            compiler_params=pltpu.CompilerParams(collective_id=0, has_side_effects=True),
        )(*args)
        result = pltpu.with_memory_space_constraint(result, pltpu.VMEM)
        return pl.pallas_call(
            unpack_body,
            out_shape=(
                jax.ShapeDtypeStruct(centres.shape, jnp.float32),
                jax.ShapeDtypeStruct(displacement.shape, jnp.float32),
            ),
            in_specs=[vmem],
            out_specs=(vmem, vmem),
        )(result)

    split = P(*AXES)
    return jax.shard_map(
        local,
        mesh=mesh,
        in_specs=(split,) * 6 + (P(),) * 5,
        out_specs=(split, split),
        check_vma=False,
    )
```

```python
import math

import jax
import jax.numpy as jnp
from jax import lax
from jax.experimental import pallas as pl
from jax.experimental.pallas import tpu as pltpu
from jax.sharding import PartitionSpec as P

CELLS = 8
NBASIS = 8
CUTOFF = 6.0
SIDE = 3.1
ENV = 0.2
LANES = 128
ZROWS = CELLS * 9
KINDS = CELLS * 3
KEPT = 18
KIND_AT = ZROWS + KEPT
HALF = CELLS * CELLS // 2
AXES = ("gx", "gy", "gz")

NN = (((1,), (0,)), ((), ()))
NT = (((1,), (1,)), ((), ()))


def halves(x):
    hi = x.astype(jnp.bfloat16)
    lo = (x - hi.astype(jnp.float32)).astype(jnp.bfloat16)
    return hi, lo


def raw(a, b, dims):
    return lax.dot_general(a, b, dims, preferred_element_type=jnp.float32)


def thrice(a):
    high, low = halves(a)
    return jnp.concatenate([high, high, low], axis=1)


def stacked(b):
    high, low = halves(b)
    return jnp.concatenate([high, low, high], axis=0)


def doubled(b):
    return jnp.concatenate(halves(b), axis=0)


def by_parts(a, bh, bl, dims=NN):
    n = a.shape[0] // 2
    both = raw(a, bh, dims)
    return both[:n] + (both[n:] + raw(a[:n], bl, dims))


def mm_exact_b(a, b, dims=NN):
    ah, al = halves(a)
    return raw(ah, b, dims) + raw(al, b, dims)


def mm_exact_a(a, b):
    n = b.shape[0]
    both = raw(a, jnp.concatenate(halves(b), axis=0), NT)
    return both[:, :n] + both[:, n:]


def slot_plan(depth):
    sides = [1] if depth == 2 else [1, -1]
    ends = (-1, 1)
    groups = [
        [((0, 0, dz), HALF) for dz in sides],
        [((dx, 0, 0), 2 * CELLS) for dx in ends],
        [((0, dy, 0), 2 * CELLS) for dy in ends],
        [((dx, 0, dz), CELLS) for dz in sides for dx in ends],
        [((0, dy, dz), CELLS // 2) for dz in sides for dy in ends],
        [((dx, dy, 0), 1) for dx in ends for dy in ends],
        [((dx, dy, dz), 1) for dz in sides for dx in ends for dy in ends],
    ]
    plan, at = [], 0
    for step, rows in [entry for group in groups for entry in group]:
        plan.append((step, at, rows))
        at += rows
    return plan, at


def origin(step, tiles):
    return 0 if step >= 0 else CELLS - tiles


def own_corner(step):
    return step[2] == 0 and step[0] != 0 and step[1] != 0


def wave(turns):
    f = turns - jnp.floor(turns + 0.5)
    f = jnp.where(f > 0.25, 0.5 - f, jnp.where(f < -0.25, -0.5 - f, f))
    x = f * (2.0 * math.pi)
    s = x * x
    p = -1.0 / 39916800.0
    for c in (1.0 / 362880.0, -1.0 / 5040.0, 1.0 / 120.0, -1.0 / 6.0):
        p = p * s + c
    return x + x * s * p


def divided(value, by):
    return jnp.floor((value + 0.5) * (1.0 / by))


def silu_pair(x):
    s = 1.0 / (1.0 + jnp.exp(-x))
    return x * s, s * (1.0 + x * (1.0 - s))


def kernel_body(sizes, plan, disp_hbm, spec_hbm, cen_hbm, nbr_hbm, cnt_hbm, alive_hbm, two_hbm,
                lat_hbm, env_hbm, out_hbm, readout_hbm, result,
                disp, spec, cen, nbr, cnt, alive, w_two, w_lat, w_env, w_out_t, readout,
                table, pack, ztable, zpack, mail, inbox, back_mail, back_inbox, halo, part, got,
                send_a, recv_a, send_b, recv_b, load):
    loads = [
        pltpu.make_async_copy(src, dst, load.at[at])
        for at, (src, dst) in enumerate(
            (
                (disp_hbm, disp),
                (spec_hbm, spec),
                (cen_hbm, cen),
                (nbr_hbm, nbr),
                (cnt_hbm, cnt),
                (alive_hbm, alive),
                (two_hbm, w_two),
                (lat_hbm, w_lat),
                (env_hbm, w_env),
                (out_hbm, w_out_t),
                (readout_hbm, readout),
            )
        )
    ]
    for copy in loads:
        copy.start()
    disp, spec, cen, nbr, cnt, alive = (
        ref.at[0] for ref in (disp, spec, cen, nbr, cnt, alive)
    )
    total = result.at[pl.ds(0, CELLS * CELLS)]
    me = tuple(lax.axis_index(a) for a in AXES)
    odd = [lax.rem(i, 2) for i in me[:2]]
    swapped = tuple(i + 1 - 2 * o for i, o in zip(me, odd)) + me[2:]

    def moved(place, step, sign):
        return tuple(
            lax.rem(i + (sign * d + n), n) if d else i for i, d, n in zip(place, step, sizes)
        )

    def holder(step):
        return moved(swapped, step, 1)

    def worker(step):
        x, y, z = moved(me, step, -1)
        return x + 1 - 2 * lax.rem(x, 2), y + 1 - 2 * lax.rem(y, 2), z

    def mine_too(step):
        return (odd[0] == (1 if step[0] > 0 else 0)) & (odd[1] == (1 if step[1] > 0 else 0))

    barrier = pltpu.get_barrier_semaphore()

    def greet(device):
        pl.semaphore_signal(
            barrier, inc=1, device_id=device, device_id_type=pl.DeviceIdType.MESH
        )

    def unless_mine(step, action):
        if own_corner(step):
            pl.when(jnp.logical_not(mine_too(step)))(action)
        else:
            action()

    for step, at, rows in reversed(plan):
        unless_mine(step, lambda step=step: greet(holder(step)))
    greet(swapped)

    for copy in loads[:2]:
        copy.wait()
    dwide, swide = 16 * ZROWS, 16 * KINDS
    dline = jnp.concatenate([disp[:, dwide * q : dwide * (q + 1)] for q in range(4)], axis=0)
    sline = jnp.concatenate([spec[:, swide * q : swide * (q + 1)] for q in range(4)], axis=0)
    sline = sline.astype(jnp.float32)
    gap = jnp.zeros((4, KEPT), jnp.float32)
    blank = jnp.zeros((4, LANES - KIND_AT - KINDS), jnp.float32)
    for j in range(16):
        kinds = sline[:, KINDS * j : KINDS * (j + 1)]
        table[pl.ds(j, 4, stride=16), :] = jnp.concatenate(
            [
                dline[:, ZROWS * j : ZROWS * (j + 1)],
                gap,
                kinds[:, KINDS - 6 : KINDS],
                kinds[:, 0 : KINDS - 6],
                blank,
            ],
            axis=1,
        )
    lane_row = lax.broadcasted_iota(jnp.int32, (1, LANES), 1)

    def high(shape):
        ids = lax.broadcasted_iota(jnp.int32, shape, 1)
        return (
            ((ids >= KEPT) & (ids < 2 * KEPT))
            | ((ids >= ZROWS) & (ids < KIND_AT))
            | ((ids >= KIND_AT + KEPT) & (ids < KIND_AT + KEPT + 12))
        )

    ztable[...] = jnp.where(
        high((HALF, LANES)),
        pltpu.roll(table[pl.ds(HALF, HALF), :], KEPT, 1),
        table[pl.ds(0, HALF), :],
    )
    for t, y in enumerate((0, 1, CELLS - 2, CELLS - 1)):
        pack[pl.ds(8 * t, 8), :] = table[pl.ds(y, 8, stride=8), :]
    for t, y in enumerate((0, CELLS - 1)):
        zpack[pl.ds(4 * t, 4), :] = ztable[pl.ds(y, 4, stride=8), :]

    def source(step, rows):
        dx, dy, dz = step
        if dx and dy:
            if dz:
                return ztable.at[pl.ds((HALF - CELLS) * (dx < 0) + (CELLS - 1) * (dy < 0), 1)]
            return table.at[pl.ds(CELLS * (CELLS - 1) * (dx < 0) + (CELLS - 1) * (dy < 0), 1)]
        if dy:
            return (zpack if dz else pack).at[pl.ds(0 if dy > 0 else rows, rows)]
        if dz:
            return ztable.at[pl.ds(HALF - rows if dx < 0 else 0, rows)]
        return table.at[pl.ds(CELLS * origin(dx, 2), rows)]

    def remote(src, dst, send, recv, device):
        return pltpu.make_async_remote_copy(
            src_ref=src,
            dst_ref=dst,
            send_sem=send,
            recv_sem=recv,
            device_id=device,
            device_id_type=pl.DeviceIdType.MESH,
        )

    pl.semaphore_wait(barrier, len(plan))
    for step, at, rows in reversed(plan):
        copy = remote(
            source(step, rows), halo.at[pl.ds(at, rows)], send_a.at[0], recv_a.at[0], worker(step)
        )
        unless_mine(step, copy.start)

    for copy in loads[2:]:
        copy.wait()

    pairs = nbr.shape[1]
    centre_total = cen.shape[1]
    slots = pairs // centre_total
    lane = lax.broadcasted_iota(jnp.int32, (centre_total, pairs), 1)
    row = lax.broadcasted_iota(jnp.int32, (centre_total, pairs), 0)
    mine = ((lane >= row * slots) & (lane < (row + 1) * slots)).astype(jnp.float32)
    mine16 = mine.astype(jnp.bfloat16)
    own = CELLS * CELLS

    def site(atom):
        one, two = atom == 1.0, atom == 2.0
        return (
            jnp.where(one, 0.75, 0.25),
            jnp.where(one | two, 0.75, 0.25),
            jnp.where(two, 0.75, 0.25),
        )

    def kind_lane(z, atom):
        turned = jnp.where(z >= CELLS - 2, z - (CELLS - 2), z + 2.0)
        return KIND_AT + 3.0 * turned + atom

    first = cen[...].astype(jnp.float32)
    cell_i = divided(first, 3.0)
    atom_i = first - 3.0 * cell_i
    col_i = divided(cell_i, CELLS)
    z_i = cell_i - CELLS * col_i
    x_i = divided(col_i, CELLS)
    y_i = col_i - CELLS * x_i
    spot_i = [a + b for a, b in zip((x_i, y_i, z_i), site(atom_i))]
    alive_lane = lax.broadcasted_iota(jnp.int32, (1, centre_total), 1)
    count = jnp.where(alive_lane < alive[...], cnt[...], 0).astype(jnp.float32)
    spread = raw(
        jnp.concatenate(
            spot_i + [count, jnp.zeros((4, centre_total), jnp.float32)], axis=0
        ).astype(jnp.bfloat16),
        mine16,
        NN,
    )
    lanef = lax.broadcasted_iota(jnp.int32, (1, pairs), 1).astype(jnp.float32)
    slot_id = lanef - slots * divided(lanef, slots)
    live = jnp.where(slot_id < spread[3:4], 1.0, 0.0).astype(jnp.float32)

    second = nbr[...].astype(jnp.float32)
    ext = CELLS + 4
    cell_j = divided(second, 3.0)
    atom_j = second - 3.0 * cell_j
    col_j = divided(cell_j, ext)
    z_j = cell_j - ext * col_j - 2.0
    x_j = divided(col_j, ext)
    y_j = col_j - ext * x_j - 2.0
    x_j = x_j - 2.0

    def side(v):
        return jnp.where(v < 0.0, -1.0, jnp.where(v >= CELLS, 1.0, 0.0))

    sx, sy, sz = side(x_j), side(y_j), side(z_j)
    x_in, y_in, z_in = x_j - CELLS * sx, y_j - CELLS * sy, z_j - CELLS * sz
    if sizes[2] == 2:
        sz = jnp.abs(sz)
    code = sx * 9.0 + sy * 3.0 + sz
    upper = jnp.where(x_in >= CELLS // 2, 1.0, 0.0)
    across, along = x_in * CELLS + y_in, y_in * CELLS + x_in
    line = jnp.full_like(code, -1.0)
    for (dx, dy, dz), at, rows in plan:
        if dx and dy:
            value = float(at)
        elif dz and dy:
            value = x_in - (CELLS // 2) * upper + float(at)
        elif dz and dx:
            value = y_in + float(at)
        elif dz:
            value = across - HALF * upper + float(at)
        elif dy:
            value = along + float(at - CELLS * origin(dy, 2))
        else:
            value = across + float(at - CELLS * origin(dx, 2))
        line = jnp.where(code == float(dx * 9 + dy * 3 + dz), value, line)
    raised = jnp.where(sz != 0.0, upper, 0.0)
    place_j = 3.0 * z_in + atom_j + (KEPT // 3) * raised
    kind_at_j = kind_lane(z_in, atom_j) + KEPT * raised
    inner = jnp.where(code == 0.0, across, -1.0)

    tail = jnp.full((1, LANES - centre_total), -8.0, jnp.float32)
    column = jnp.concatenate([inner, col_i, tail], axis=1).astype(jnp.int32)
    place = jnp.concatenate(
        [jnp.where(code == 0.0, place_j, -8.0), 3.0 * z_i + atom_i, tail], axis=1
    ).astype(jnp.int32)
    kind_at = jnp.concatenate([kind_at_j, kind_lane(z_i, atom_i), tail], axis=1).astype(jnp.int32)

    def hot(index, length):
        ids = lax.broadcasted_iota(jnp.int32, (length, index.shape[1]), 0)
        return jnp.where(ids == index, 1.0, 0.0).astype(jnp.bfloat16)

    def third(rows, width):
        ids = lax.broadcasted_iota(jnp.int32, (rows, width), 0).astype(jnp.float32)
        group = divided(ids, 3.0)
        return group.astype(jnp.int32), (ids - 3.0 * group).astype(jnp.int32)

    def picked(stack, at, kind_at):
        width = stack.shape[1]
        group, _ = third(96, width)
        _, turn = third(24, width)
        kept = jnp.where(group == at, stack[0:96], 0.0)
        folded = (kept[0:24] + kept[24:48]) + (kept[48:72] + kept[72:96])
        out = [
            jnp.sum(jnp.where(turn == c, folded, 0.0), axis=0, keepdims=True) for c in range(3)
        ]
        ids = lax.broadcasted_iota(jnp.int32, (32, width), 0) + 88
        kind = jnp.sum(jnp.where(ids == kind_at, stack[88:120], 0.0), axis=0, keepdims=True)
        return out, kind

    def placed(at, values):
        width = at.shape[1]
        group, _ = third(96, width)
        _, turn = third(24, width)
        cycle = jnp.where(
            turn == 0, values[0], jnp.where(turn == 1, values[1], values[2])
        )
        out = jnp.where(group == at, jnp.concatenate([cycle] * 4, axis=0), 0.0)
        return jnp.concatenate([out, jnp.zeros((LANES - 96, width), jnp.float32)], axis=0)

    def fetch(block, onehot):
        both = raw(jnp.concatenate(halves(block.T), axis=0), onehot, NN)
        return both[:LANES] + both[LANES:]

    hot_own = hot(column, own)
    shift, kind = picked(fetch(table[...], hot_own), place, kind_at)
    from_centre = mm_exact_b(
        jnp.concatenate(
            [v[:, pairs : pairs + centre_total] for v in shift + [kind]]
            + [jnp.zeros((4, centre_total), jnp.float32)],
            axis=0,
        ),
        mine16,
    )
    spot_j = [a + b for a, b in zip((x_j, y_j, z_j), site(atom_j))]
    mail[...] = jnp.concatenate(
        [
            ((spot_j[c] - spread[c : c + 1]) + (shift[c][:, 0:pairs] - from_centre[c : c + 1]))
            * SIDE
            for c in range(3)
        ]
        + [
            from_centre[3:4] + 2.0 * live,
            jnp.where(code == 0.0, kind[:, 0:pairs], 0.0),
            line,
            place_j,
            kind_at_j,
        ],
        axis=0,
    )
    post = remote(mail, inbox, send_a.at[1], recv_a.at[1], worker((0, 0, 0)))
    post.start()

    two = w_two[...]
    two = jnp.concatenate([two[4:12], two[0:4], jnp.zeros_like(two[0:4])], axis=0)
    out_t = w_out_t[...]
    width = w_lat.shape[0]
    two_3, lat_3, env_3 = thrice(two.T), thrice(w_lat[...].T), thrice(w_env[...].T)
    out_a, out_b = thrice(out_t[:, 0:width]), doubled(out_t[:, width:])
    back_3 = thrice(out_t.T)
    gain = jnp.broadcast_to(readout[...], (8, width)).T[:, 0:1]

    crossing = plan[-1][1] + plan[-1][2] - 1
    halo_rows = halo.shape[0]

    def every(ref, send, recv):
        span = pl.ds(0, crossing)
        return remote(ref.at[span], ref.at[span], send, recv, swapped)

    ids = lax.broadcasted_iota(jnp.int32, (8, LANES), 0)

    def with_mine(block, row_of):
        pieces = block
        corner = [(step, at) for step, at, rows in plan if own_corner(step)]
        base = corner[0][1] // 8 * 8
        tile = block[base : base + 8]
        for step, at in corner:
            tile = jnp.where((ids == at - base) & mine_too(step), row_of(step, at), tile)
        pieces = [block[0:base], tile, block[base + 8 :]]
        return jnp.concatenate([p for p in pieces if p.shape[0]], axis=0)

    arrivals = every(halo, send_a.at[0], recv_a.at[0])
    wide = 2 * LANES
    per = wide // slots
    lines = -(-9 * per // 16) * 16
    member = (
        lax.broadcasted_iota(jnp.int32, (per, wide), 1)
        - slots * lax.broadcasted_iota(jnp.int32, (per, wide), 0)
    )
    member = ((member >= 0) & (member < slots)).astype(jnp.float32)
    unused = jnp.zeros((lines - 9 * per, wide), jnp.float32)
    spot = lax.broadcasted_iota(jnp.int32, (width, 3 * lines), 1)
    term = jnp.where(spot >= 2 * lines, 2, jnp.where(spot >= lines, 1, 0))
    inner_spot = spot - lines * term
    groups = [
        (inner_spot >= a * per) & (inner_spot < b * per) for a, b in ((0, 1), (1, 4), (4, 9))
    ]
    block_row = lax.broadcasted_iota(jnp.int32, (lines, 3 * width), 0)
    block_lane = lax.broadcasted_iota(jnp.int32, (lines, 3 * width), 1)
    blocks = [
        (block_row >= a * per) & (block_row < b * per) & (block_lane >= k * width)
        & (block_lane < (k + 1) * width)
        for k, (a, b) in enumerate(((0, 1), (1, 4), (4, 9)))
    ]
    blocks = blocks[0] | blocks[1] | blocks[2]
    order = (lax.broadcasted_iota(jnp.int32, (NBASIS, wide), 0) + 1).astype(jnp.float32)
    s3, s5, s15 = math.sqrt(3.0), math.sqrt(5.0), math.sqrt(15.0)
    norm = math.sqrt(2.0 / CUTOFF)

    def split(a):
        high = a.astype(jnp.bfloat16).astype(jnp.float32)
        return jnp.where(term == 2, a - high, high)

    post.wait_recv()
    letter = inbox[...]
    hot_j = hot(letter[5:6].astype(jnp.int32), halo_rows)
    there = letter[6:7].astype(jnp.int32)
    arrivals.wait_recv()

    block = with_mine(halo[...], lambda step, at: source(step, 1)[...])
    total_rows = plan[-1][1] + plan[-1][2]
    if total_rows < halo_rows:
        every_id = lax.broadcasted_iota(jnp.int32, (halo_rows, LANES), 0)
        block = jnp.where(every_id < total_rows, block, 0.0)
    block = doubled(block.T)

    def network(at):
        note = letter[:, at : at + wide]
        both = raw(block, hot_j[:, at : at + wide], NN)
        yield
        shift_j, kind_j = picked(
            both[:LANES] + both[LANES:], there[:, at : at + wide], note[7:8].astype(jnp.int32)
        )
        yield
        rx, ry, rz = [note[c : c + 1] + SIDE * shift_j[c] for c in range(3)]
        live = jnp.where(note[3:4] > 1.5, 1.0, 0.0)
        kind_i = note[3:4] - 2.0 * live
        kind_j = note[4:5] + kind_j
        dist = jnp.sqrt(rx * rx + ry * ry + rz * rz)
        inv = 1.0 / dist
        ux, uy, uz = rx * inv, ry * inv, rz * inv
        ratio = dist * (1.0 / CUTOFF)
        r2 = ratio * ratio
        r5 = r2 * r2 * ratio
        inside = ratio < 1.0
        bell = jnp.where(
            inside, 1.0 + r5 * ratio * (-28.0 + ratio * (48.0 - 21.0 * ratio)), 0.0
        )
        slope = jnp.where(
            inside, r5 * (1.0 - ratio) * (1.0 - ratio) * (-168.0 / CUTOFF), 0.0
        )
        turns = order * (dist * (0.5 / CUTOFF))
        sines, cosines = wave(turns), wave(turns + 0.25)
        basis = norm * sines * (inv * bell)
        basis_d = norm * (
            cosines * order * (inv * bell * (math.pi / CUTOFF))
            + sines * (inv * (slope - bell * inv))
        )
        kinds = [1.0 - kind_i, kind_i, 1.0 - kind_j, kind_j]
        inputs = jnp.concatenate(
            [basis] + kinds + [jnp.zeros((4, wide), jnp.float32)], axis=0
        )
        inputs_t = jnp.concatenate([basis_d, jnp.zeros((8, wide), jnp.float32)], axis=0)

        hidden = raw(two_3, stacked(inputs), NN)
        hidden_t = raw(two_3, stacked(inputs_t), NN)
        yield
        hidden, hidden_d = silu_pair(hidden)
        latent = raw(lat_3, stacked(hidden), NN)
        latent_t = raw(lat_3, stacked(hidden_t * hidden_d), NN)
        yield
        latent, latent_d = silu_pair(latent)
        latent_t = latent_t * latent_d
        lat_h, lat_l = halves(latent)
        scale = bell * live
        scale_t = slope * live
        harm = [
            jnp.ones_like(ux),
            s3 * ux,
            s3 * uy,
            s3 * uz,
            s15 * ux * uy,
            s15 * uy * uz,
            0.5 * s5 * (3.0 * uz * uz - 1.0),
            s15 * ux * uz,
            0.5 * s15 * (ux * ux - uy * uy),
        ]
        rows = jnp.concatenate([h * member for h in harm] + [unused], axis=0)
        rows_h, rows_l = halves(rows)
        rows_3 = jnp.concatenate([rows_h, rows_l, rows_h], axis=0)
        scaled_h, scaled_l = [
            jnp.concatenate([v] * 3, axis=0) for v in halves(rows * scale)
        ]
        gathered = by_parts(jnp.concatenate([lat_h, lat_l], axis=0), scaled_h, scaled_l, NT)
        yield
        environ = ENV * raw(env_3, stacked(gathered), NN)
        lat_s = jnp.concatenate([lat_h, lat_l, lat_h], axis=0)
        plain = raw(env_3, lat_s, NN)
        yield
        environ_s = split(environ)
        chosen = jnp.concatenate(
            [jnp.where(g, environ_s, 0.0) for g in groups], axis=0
        ).astype(jnp.bfloat16)
        mixed = raw(chosen, rows_3, NN)
        partly = raw(out_a, lat_s, NN)
        plain_t = raw(env_3, stacked(latent_t), NN)
        weight = plain * scale
        yield
        mixed = [mixed[width * k : width * (k + 1)] for k in range(3)]
        joined_h, joined_l = halves(jnp.concatenate([weight * a for a in mixed], axis=0))
        updated = by_parts(out_b, joined_h, joined_l) + partly
        yield
        weight_t = plain_t * scale + plain * scale_t
        near = jnp.concatenate([jnp.where(g, environ, 0.0)[:, 0:LANES] for g in groups], axis=0)
        near = doubled(near.T[0:lines])
        (weight_h, weight_l), (slant_h, slant_l) = halves(weight), halves(weight_t)
        updated, updated_d = silu_pair(updated)
        d_out = (gain * scale) * updated_d
        back = raw(back_3, stacked(d_out), NN)
        score = jnp.sum(gain * updated, axis=0, keepdims=True)
        pair_energy = score * scale
        yield
        d_mixed = [back[width * (k + 1) : width * (k + 2)] for k in range(3)]
        pass_h, pass_l = halves(jnp.concatenate([q * weight for q in d_mixed], axis=0))
        d_env = by_parts(jnp.concatenate([rows_h, rows_l], axis=0), pass_h, pass_l, NT)
        d_rows = by_parts(near, pass_h, pass_l)
        yield
        along = d_mixed[0] * mixed[0] + d_mixed[1] * mixed[1] + d_mixed[2] * mixed[2]
        d_dist = (
            jnp.sum(along * weight_t + back[0:width] * latent_t, axis=0, keepdims=True)
            + score * scale_t
        )
        d_env = doubled(jnp.where(blocks, ENV * d_env, 0.0))
        d_rows = d_rows + by_parts(
            d_env,
            jnp.concatenate([weight_h] * 3, axis=0),
            jnp.concatenate([weight_l] * 3, axis=0),
        )
        slanted = by_parts(
            d_env,
            jnp.concatenate([slant_h] * 3, axis=0),
            jnp.concatenate([slant_l] * 3, axis=0),
        )
        yield
        d_harm = [
            jnp.sum(d_rows[m * per : (m + 1) * per] * member, axis=0, keepdims=True)
            for m in range(9)
        ]
        d_dist = d_dist + jnp.sum(rows * slanted, axis=0, keepdims=True)
        dux = s3 * d_harm[1] + s15 * (uy * d_harm[4] + uz * d_harm[7] + ux * d_harm[8])
        duy = s3 * d_harm[2] + s15 * (ux * d_harm[4] + uz * d_harm[5] - uy * d_harm[8])
        duz = (
            s3 * d_harm[3]
            + s15 * (uy * d_harm[5] + ux * d_harm[7])
            + 3.0 * s5 * uz * d_harm[6]
        )
        radial = d_dist - (ux * dux + uy * duy + uz * duz) * inv
        yield [d * inv + u * radial for d, u in ((dux, ux), (duy, uy), (duz, uz))] + [
            pair_energy
        ]

    runs = [network(at) for at in range(0, pairs, wide)]
    found = [None] * len(runs)
    while found[0] is None:
        found = [next(run) for run in runs]
    *grad, pair_energy = [jnp.concatenate(v, axis=1) for v in zip(*found)]
    sums = mm_exact_b(
        jnp.concatenate(grad + [pair_energy, jnp.zeros((4, pairs), jnp.float32)], axis=0),
        mine16,
        NT,
    )
    partial = mm_exact_a(hot_j, placed(there, [-g for g in grad]))
    back_mail[0:3, 0:pairs] = jnp.concatenate(grad, axis=0)
    back_mail[:, pairs : pairs + centre_total] = sums[0:4]
    reply = remote(back_mail, back_inbox, send_b.at[1], recv_b.at[1], swapped)
    reply.start()
    part[...] = partial
    for step, at, rows in reversed(plan):
        span = pl.ds(at, rows)
        copy = remote(part.at[span], got.at[span], send_b.at[0], recv_b.at[0], holder(step))
        unless_mine(step, copy.start)

    reply.wait_recv()
    answer = back_inbox[...]
    signs = jnp.where(
        lax.broadcasted_iota(jnp.int32, (1, pairs + LANES), 1) < pairs, -1.0, 1.0
    )
    total[...] = mm_exact_a(
        hot_own, placed(place, [signs * answer[c : c + 1] for c in range(3)])
    )
    result[pl.ds(own, 8), 0:centre_total] = jnp.broadcast_to(
        answer[3:4, pairs : pairs + centre_total], (8, centre_total)
    )
    returns = every(got, send_b.at[0], recv_b.at[0])
    returns.wait_recv()

    def add(spot, value):
        total[spot, :] = total[spot, :] + value

    for (dx, dy, dz), at, rows in plan:
        value = got[pl.ds(at, rows), :]
        x, y = (CELLS - 1) * (dx < 0), (CELLS - 1) * (dy < 0)
        if own_corner((dx, dy, dz)):
            value = jnp.where(mine_too((dx, dy, dz)), part[pl.ds(at, 1), :], value)
            add(pl.ds(CELLS * x + y, 1), value)
        elif dz:
            top = high(value.shape)
            low = jnp.where(top, 0.0, value)
            lifted = pltpu.roll(jnp.where(top, value, 0.0), LANES - KEPT, 1)
            if dx:
                spot = pl.ds(CELLS * x + y, rows)
                add(spot, lifted if dx < 0 else low)
            elif dy:
                add(pl.ds(y, rows, stride=CELLS), low)
                add(pl.ds(HALF + y, rows, stride=CELLS), lifted)
            else:
                add(pl.ds(0, HALF), low)
                add(pl.ds(HALF, HALF), lifted)
        elif dy:
            for t in range(2):
                add(pl.ds(origin(dy, 2) + t, 8, stride=8), value[8 * t : 8 * t + 8])
        else:
            add(pl.ds(CELLS * origin(dx, 2), rows), value)
    for copy in (post, arrivals, reply, returns):
        copy.wait_send()


def unpack_body(result, energy, forces):
    energy[0] = result[pl.ds(CELLS * CELLS, 1), 0 : energy.shape[2]]
    final = jnp.concatenate(
        [result[pl.ds(j, 4, stride=16), :][:, 0:ZROWS] for j in range(16)], axis=1
    )
    wide = 16 * ZROWS
    for q in range(4):
        forces[0, :, wide * q : wide * (q + 1)] = final[q : q + 1, :]


def solution(mesh):
    sizes = tuple(mesh.shape[a] for a in AXES)
    plan, line_total = slot_plan(sizes[2])

    def local(displacement, species, centres, neighbours, neighbour_count, live_centres,
              w_two, w_lat, w_env, w_out, readout):
        pairs = neighbours.shape[2]
        vmem = pl.BlockSpec(memory_space=pltpu.VMEM)
        rows = -(-line_total // 8) * 8
        args = [
            displacement, species, centres, neighbours, neighbour_count, live_centres,
            w_two, w_lat, w_env, w_out.T, readout.reshape(1, -1),
        ]

        def body(*refs):
            kernel_body(sizes, plan, *refs)

        sizes_vmem = [
            (CELLS * CELLS, LANES), (4 * CELLS, LANES), (HALF, LANES), (CELLS, LANES),
            (8, pairs), (8, pairs), (4, pairs + LANES), (4, pairs + LANES),
            (rows, LANES), (rows, LANES), (rows, LANES),
        ]
        result = pl.pallas_call(
            body,
            out_shape=pltpu.VMEM((CELLS * CELLS + 8, LANES), jnp.float32),
            in_specs=[pl.BlockSpec(memory_space=pltpu.HBM)] * len(args),
            out_specs=vmem,
            scratch_shapes=[pltpu.VMEM(x.shape, x.dtype) for x in args]
            + [pltpu.VMEM(shape, jnp.float32) for shape in sizes_vmem]
            + [pltpu.SemaphoreType.DMA((2,))] * 4
            + [pltpu.SemaphoreType.DMA((len(args),))],
            compiler_params=pltpu.CompilerParams(collective_id=0, has_side_effects=True),
        )(*args)
        result = pltpu.with_memory_space_constraint(result, pltpu.VMEM)
        return pl.pallas_call(
            unpack_body,
            out_shape=(
                jax.ShapeDtypeStruct(centres.shape, jnp.float32),
                jax.ShapeDtypeStruct(displacement.shape, jnp.float32),
            ),
            in_specs=[vmem],
            out_specs=(vmem, vmem),
        )(result)

    split = P(*AXES)
    return jax.shard_map(
        local,
        mesh=mesh,
        in_specs=(split,) * 6 + (P(),) * 5,
        out_specs=(split, split),
        check_vma=False,
    )
```

```python
import math

import jax
import jax.numpy as jnp
from jax import lax
from jax.experimental import pallas as pl
from jax.experimental.pallas import tpu as pltpu
from jax.sharding import PartitionSpec as P

CELLS = 8
NBASIS = 8
CUTOFF = 6.0
SIDE = 3.1
ENV = 0.2
LANES = 128
ZROWS = CELLS * 9
KINDS = CELLS * 3
KEPT = 18
KIND_AT = ZROWS + KEPT
HALF = CELLS * CELLS // 2
AXES = ("gx", "gy", "gz")

NN = (((1,), (0,)), ((), ()))
NT = (((1,), (1,)), ((), ()))


def halves(x):
    hi = x.astype(jnp.bfloat16)
    lo = (x - hi.astype(jnp.float32)).astype(jnp.bfloat16)
    return hi, lo


def raw(a, b, dims):
    return lax.dot_general(a, b, dims, preferred_element_type=jnp.float32)


def thrice(a):
    high, low = halves(a)
    return jnp.concatenate([high, high, low], axis=1)


def stacked(b):
    high, low = halves(b)
    return jnp.concatenate([high, low, high], axis=0)


def doubled(b):
    return jnp.concatenate(halves(b), axis=0)


def by_parts(a, bh, bl, dims=NN):
    n = a.shape[0] // 2
    both = raw(a, bh, dims)
    return both[:n] + (both[n:] + raw(a[:n], bl, dims))


def mm_exact_b(a, b, dims=NN):
    ah, al = halves(a)
    return raw(ah, b, dims) + raw(al, b, dims)


def mm_exact_a(a, b):
    n = b.shape[0]
    both = raw(a, jnp.concatenate(halves(b), axis=0), NT)
    return both[:, :n] + both[:, n:]


def slot_plan(depth):
    sides = [1] if depth == 2 else [1, -1]
    ends = (-1, 1)
    groups = [
        [((0, 0, dz), HALF) for dz in sides],
        [((dx, 0, 0), 2 * CELLS) for dx in ends],
        [((0, dy, 0), 2 * CELLS) for dy in ends],
        [((dx, 0, dz), CELLS) for dz in sides for dx in ends],
        [((0, dy, dz), CELLS // 2) for dz in sides for dy in ends],
        [((dx, dy, 0), 1) for dx in ends for dy in ends],
        [((dx, dy, dz), 1) for dz in sides for dx in ends for dy in ends],
    ]
    plan, at = [], 0
    for step, rows in [entry for group in groups for entry in group]:
        plan.append((step, at, rows))
        at += rows
    return plan, at


def origin(step, tiles):
    return 0 if step >= 0 else CELLS - tiles


def by_reach(plan):
    def rank(entry):
        (dx, dy, dz), _, rows = entry
        return dy == 0, dy < 0, rows > CELLS, dz, rows

    return sorted(plan, key=rank)


def own_corner(step):
    return step[2] == 0 and step[0] != 0 and step[1] != 0


def wave(turns):
    f = turns - jnp.floor(turns + 0.5)
    f = jnp.where(f > 0.25, 0.5 - f, jnp.where(f < -0.25, -0.5 - f, f))
    x = f * (2.0 * math.pi)
    s = x * x
    p = -1.0 / 39916800.0
    for c in (1.0 / 362880.0, -1.0 / 5040.0, 1.0 / 120.0, -1.0 / 6.0):
        p = p * s + c
    return x + x * s * p


def divided(value, by):
    return jnp.floor((value + 0.5) * (1.0 / by))


def silu_pair(x):
    s = 0.5 + 0.5 * jnp.tanh(0.5 * x)
    return x * s, s * (1.0 + x * (1.0 - s))


def kernel_body(sizes, plan, disp_hbm, spec_hbm, cen_hbm, nbr_hbm, cnt_hbm, alive_hbm, two_hbm,
                lat_hbm, env_hbm, out_hbm, readout_hbm, result,
                disp, spec, cen, nbr, cnt, alive, w_two, w_lat, w_env, w_out_t, readout,
                table, pack, ztable, zpack, note, inbox, mail, mail_in, back_mail, back_inbox, halo, part, got,
                send_a, recv_a, send_b, recv_b, load):
    loads = [
        pltpu.make_async_copy(src, dst, load.at[at])
        for at, (src, dst) in enumerate(
            (
                (disp_hbm, disp),
                (spec_hbm, spec),
                (cen_hbm, cen),
                (nbr_hbm, nbr),
                (cnt_hbm, cnt),
                (alive_hbm, alive),
                (two_hbm, w_two),
                (lat_hbm, w_lat),
                (env_hbm, w_env),
                (out_hbm, w_out_t),
                (readout_hbm, readout),
            )
        )
    ]
    for copy in loads:
        copy.start()
    disp, spec, cen, nbr, cnt, alive = (
        ref.at[0] for ref in (disp, spec, cen, nbr, cnt, alive)
    )
    total = result.at[pl.ds(0, CELLS * CELLS)]
    me = tuple(lax.axis_index(a) for a in AXES)
    odd = [lax.rem(i, 2) for i in me[:2]]
    swapped = tuple(i + 1 - 2 * o for i, o in zip(me, odd)) + me[2:]

    def moved(place, step, sign):
        return tuple(
            lax.rem(i + (sign * d + n), n) if d else i for i, d, n in zip(place, step, sizes)
        )

    def holder(step):
        return moved(swapped, step, 1)

    def worker(step):
        x, y, z = moved(me, step, -1)
        return x + 1 - 2 * lax.rem(x, 2), y + 1 - 2 * lax.rem(y, 2), z

    def mine_too(step):
        return (odd[0] == (1 if step[0] > 0 else 0)) & (odd[1] == (1 if step[1] > 0 else 0))

    barrier = pltpu.get_barrier_semaphore()

    def greet(device):
        pl.semaphore_signal(
            barrier, inc=1, device_id=device, device_id_type=pl.DeviceIdType.MESH
        )

    def unless_mine(step, action):
        if own_corner(step):
            pl.when(jnp.logical_not(mine_too(step)))(action)
        else:
            action()

    for step, at, rows in by_reach(plan):
        unless_mine(step, lambda step=step: greet(holder(step)))
    greet(swapped)

    for copy in loads[:6]:
        copy.wait()
    dwide, swide = 16 * ZROWS, 16 * KINDS
    dline = jnp.concatenate([disp[:, dwide * q : dwide * (q + 1)] for q in range(4)], axis=0)
    sline = jnp.concatenate([spec[:, swide * q : swide * (q + 1)] for q in range(4)], axis=0)
    sline = sline.astype(jnp.float32)
    gap = jnp.zeros((4, KEPT), jnp.float32)
    blank = jnp.zeros((4, LANES - KIND_AT - KINDS), jnp.float32)
    for j in range(16):
        kinds = sline[:, KINDS * j : KINDS * (j + 1)]
        table[pl.ds(j, 4, stride=16), :] = jnp.concatenate(
            [
                dline[:, ZROWS * j : ZROWS * (j + 1)],
                gap,
                kinds[:, KINDS - 6 : KINDS],
                kinds[:, 0 : KINDS - 6],
                blank,
            ],
            axis=1,
        )
    lane_row = lax.broadcasted_iota(jnp.int32, (1, LANES), 1)

    def high(shape):
        ids = lax.broadcasted_iota(jnp.int32, shape, 1)
        return (
            ((ids >= KEPT) & (ids < 2 * KEPT))
            | ((ids >= ZROWS) & (ids < KIND_AT))
            | ((ids >= KIND_AT + KEPT) & (ids < KIND_AT + KEPT + 12))
        )

    ztable[...] = jnp.where(
        high((HALF, LANES)),
        pltpu.roll(table[pl.ds(HALF, HALF), :], KEPT, 1),
        table[pl.ds(0, HALF), :],
    )
    for t, y in enumerate((0, 1, CELLS - 2, CELLS - 1)):
        pack[pl.ds(8 * t, 8), :] = table[pl.ds(y, 8, stride=8), :]
    for t, y in enumerate((0, CELLS - 1)):
        zpack[pl.ds(4 * t, 4), :] = ztable[pl.ds(y, 4, stride=8), :]

    def source(step, rows):
        dx, dy, dz = step
        if dx and dy:
            if dz:
                return ztable.at[pl.ds((HALF - CELLS) * (dx < 0) + (CELLS - 1) * (dy < 0), 1)]
            return table.at[pl.ds(CELLS * (CELLS - 1) * (dx < 0) + (CELLS - 1) * (dy < 0), 1)]
        if dy:
            return (zpack if dz else pack).at[pl.ds(0 if dy > 0 else rows, rows)]
        if dz:
            return ztable.at[pl.ds(HALF - rows if dx < 0 else 0, rows)]
        return table.at[pl.ds(CELLS * origin(dx, 2), rows)]

    def remote(src, dst, send, recv, device):
        return pltpu.make_async_remote_copy(
            src_ref=src,
            dst_ref=dst,
            send_sem=send,
            recv_sem=recv,
            device_id=device,
            device_id_type=pl.DeviceIdType.MESH,
        )


    pairs = nbr.shape[1]
    centre_total = cen.shape[1]
    slots = pairs // centre_total
    lane = lax.broadcasted_iota(jnp.int32, (centre_total, pairs), 1)
    row = lax.broadcasted_iota(jnp.int32, (centre_total, pairs), 0)
    mine = ((lane >= row * slots) & (lane < (row + 1) * slots)).astype(jnp.float32)
    mine16 = mine.astype(jnp.bfloat16)
    own = CELLS * CELLS

    def site(atom):
        one, two = atom == 1.0, atom == 2.0
        return (
            jnp.where(one, 0.75, 0.25),
            jnp.where(one | two, 0.75, 0.25),
            jnp.where(two, 0.75, 0.25),
        )

    def kind_lane(z, atom):
        turned = jnp.where(z >= CELLS - 2, z - (CELLS - 2), z + 2.0)
        return KIND_AT + 3.0 * turned + atom

    first = cen[...].astype(jnp.float32)
    cell_i = divided(first, 3.0)
    atom_i = first - 3.0 * cell_i
    col_i = divided(cell_i, CELLS)
    z_i = cell_i - CELLS * col_i
    x_i = divided(col_i, CELLS)
    y_i = col_i - CELLS * x_i
    spot_i = [a + b for a, b in zip((x_i, y_i, z_i), site(atom_i))]
    alive_lane = lax.broadcasted_iota(jnp.int32, (1, centre_total), 1)
    count = jnp.where(alive_lane < alive[...], cnt[...], 0).astype(jnp.float32)
    spread = raw(
        jnp.concatenate(
            spot_i + [count, col_i, 3.0 * z_i + atom_i, kind_lane(z_i, atom_i)]
            + [jnp.zeros((1, centre_total), jnp.float32)],
            axis=0,
        ).astype(jnp.bfloat16),
        mine16,
        NN,
    )
    lanef = lax.broadcasted_iota(jnp.int32, (1, pairs), 1).astype(jnp.float32)
    slot_id = lanef - slots * divided(lanef, slots)
    live = jnp.where(slot_id < spread[3:4], 1.0, 0.0).astype(jnp.float32)

    second = nbr[...].astype(jnp.float32)
    ext = CELLS + 4
    cell_j = divided(second, 3.0)
    atom_j = second - 3.0 * cell_j
    col_j = divided(cell_j, ext)
    z_j = cell_j - ext * col_j - 2.0
    x_j = divided(col_j, ext)
    y_j = col_j - ext * x_j - 2.0
    x_j = x_j - 2.0

    def side(v):
        return jnp.where(v < 0.0, -1.0, jnp.where(v >= CELLS, 1.0, 0.0))

    sx, sy, sz = side(x_j), side(y_j), side(z_j)
    x_in, y_in, z_in = x_j - CELLS * sx, y_j - CELLS * sy, z_j - CELLS * sz
    if sizes[2] == 2:
        sz = jnp.abs(sz)
    code = sx * 9.0 + sy * 3.0 + sz
    upper = jnp.where(x_in >= CELLS // 2, 1.0, 0.0)
    across, along = x_in * CELLS + y_in, y_in * CELLS + x_in
    line = jnp.full_like(code, -1.0)
    for (dx, dy, dz), at, rows in plan:
        if dx and dy:
            value = float(at)
        elif dz and dy:
            value = x_in - (CELLS // 2) * upper + float(at)
        elif dz and dx:
            value = y_in + float(at)
        elif dz:
            value = across - HALF * upper + float(at)
        elif dy:
            value = along + float(at - CELLS * origin(dy, 2))
        else:
            value = across + float(at - CELLS * origin(dx, 2))
        line = jnp.where(code == float(dx * 9 + dy * 3 + dz), value, line)
    raised = jnp.where(sz != 0.0, upper, 0.0)
    place_j = 3.0 * z_in + atom_j + (KEPT // 3) * raised
    kind_at_j = kind_lane(z_in, atom_j) + KEPT * raised
    inner = jnp.where(code == 0.0, across, -1.0)

    place = jnp.concatenate(
        [jnp.where(code == 0.0, place_j, -8.0), spread[5:6]], axis=1
    ).astype(jnp.int32)
    kind_at = jnp.concatenate([kind_at_j, spread[6:7]], axis=1).astype(jnp.int32)
    column = jnp.concatenate([inner, spread[4:5]], axis=1).astype(jnp.int32)

    def hot(index, length):
        ids = lax.broadcasted_iota(jnp.int32, (length, index.shape[1]), 0)
        return jnp.where(ids == index, 1.0, 0.0).astype(jnp.bfloat16)

    def third(rows, width):
        ids = lax.broadcasted_iota(jnp.int32, (rows, width), 0).astype(jnp.float32)
        group = divided(ids, 3.0)
        return group.astype(jnp.int32), (ids - 3.0 * group).astype(jnp.int32)

    def picked(stack, at, kind_at):
        width = stack.shape[1]
        group, _ = third(96, width)
        _, turn = third(24, width)
        kept = jnp.where(group == at, stack[0:96], 0.0)
        folded = (kept[0:24] + kept[24:48]) + (kept[48:72] + kept[72:96])
        out = [
            jnp.sum(jnp.where(turn == c, folded, 0.0), axis=0, keepdims=True) for c in range(3)
        ]
        ids = lax.broadcasted_iota(jnp.int32, (32, width), 0) + 88
        kind = jnp.sum(jnp.where(ids == kind_at, stack[88:120], 0.0), axis=0, keepdims=True)
        return out, kind

    def placed(at, values):
        width = at.shape[1]
        group, _ = third(96, width)
        _, turn = third(24, width)
        cycle = jnp.where(
            turn == 0, values[0], jnp.where(turn == 1, values[1], values[2])
        )
        out = jnp.where(group == at, jnp.concatenate([cycle] * 4, axis=0), 0.0)
        return jnp.concatenate([out, jnp.zeros((LANES - 96, width), jnp.float32)], axis=0)

    def fetch(block, onehot):
        return raw(
            jnp.concatenate(halves(block.T), axis=1),
            jnp.concatenate([onehot, onehot], axis=0),
            NN,
        )

    hot_own = hot(column, own)
    note[...] = jnp.concatenate([line, place_j, kind_at_j, live], axis=0)
    spot_j = [a + b for a, b in zip((x_j, y_j, z_j), site(atom_j))]
    apart = [spot_j[c] - spread[c : c + 1] for c in range(3)]

    pl.semaphore_wait(barrier, len(plan))
    post = None
    for step, at, rows in by_reach(plan):
        if step[1] == 0 and post is None:
            post = remote(note, inbox, send_a.at[1], recv_a.at[1], worker((0, 0, 0)))
            post.start()
        copy = remote(
            source(step, rows), halo.at[pl.ds(at, rows)], send_a.at[0], recv_a.at[0], worker(step)
        )
        unless_mine(step, copy.start)


    shift, kind = picked(fetch(table[...], hot_own), place, kind_at)
    mail[...] = jnp.concatenate(
        [(apart[c] + (shift[c][:, 0:pairs] - shift[c][:, pairs:])) * SIDE for c in range(3)]
        + [kind[:, pairs:] + 2.0 * jnp.where(code == 0.0, kind[:, 0:pairs], 0.0)],
        axis=0,
    )
    parcel = remote(mail, mail_in, send_a.at[2], recv_a.at[2], worker((0, 0, 0)))
    parcel.start()

    for copy in loads[6:]:
        copy.wait()
    two = w_two[...]
    two = jnp.concatenate([two[4:12], two[0:4], jnp.zeros_like(two[0:4])], axis=0)
    out_t = w_out_t[...]
    width = w_lat.shape[0]
    two_3, lat_3, env_3 = thrice(two.T), thrice(w_lat[...].T), thrice(w_env[...].T)
    out_a, out_b = thrice(out_t[:, 0:width]), doubled(out_t[:, width:])
    back_3 = thrice(out_t.T)
    gain = jnp.broadcast_to(readout[...], (8, width)).T[:, 0:1]

    crossing = plan[-1][1] + plan[-1][2] - 1
    halo_rows = halo.shape[0]

    def every(ref, send, recv):
        span = pl.ds(0, crossing)
        return remote(ref.at[span], ref.at[span], send, recv, swapped)

    ids = lax.broadcasted_iota(jnp.int32, (8, LANES), 0)

    def with_mine(block, row_of):
        corner = [(step, at) for step, at, rows in plan if own_corner(step)]
        base = corner[0][1] // 8 * 8
        tile = block[base : base + 8]
        for step, at in corner:
            tile = jnp.where((ids == at - base) & mine_too(step), row_of(step, at), tile)
        pieces = [block[0:base]] if base else []
        pieces.append(tile)
        if base + 8 < block.shape[0]:
            pieces.append(block[base + 8 :])
        return jnp.concatenate(pieces, axis=0)

    arrivals = every(halo, send_a.at[0], recv_a.at[0])
    wide = 2 * LANES
    per = wide // slots
    lines = -(-9 * per // 16) * 16
    member = (
        lax.broadcasted_iota(jnp.int32, (per, wide), 1)
        - slots * lax.broadcasted_iota(jnp.int32, (per, wide), 0)
    )
    member = ((member >= 0) & (member < slots)).astype(jnp.float32)
    unused = jnp.zeros((lines - 9 * per, wide), jnp.float32)
    spot = lax.broadcasted_iota(jnp.int32, (width, 3 * lines), 1)
    term = jnp.where(spot >= 2 * lines, 2, jnp.where(spot >= lines, 1, 0))
    inner_spot = spot - lines * term
    groups = [
        (inner_spot >= a * per) & (inner_spot < b * per) for a, b in ((0, 1), (1, 4), (4, 9))
    ]
    block_row = lax.broadcasted_iota(jnp.int32, (lines, 3 * width), 0)
    block_lane = lax.broadcasted_iota(jnp.int32, (lines, 3 * width), 1)
    blocks = [
        (block_row >= a * per) & (block_row < b * per) & (block_lane >= k * width)
        & (block_lane < (k + 1) * width)
        for k, (a, b) in enumerate(((0, 1), (1, 4), (4, 9)))
    ]
    blocks = blocks[0] | blocks[1] | blocks[2]
    order = (lax.broadcasted_iota(jnp.int32, (NBASIS, wide), 0) + 1).astype(jnp.float32)
    s3, s5, s15 = math.sqrt(3.0), math.sqrt(5.0), math.sqrt(15.0)
    norm = math.sqrt(2.0 / CUTOFF)

    def split(a):
        high = a.astype(jnp.bfloat16).astype(jnp.float32)
        return jnp.where(term == 2, a - high, high)

    post.wait_recv()
    letter = inbox[...]
    hot_j = hot(letter[0:1].astype(jnp.int32), halo_rows)
    twice_j = jnp.concatenate([hot_j, hot_j], axis=0)
    there = letter[1:2].astype(jnp.int32)
    kind_there = letter[2:3].astype(jnp.int32)
    arrivals.wait_recv()

    block = with_mine(halo[...], lambda step, at: source(step, 1)[...])
    total_rows = plan[-1][1] + plan[-1][2]
    if total_rows < halo_rows:
        every_id = lax.broadcasted_iota(jnp.int32, (halo_rows, LANES), 0)
        block = jnp.where(every_id < total_rows, block, 0.0)

    block = jnp.concatenate([v.T for v in halves(block)], axis=1)

    stacks = [raw(block, twice_j[:, at : at + wide], NN) for at in range(0, pairs, wide)]
    parcel.wait_recv()
    sheet = mail_in[...]

    def network(at):
        span = slice(at, at + wide)
        shift_j, kind_j = picked(stacks[at // wide], there[:, span], kind_there[:, span])
        yield
        rx, ry, rz = [sheet[c : c + 1, span] + SIDE * shift_j[c] for c in range(3)]
        live = letter[3:4, span]
        own_j = jnp.where(sheet[3:4, span] > 1.5, 1.0, 0.0)
        kind_i = sheet[3:4, span] - 2.0 * own_j
        kind_j = own_j + kind_j
        square = rx * rx + ry * ry + rz * rz
        inv = lax.rsqrt(square)
        dist = square * inv
        ux, uy, uz = rx * inv, ry * inv, rz * inv
        ratio = dist * (1.0 / CUTOFF)
        r2 = ratio * ratio
        r5 = r2 * r2 * ratio
        inside = ratio < 1.0
        bell = jnp.where(
            inside, 1.0 + r5 * ratio * (-28.0 + ratio * (48.0 - 21.0 * ratio)), 0.0
        )
        slope = jnp.where(
            inside, r5 * (1.0 - ratio) * (1.0 - ratio) * (-168.0 / CUTOFF), 0.0
        )
        turns = order * (dist * (0.5 / CUTOFF))
        sines, cosines = wave(turns), wave(turns + 0.25)
        basis = norm * sines * (inv * bell)
        basis_d = norm * (
            cosines * order * (inv * bell * (math.pi / CUTOFF))
            + sines * (inv * (slope - bell * inv))
        )
        kinds = [1.0 - kind_i, kind_i, 1.0 - kind_j, kind_j]
        inputs = jnp.concatenate(
            [basis] + kinds + [jnp.zeros((4, wide), jnp.float32)], axis=0
        )
        inputs_t = jnp.concatenate([basis_d, jnp.zeros((8, wide), jnp.float32)], axis=0)

        hidden = raw(two_3, stacked(inputs), NN)
        hidden_t = raw(two_3, stacked(inputs_t), NN)
        yield
        hidden, hidden_d = silu_pair(hidden)
        latent = raw(lat_3, stacked(hidden), NN)
        latent_t = raw(lat_3, stacked(hidden_t * hidden_d), NN)
        yield
        latent, latent_d = silu_pair(latent)
        latent_t = latent_t * latent_d
        lat_h, lat_l = halves(latent)
        scale = bell * live
        scale_t = slope * live
        harm = [
            jnp.ones_like(ux),
            s3 * ux,
            s3 * uy,
            s3 * uz,
            s15 * ux * uy,
            s15 * uy * uz,
            0.5 * s5 * (3.0 * uz * uz - 1.0),
            s15 * ux * uz,
            0.5 * s15 * (ux * ux - uy * uy),
        ]
        rows = jnp.concatenate([h * member for h in harm] + [unused], axis=0)
        rows_h, rows_l = halves(rows)
        rows_3 = jnp.concatenate([rows_h, rows_l, rows_h], axis=0)
        scaled_h, scaled_l = [
            jnp.concatenate([v] * 3, axis=0) for v in halves(rows * scale)
        ]
        gathered = by_parts(jnp.concatenate([lat_h, lat_l], axis=0), scaled_h, scaled_l, NT)
        yield
        environ = ENV * raw(env_3, stacked(gathered), NN)
        lat_s = jnp.concatenate([lat_h, lat_l, lat_h], axis=0)
        plain = raw(env_3, lat_s, NN)
        yield
        environ_s = split(environ)
        chosen = jnp.concatenate(
            [jnp.where(g, environ_s, 0.0) for g in groups], axis=0
        ).astype(jnp.bfloat16)
        mixed = raw(chosen, rows_3, NN)
        partly = raw(out_a, lat_s, NN)
        plain_t = raw(env_3, stacked(latent_t), NN)
        weight = plain * scale
        yield
        mixed = [mixed[width * k : width * (k + 1)] for k in range(3)]
        joined_h, joined_l = halves(jnp.concatenate([weight * a for a in mixed], axis=0))
        updated = by_parts(out_b, joined_h, joined_l) + partly
        yield
        weight_t = plain_t * scale + plain * scale_t
        near = jnp.concatenate([jnp.where(g, environ, 0.0)[:, 0:LANES] for g in groups], axis=0)
        near = doubled(near.T[0:lines])
        weight_s, slant_s = stacked(weight), stacked(weight_t)
        updated, updated_d = silu_pair(updated)
        d_out = (gain * scale) * updated_d
        back = raw(back_3, stacked(d_out), NN)
        score = jnp.sum(gain * updated, axis=0, keepdims=True)
        pair_energy = score * scale
        yield
        d_mixed = [back[width * (k + 1) : width * (k + 2)] for k in range(3)]
        pass_h, pass_l = halves(jnp.concatenate([q * weight for q in d_mixed], axis=0))
        d_env = by_parts(jnp.concatenate([rows_h, rows_l], axis=0), pass_h, pass_l, NT)
        d_rows = by_parts(near, pass_h, pass_l)
        yield
        along = d_mixed[0] * mixed[0] + d_mixed[1] * mixed[1] + d_mixed[2] * mixed[2]
        d_dist = (
            jnp.sum(along * weight_t + back[0:width] * latent_t, axis=0, keepdims=True)
            + score * scale_t
        )
        d_env = jnp.where(blocks, ENV * d_env, 0.0)
        d_env = jnp.concatenate([d_env, jnp.zeros((lines, width), jnp.float32)], axis=1)
        d_env = d_env[:, 0:LANES] + d_env[:, LANES:]
        d_env_h, d_env_l = halves(d_env + pltpu.roll(d_env, width, 1))
        d_env = jnp.concatenate([d_env_h, d_env_l[:, 0:width]], axis=1)
        d_rows = d_rows + raw(d_env, weight_s, NN)
        slanted = raw(d_env, slant_s, NN)
        yield
        turned = [d_rows[m * per : (m + 1) * per] for m in range(9)]
        dux = s3 * turned[1] + s15 * (uy * turned[4] + uz * turned[7] + ux * turned[8])
        duy = s3 * turned[2] + s15 * (ux * turned[4] + uz * turned[5] - uy * turned[8])
        duz = (
            s3 * turned[3]
            + s15 * (uy * turned[5] + ux * turned[7])
            + 3.0 * s5 * uz * turned[6]
        )
        dux, duy, duz = [
            jnp.sum(d * member, axis=0, keepdims=True) for d in (dux, duy, duz)
        ]
        d_dist = d_dist + jnp.sum(rows * slanted, axis=0, keepdims=True)
        radial = d_dist - (ux * dux + uy * duy + uz * duz) * inv
        yield [d * inv + u * radial for d, u in ((dux, ux), (duy, uy), (duz, uz))] + [
            pair_energy
        ]

    runs = [network(at) for at in range(0, pairs, wide)]
    found = [None] * len(runs)
    while found[0] is None:
        found = [next(run) for run in runs]
    *grad, pair_energy = [jnp.concatenate(v, axis=1) for v in zip(*found)]
    back_mail[...] = jnp.concatenate(grad + [pair_energy], axis=0)
    reply = remote(back_mail, back_inbox, send_b.at[1], recv_b.at[1], swapped)
    reply.start()
    partial = mm_exact_a(hot_j, placed(there, [-g for g in grad]))
    part[...] = partial
    for step, at, rows in by_reach(plan):
        span = pl.ds(at, rows)
        copy = remote(part.at[span], got.at[span], send_b.at[0], recv_b.at[0], holder(step))
        unless_mine(step, copy.start)

    reply.wait_recv()
    answer = back_inbox[...]
    moves = [answer[c : c + 1] for c in range(3)]
    settled = mm_exact_a(
        hot_own,
        jnp.concatenate(
            [placed(place[:, 0:pairs], [-m for m in moves]), placed(place[:, pairs:], moves)],
            axis=1,
        ),
    )
    energies = mm_exact_b(jnp.broadcast_to(answer[3:4], (8, pairs)), mine16, NT)
    result[pl.ds(own, 8), 0:centre_total] = energies
    below = lax.broadcasted_iota(jnp.int32, (CELLS, LANES), 0)
    upper_lanes = high((CELLS, LANES))
    returns = every(got, send_b.at[0], recv_b.at[0])
    returns.wait_recv()

    slabs = [settled[CELLS * x : CELLS * (x + 1)] for x in range(CELLS)]
    columns = {y: [[] for x in range(CELLS)] for y in (0, 1, CELLS - 2, CELLS - 1)}

    def low_part(value):
        return jnp.where(upper_lanes[0 : value.shape[0]], 0.0, value)

    def high_part(value):
        kept = jnp.where(upper_lanes[0 : value.shape[0]], value, 0.0)
        return pltpu.roll(kept, LANES - KEPT, 1)

    for (dx, dy, dz), at, rows in plan:
        x, y = (CELLS - 1) * (dx < 0), (CELLS - 1) * (dy < 0)
        if own_corner((dx, dy, dz)):
            value = jnp.where(
                mine_too((dx, dy, dz)), part[pl.ds(at, 1), :], got[pl.ds(at, 1), :]
            )
            columns[y][x].append(value)
        elif dx and dy:
            value = got[pl.ds(at, 1), :]
            columns[y][x].append(high_part(value) if dx < 0 else low_part(value))
        elif dz and dy:
            value = got[pl.ds(at, rows), :]
            for part_of, base in ((low_part(value), 0), (high_part(value), rows)):
                for r in range(rows):
                    columns[y][base + r].append(part_of[r : r + 1])
        elif dz and dx:
            value = got[pl.ds(at, rows), :]
            slabs[x] = slabs[x] + (high_part(value) if dx < 0 else low_part(value))
        elif dz:
            for r in range(CELLS // 2):
                value = got[pl.ds(at + CELLS * r, CELLS), :]
                slabs[r] = slabs[r] + low_part(value)
                slabs[CELLS // 2 + r] = slabs[CELLS // 2 + r] + high_part(value)
        elif dy:
            for t in range(2):
                for r in range(CELLS):
                    columns[origin(dy, 2) + t][r].append(got[pl.ds(at + 8 * t + r, 1), :])
        else:
            for t in range(2):
                x = origin(dx, 2) + t
                slabs[x] = slabs[x] + got[pl.ds(at + CELLS * t, CELLS), :]
    for x in range(CELLS):
        side = jnp.zeros((CELLS, LANES), jnp.float32)
        for y, lists in columns.items():
            value = sum(lists[x][1:], lists[x][0])
            side = jnp.where(below == y, value, side)
        total[pl.ds(CELLS * x, CELLS), :] = slabs[x] + side
    for copy in (post, parcel, arrivals, reply, returns):
        copy.wait_send()


def unpack_body(result, energy, forces):
    energy[0] = result[pl.ds(CELLS * CELLS, 1), 0 : energy.shape[2]]
    final = jnp.concatenate(
        [result[pl.ds(j, 4, stride=16), :][:, 0:ZROWS] for j in range(16)], axis=1
    )
    wide = 16 * ZROWS
    for q in range(4):
        forces[0, :, wide * q : wide * (q + 1)] = final[q : q + 1, :]


def solution(mesh):
    sizes = tuple(mesh.shape[a] for a in AXES)
    plan, line_total = slot_plan(sizes[2])

    def local(displacement, species, centres, neighbours, neighbour_count, live_centres,
              w_two, w_lat, w_env, w_out, readout):
        pairs = neighbours.shape[2]
        vmem = pl.BlockSpec(memory_space=pltpu.VMEM)
        rows = -(-line_total // 8) * 8
        args = [
            displacement, species, centres, neighbours, neighbour_count, live_centres,
            w_two, w_lat, w_env, w_out.T, readout.reshape(1, -1),
        ]

        def body(*refs):
            pl.run_scoped(
                lambda load: kernel_body(sizes, plan, *refs, load),
                pltpu.SemaphoreType.DMA((len(args),)),
            )

        sizes_vmem = [
            (CELLS * CELLS, LANES), (4 * CELLS, LANES), (HALF, LANES), (CELLS, LANES),
            (4, pairs), (4, pairs), (4, pairs), (4, pairs), (4, pairs), (4, pairs),
            (rows, LANES), (rows, LANES), (rows, LANES),
        ]
        result = pl.pallas_call(
            body,
            out_shape=pltpu.VMEM((CELLS * CELLS + 8, LANES), jnp.float32),
            in_specs=[pl.BlockSpec(memory_space=pltpu.HBM)] * len(args),
            out_specs=vmem,
            scratch_shapes=[pltpu.VMEM(x.shape, x.dtype) for x in args]
            + [pltpu.VMEM(shape, jnp.float32) for shape in sizes_vmem]
            + [pltpu.SemaphoreType.DMA((3,))] * 2
            + [pltpu.SemaphoreType.DMA((2,))] * 2,
            compiler_params=pltpu.CompilerParams(collective_id=0, has_side_effects=True),
        )(*args)
        result = pltpu.with_memory_space_constraint(result, pltpu.VMEM)
        return pl.pallas_call(
            unpack_body,
            out_shape=(
                jax.ShapeDtypeStruct(centres.shape, jnp.float32),
                jax.ShapeDtypeStruct(displacement.shape, jnp.float32),
            ),
            in_specs=[vmem],
            out_specs=(vmem, vmem),
        )(result)

    split = P(*AXES)
    return jax.shard_map(
        local,
        mesh=mesh,
        in_specs=(split,) * 6 + (P(),) * 5,
        out_specs=(split, split),
        check_vma=False,
    )
```

```python
import math

import jax
import jax.numpy as jnp
from jax import lax
from jax.experimental import pallas as pl
from jax.experimental.pallas import tpu as pltpu
from jax.sharding import PartitionSpec as P

CELLS = 8
NBASIS = 8
CUTOFF = 6.0
SIDE = 3.1
ENV = 0.2
LANES = 128
ZROWS = CELLS * 9
KINDS = CELLS * 3
KEPT = 18
KIND_AT = ZROWS + KEPT
HALF = CELLS * CELLS // 2
AXES = ("gx", "gy", "gz")

NN = (((1,), (0,)), ((), ()))
NT = (((1,), (1,)), ((), ()))


def halves(x):
    hi = x.astype(jnp.bfloat16)
    lo = (x - hi.astype(jnp.float32)).astype(jnp.bfloat16)
    return hi, lo


def raw(a, b, dims):
    return lax.dot_general(a, b, dims, preferred_element_type=jnp.float32)


def thrice(a):
    high, low = halves(a)
    return jnp.concatenate([high, high, low], axis=1)


def stacked(b):
    high, low = halves(b)
    return jnp.concatenate([high, low, high], axis=0)


def doubled(b):
    return jnp.concatenate(halves(b), axis=0)


def by_parts(a, bh, bl, dims=NN):
    n = a.shape[0] // 2
    both = raw(a, bh, dims)
    return both[:n] + (both[n:] + raw(a[:n], bl, dims))


def mm_exact_b(a, b, dims=NN):
    ah, al = halves(a)
    return raw(ah, b, dims) + raw(al, b, dims)


def mm_exact_a(a, b):
    n = b.shape[0]
    both = raw(a, jnp.concatenate(halves(b), axis=0), NT)
    return both[:, :n] + both[:, n:]


def slot_plan(depth):
    sides = [1] if depth == 2 else [1, -1]
    ends = (-1, 1)
    groups = [
        [((0, dy, dz), CELLS // 2) for dz in sides for dy in ends],
        [((dx, dy, 0), 1) for dx in ends for dy in ends],
        [((dx, dy, dz), 1) for dz in sides for dx in ends for dy in ends],
        [((0, dy, 0), 2 * CELLS) for dy in ends],
        [((dx, 0, dz), CELLS) for dz in sides for dx in ends],
        [((dx, 0, 0), 2 * CELLS) for dx in ends],
        [((0, 0, dz), HALF) for dz in sides],
    ]
    plan, at = [], 0
    for step, rows in [entry for group in groups for entry in group]:
        plan.append((step, at, rows))
        at += rows
    return plan, at


def origin(step, tiles):
    return 0 if step >= 0 else CELLS - tiles


def by_reach(plan):
    def rank(entry):
        (dx, dy, dz), _, rows = entry
        return dy == 0, dy < 0, rows > CELLS, dz, rows

    return sorted(plan, key=rank)


def own_corner(step):
    return step[2] == 0 and step[0] != 0 and step[1] != 0


def wave(turns):
    f = turns - jnp.floor(turns + 0.5)
    f = jnp.where(f > 0.25, 0.5 - f, jnp.where(f < -0.25, -0.5 - f, f))
    x = f * (2.0 * math.pi)
    s = x * x
    p = -1.0 / 39916800.0
    for c in (1.0 / 362880.0, -1.0 / 5040.0, 1.0 / 120.0, -1.0 / 6.0):
        p = p * s + c
    return x + x * s * p


def divided(value, by):
    return jnp.floor((value + 0.5) * (1.0 / by))


def silu_pair(x):
    s = 0.5 + 0.5 * jnp.tanh(0.5 * x)
    return x * s, s * (1.0 + x * (1.0 - s))


def kernel_body(sizes, plan, disp_hbm, spec_hbm, cen_hbm, nbr_hbm, cnt_hbm, alive_hbm, two_hbm,
                lat_hbm, env_hbm, out_hbm, readout_hbm, result,
                disp, spec, cen, nbr, cnt, alive, w_two, w_lat, w_env, w_out_t, readout,
                table, pack, ztable, zpack, note, inbox, mail, mail_in, back_mail, back_inbox, halo, part, got,
                send_a, recv_a, send_b, recv_b, load):
    loads = [
        pltpu.make_async_copy(src, dst, load.at[at])
        for at, (src, dst) in enumerate(
            (
                (disp_hbm, disp),
                (spec_hbm, spec),
                (cen_hbm, cen),
                (nbr_hbm, nbr),
                (cnt_hbm, cnt),
                (alive_hbm, alive),
                (two_hbm, w_two),
                (lat_hbm, w_lat),
                (env_hbm, w_env),
                (out_hbm, w_out_t),
                (readout_hbm, readout),
            )
        )
    ]
    for copy in loads:
        copy.start()
    disp, spec, cen, nbr, cnt, alive = (
        ref.at[0] for ref in (disp, spec, cen, nbr, cnt, alive)
    )
    total = result.at[pl.ds(0, CELLS * CELLS)]
    me = tuple(lax.axis_index(a) for a in AXES)
    odd = [lax.rem(i, 2) for i in me[:2]]
    swapped = tuple(i + 1 - 2 * o for i, o in zip(me, odd)) + me[2:]

    def moved(place, step, sign):
        return tuple(
            lax.rem(i + (sign * d + n), n) if d else i for i, d, n in zip(place, step, sizes)
        )

    def holder(step):
        return moved(swapped, step, 1)

    def worker(step):
        x, y, z = moved(me, step, -1)
        return x + 1 - 2 * lax.rem(x, 2), y + 1 - 2 * lax.rem(y, 2), z

    def mine_too(step):
        return (odd[0] == (1 if step[0] > 0 else 0)) & (odd[1] == (1 if step[1] > 0 else 0))

    barrier = pltpu.get_barrier_semaphore()

    def greet(device):
        pl.semaphore_signal(
            barrier, inc=1, device_id=device, device_id_type=pl.DeviceIdType.MESH
        )

    def unless_mine(step, action):
        if own_corner(step):
            pl.when(jnp.logical_not(mine_too(step)))(action)
        else:
            action()

    for step, at, rows in by_reach(plan):
        unless_mine(step, lambda step=step: greet(holder(step)))
    greet(swapped)

    for copy in loads[:6]:
        copy.wait()
    dwide, swide = 16 * ZROWS, 16 * KINDS
    dline = jnp.concatenate([disp[:, dwide * q : dwide * (q + 1)] for q in range(4)], axis=0)
    sline = jnp.concatenate([spec[:, swide * q : swide * (q + 1)] for q in range(4)], axis=0)
    sline = sline.astype(jnp.float32)
    gap = jnp.zeros((4, KEPT), jnp.float32)
    blank = jnp.zeros((4, LANES - KIND_AT - KINDS), jnp.float32)
    for j in range(16):
        kinds = sline[:, KINDS * j : KINDS * (j + 1)]
        table[pl.ds(j, 4, stride=16), :] = jnp.concatenate(
            [
                dline[:, ZROWS * j : ZROWS * (j + 1)],
                gap,
                kinds[:, KINDS - 6 : KINDS],
                kinds[:, 0 : KINDS - 6],
                blank,
            ],
            axis=1,
        )
    lane_row = lax.broadcasted_iota(jnp.int32, (1, LANES), 1)

    def high(shape):
        ids = lax.broadcasted_iota(jnp.int32, shape, 1)
        return (
            ((ids >= KEPT) & (ids < 2 * KEPT))
            | ((ids >= ZROWS) & (ids < KIND_AT))
            | ((ids >= KIND_AT + KEPT) & (ids < KIND_AT + KEPT + 12))
        )

    ztable[...] = jnp.where(
        high((HALF, LANES)),
        pltpu.roll(table[pl.ds(HALF, HALF), :], KEPT, 1),
        table[pl.ds(0, HALF), :],
    )
    for t, y in enumerate((0, 1, CELLS - 2, CELLS - 1)):
        pack[pl.ds(8 * t, 8), :] = table[pl.ds(y, 8, stride=8), :]
    for t, y in enumerate((0, CELLS - 1)):
        zpack[pl.ds(4 * t, 4), :] = ztable[pl.ds(y, 4, stride=8), :]

    def source(step, rows):
        dx, dy, dz = step
        if dx and dy:
            if dz:
                return ztable.at[pl.ds((HALF - CELLS) * (dx < 0) + (CELLS - 1) * (dy < 0), 1)]
            return table.at[pl.ds(CELLS * (CELLS - 1) * (dx < 0) + (CELLS - 1) * (dy < 0), 1)]
        if dy:
            return (zpack if dz else pack).at[pl.ds(0 if dy > 0 else rows, rows)]
        if dz:
            return ztable.at[pl.ds(HALF - rows if dx < 0 else 0, rows)]
        return table.at[pl.ds(CELLS * origin(dx, 2), rows)]

    def remote(src, dst, send, recv, device):
        return pltpu.make_async_remote_copy(
            src_ref=src,
            dst_ref=dst,
            send_sem=send,
            recv_sem=recv,
            device_id=device,
            device_id_type=pl.DeviceIdType.MESH,
        )


    pairs = nbr.shape[1]
    centre_total = cen.shape[1]
    slots = pairs // centre_total
    lane = lax.broadcasted_iota(jnp.int32, (centre_total, pairs), 1)
    row = lax.broadcasted_iota(jnp.int32, (centre_total, pairs), 0)
    mine = ((lane >= row * slots) & (lane < (row + 1) * slots)).astype(jnp.float32)
    mine16 = mine.astype(jnp.bfloat16)
    own = CELLS * CELLS

    def site(atom):
        one, two = atom == 1.0, atom == 2.0
        return (
            jnp.where(one, 0.75, 0.25),
            jnp.where(one | two, 0.75, 0.25),
            jnp.where(two, 0.75, 0.25),
        )

    def kind_lane(z, atom):
        turned = jnp.where(z >= CELLS - 2, z - (CELLS - 2), z + 2.0)
        return KIND_AT + 3.0 * turned + atom

    first = cen[...].astype(jnp.float32)
    cell_i = divided(first, 3.0)
    atom_i = first - 3.0 * cell_i
    col_i = divided(cell_i, CELLS)
    z_i = cell_i - CELLS * col_i
    x_i = divided(col_i, CELLS)
    y_i = col_i - CELLS * x_i
    spot_i = [a + b for a, b in zip((x_i, y_i, z_i), site(atom_i))]
    alive_lane = lax.broadcasted_iota(jnp.int32, (1, centre_total), 1)
    count = jnp.where(alive_lane < alive[...], cnt[...], 0).astype(jnp.float32)
    spread = raw(
        jnp.concatenate(
            spot_i + [count, col_i, 3.0 * z_i + atom_i, kind_lane(z_i, atom_i)]
            + [jnp.zeros((1, centre_total), jnp.float32)],
            axis=0,
        ).astype(jnp.bfloat16),
        mine16,
        NN,
    )
    lanef = lax.broadcasted_iota(jnp.int32, (1, pairs), 1).astype(jnp.float32)
    slot_id = lanef - slots * divided(lanef, slots)
    live = jnp.where(slot_id < spread[3:4], 1.0, 0.0).astype(jnp.float32)

    second = nbr[...].astype(jnp.float32)
    ext = CELLS + 4
    cell_j = divided(second, 3.0)
    atom_j = second - 3.0 * cell_j
    col_j = divided(cell_j, ext)
    z_j = cell_j - ext * col_j - 2.0
    x_j = divided(col_j, ext)
    y_j = col_j - ext * x_j - 2.0
    x_j = x_j - 2.0

    def side(v):
        return jnp.where(v < 0.0, -1.0, jnp.where(v >= CELLS, 1.0, 0.0))

    sx, sy, sz = side(x_j), side(y_j), side(z_j)
    x_in, y_in, z_in = x_j - CELLS * sx, y_j - CELLS * sy, z_j - CELLS * sz
    if sizes[2] == 2:
        sz = jnp.abs(sz)
    code = sx * 9.0 + sy * 3.0 + sz
    upper = jnp.where(x_in >= CELLS // 2, 1.0, 0.0)
    across, along = x_in * CELLS + y_in, y_in * CELLS + x_in
    line = jnp.full_like(code, -1.0)
    for (dx, dy, dz), at, rows in plan:
        if dx and dy:
            value = float(at)
        elif dz and dy:
            value = x_in - (CELLS // 2) * upper + float(at)
        elif dz and dx:
            value = y_in + float(at)
        elif dz:
            value = across - HALF * upper + float(at)
        elif dy:
            value = along + float(at - CELLS * origin(dy, 2))
        else:
            value = across + float(at - CELLS * origin(dx, 2))
        line = jnp.where(code == float(dx * 9 + dy * 3 + dz), value, line)
    raised = jnp.where(sz != 0.0, upper, 0.0)
    place_j = 3.0 * z_in + atom_j + (KEPT // 3) * raised
    kind_at_j = kind_lane(z_in, atom_j) + KEPT * raised
    inner = jnp.where(code == 0.0, across, -1.0)

    place = jnp.concatenate(
        [jnp.where(code == 0.0, place_j, -8.0), spread[5:6]], axis=1
    ).astype(jnp.int32)
    kind_at = jnp.concatenate([kind_at_j, spread[6:7]], axis=1).astype(jnp.int32)
    column = jnp.concatenate([inner, spread[4:5]], axis=1).astype(jnp.int32)

    def hot(index, length):
        ids = lax.broadcasted_iota(jnp.int32, (length, index.shape[1]), 0)
        return jnp.where(ids == index, 1.0, 0.0).astype(jnp.bfloat16)

    def third(rows, width):
        ids = lax.broadcasted_iota(jnp.int32, (rows, width), 0).astype(jnp.float32)
        group = divided(ids, 3.0)
        return group.astype(jnp.int32), (ids - 3.0 * group).astype(jnp.int32)

    def picked(stack, at, kind_at):
        width = stack.shape[1]
        group, _ = third(96, width)
        _, turn = third(24, width)
        kept = jnp.where(group == at, stack[0:96], 0.0)
        folded = (kept[0:24] + kept[24:48]) + (kept[48:72] + kept[72:96])
        out = [
            jnp.sum(jnp.where(turn == c, folded, 0.0), axis=0, keepdims=True) for c in range(3)
        ]
        ids = lax.broadcasted_iota(jnp.int32, (32, width), 0) + 88
        kind = jnp.sum(jnp.where(ids == kind_at, stack[88:120], 0.0), axis=0, keepdims=True)
        return out, kind

    def placed(at, values):
        width = at.shape[1]
        group, _ = third(96, width)
        _, turn = third(24, width)
        cycle = jnp.where(
            turn == 0, values[0], jnp.where(turn == 1, values[1], values[2])
        )
        out = jnp.where(group == at, jnp.concatenate([cycle] * 4, axis=0), 0.0)
        return jnp.concatenate([out, jnp.zeros((LANES - 96, width), jnp.float32)], axis=0)

    def fetch(block, onehot):
        return raw(
            jnp.concatenate(halves(block.T), axis=1),
            jnp.concatenate([onehot, onehot], axis=0),
            NN,
        )

    hot_own = hot(column, own)
    note[...] = jnp.concatenate([line, place_j, kind_at_j, live], axis=0)
    spot_j = [a + b for a, b in zip((x_j, y_j, z_j), site(atom_j))]
    apart = [spot_j[c] - spread[c : c + 1] for c in range(3)]

    pl.semaphore_wait(barrier, len(plan))
    post = None
    for step, at, rows in by_reach(plan):
        if step[1] == 0 and post is None:
            post = remote(note, inbox, send_a.at[1], recv_a.at[1], worker((0, 0, 0)))
            post.start()
        copy = remote(
            source(step, rows), halo.at[pl.ds(at, rows)], send_a.at[0], recv_a.at[0], worker(step)
        )
        unless_mine(step, copy.start)


    shift, kind = picked(fetch(table[...], hot_own), place, kind_at)
    mail[...] = jnp.concatenate(
        [(apart[c] + (shift[c][:, 0:pairs] - shift[c][:, pairs:])) * SIDE for c in range(3)]
        + [kind[:, pairs:] + 2.0 * jnp.where(code == 0.0, kind[:, 0:pairs], 0.0)],
        axis=0,
    )
    parcel = remote(mail, mail_in, send_a.at[2], recv_a.at[2], worker((0, 0, 0)))
    parcel.start()

    for copy in loads[6:]:
        copy.wait()
    two = w_two[...]
    two = jnp.concatenate([two[4:12], two[0:4], jnp.zeros_like(two[0:4])], axis=0)
    out_t = w_out_t[...]
    width = w_lat.shape[0]
    two_3, lat_3, env_3 = thrice(two.T), thrice(w_lat[...].T), thrice(w_env[...].T)
    out_a, out_b = thrice(out_t[:, 0:width]), doubled(out_t[:, width:])
    back_3 = thrice(out_t.T)
    gain = jnp.broadcast_to(readout[...], (8, width)).T[:, 0:1]

    crossing = plan[-1][1] + plan[-1][2] - 1
    halo_rows = halo.shape[0]

    def every(ref, send, recv):
        span = pl.ds(0, crossing)
        return remote(ref.at[span], ref.at[span], send, recv, swapped)

    ids = lax.broadcasted_iota(jnp.int32, (8, LANES), 0)

    def with_mine(block, row_of):
        corner = [(step, at) for step, at, rows in plan if own_corner(step)]
        base = corner[0][1] // 8 * 8
        tile = block[base : base + 8]
        for step, at in corner:
            tile = jnp.where((ids == at - base) & mine_too(step), row_of(step, at), tile)
        pieces = [block[0:base]] if base else []
        pieces.append(tile)
        if base + 8 < block.shape[0]:
            pieces.append(block[base + 8 :])
        return jnp.concatenate(pieces, axis=0)

    arrivals = every(halo, send_a.at[0], recv_a.at[0])
    wide = 2 * LANES
    per = wide // slots
    lines = -(-9 * per // 16) * 16
    member = (
        lax.broadcasted_iota(jnp.int32, (per, wide), 1)
        - slots * lax.broadcasted_iota(jnp.int32, (per, wide), 0)
    )
    member = ((member >= 0) & (member < slots)).astype(jnp.float32)
    unused = jnp.zeros((lines - 9 * per, wide), jnp.float32)
    spot = lax.broadcasted_iota(jnp.int32, (width, 3 * lines), 1)
    term = jnp.where(spot >= 2 * lines, 2, jnp.where(spot >= lines, 1, 0))
    inner_spot = spot - lines * term
    groups = [
        (inner_spot >= a * per) & (inner_spot < b * per) for a, b in ((0, 1), (1, 4), (4, 9))
    ]
    block_row = lax.broadcasted_iota(jnp.int32, (lines, 3 * width), 0)
    block_lane = lax.broadcasted_iota(jnp.int32, (lines, 3 * width), 1)
    blocks = [
        (block_row >= a * per) & (block_row < b * per) & (block_lane >= k * width)
        & (block_lane < (k + 1) * width)
        for k, (a, b) in enumerate(((0, 1), (1, 4), (4, 9)))
    ]
    blocks = blocks[0] | blocks[1] | blocks[2]
    order = (lax.broadcasted_iota(jnp.int32, (NBASIS, wide), 0) + 1).astype(jnp.float32)
    s3, s5, s15 = math.sqrt(3.0), math.sqrt(5.0), math.sqrt(15.0)
    norm = math.sqrt(2.0 / CUTOFF)

    def split(a):
        high = a.astype(jnp.bfloat16).astype(jnp.float32)
        return jnp.where(term == 2, a - high, high)

    post.wait_recv()
    letter = inbox[...]
    hot_j = hot(letter[0:1].astype(jnp.int32), halo_rows)
    twice_j = jnp.concatenate([hot_j, hot_j], axis=0)
    there = letter[1:2].astype(jnp.int32)
    kind_there = letter[2:3].astype(jnp.int32)
    arrivals.wait_recv()

    block = with_mine(halo[...], lambda step, at: source(step, 1)[...])
    total_rows = plan[-1][1] + plan[-1][2]
    if total_rows < halo_rows:
        every_id = lax.broadcasted_iota(jnp.int32, (halo_rows, LANES), 0)
        block = jnp.where(every_id < total_rows, block, 0.0)

    block = jnp.concatenate([v.T for v in halves(block)], axis=1)

    stacks = [raw(block, twice_j[:, at : at + wide], NN) for at in range(0, pairs, wide)]
    parcel.wait_recv()
    sheet = mail_in[...]

    def network(at):
        span = slice(at, at + wide)
        shift_j, kind_j = picked(stacks[at // wide], there[:, span], kind_there[:, span])
        yield
        rx, ry, rz = [sheet[c : c + 1, span] + SIDE * shift_j[c] for c in range(3)]
        live = letter[3:4, span]
        own_j = jnp.where(sheet[3:4, span] > 1.5, 1.0, 0.0)
        kind_i = sheet[3:4, span] - 2.0 * own_j
        kind_j = own_j + kind_j
        square = rx * rx + ry * ry + rz * rz
        inv = lax.rsqrt(square)
        dist = square * inv
        ux, uy, uz = rx * inv, ry * inv, rz * inv
        ratio = dist * (1.0 / CUTOFF)
        r2 = ratio * ratio
        r5 = r2 * r2 * ratio
        inside = ratio < 1.0
        bell = jnp.where(
            inside, 1.0 + r5 * ratio * (-28.0 + ratio * (48.0 - 21.0 * ratio)), 0.0
        )
        slope = jnp.where(
            inside, r5 * (1.0 - ratio) * (1.0 - ratio) * (-168.0 / CUTOFF), 0.0
        )
        turns = order * (dist * (0.5 / CUTOFF))
        sines, cosines = wave(turns), wave(turns + 0.25)
        basis = norm * sines * (inv * bell)
        basis_d = norm * (
            cosines * order * (inv * bell * (math.pi / CUTOFF))
            + sines * (inv * (slope - bell * inv))
        )
        kinds = [1.0 - kind_i, kind_i, 1.0 - kind_j, kind_j]
        inputs = jnp.concatenate(
            [basis] + kinds + [jnp.zeros((4, wide), jnp.float32)], axis=0
        )
        inputs_t = jnp.concatenate([basis_d, jnp.zeros((8, wide), jnp.float32)], axis=0)

        hidden = raw(two_3, stacked(inputs), NN)
        hidden_t = raw(two_3, stacked(inputs_t), NN)
        yield
        hidden, hidden_d = silu_pair(hidden)
        latent = raw(lat_3, stacked(hidden), NN)
        latent_t = raw(lat_3, stacked(hidden_t * hidden_d), NN)
        yield
        latent, latent_d = silu_pair(latent)
        latent_t = latent_t * latent_d
        lat_h, lat_l = halves(latent)
        scale = bell * live
        scale_t = slope * live
        harm = [
            jnp.ones_like(ux),
            s3 * ux,
            s3 * uy,
            s3 * uz,
            s15 * ux * uy,
            s15 * uy * uz,
            0.5 * s5 * (3.0 * uz * uz - 1.0),
            s15 * ux * uz,
            0.5 * s15 * (ux * ux - uy * uy),
        ]
        rows = jnp.concatenate([h * member for h in harm] + [unused], axis=0)
        rows_h, rows_l = halves(rows)
        rows_3 = jnp.concatenate([rows_h, rows_l, rows_h], axis=0)
        scaled_h, scaled_l = [
            jnp.concatenate([v] * 3, axis=0) for v in halves(rows * scale)
        ]
        gathered = by_parts(jnp.concatenate([lat_h, lat_l], axis=0), scaled_h, scaled_l, NT)
        yield
        environ = ENV * raw(env_3, stacked(gathered), NN)
        lat_s = jnp.concatenate([lat_h, lat_l, lat_h], axis=0)
        plain = raw(env_3, lat_s, NN)
        yield
        environ_s = split(environ)
        chosen = jnp.concatenate(
            [jnp.where(g, environ_s, 0.0) for g in groups], axis=0
        ).astype(jnp.bfloat16)
        mixed = raw(chosen, rows_3, NN)
        partly = raw(out_a, lat_s, NN)
        plain_t = raw(env_3, stacked(latent_t), NN)
        weight = plain * scale
        yield
        mixed = [mixed[width * k : width * (k + 1)] for k in range(3)]
        joined_h, joined_l = halves(jnp.concatenate([weight * a for a in mixed], axis=0))
        updated = by_parts(out_b, joined_h, joined_l) + partly
        yield
        weight_t = plain_t * scale + plain * scale_t
        near = jnp.concatenate([jnp.where(g, environ, 0.0)[:, 0:LANES] for g in groups], axis=0)
        near = doubled(near.T[0:lines])
        weight_s, slant_s = stacked(weight), stacked(weight_t)
        updated, updated_d = silu_pair(updated)
        d_out = (gain * scale) * updated_d
        back = raw(back_3, stacked(d_out), NN)
        score = jnp.sum(gain * updated, axis=0, keepdims=True)
        pair_energy = score * scale
        yield
        d_mixed = [back[width * (k + 1) : width * (k + 2)] for k in range(3)]
        pass_h, pass_l = halves(jnp.concatenate([q * weight for q in d_mixed], axis=0))
        d_env = by_parts(jnp.concatenate([rows_h, rows_l], axis=0), pass_h, pass_l, NT)
        d_rows = by_parts(near, pass_h, pass_l)
        yield
        along = d_mixed[0] * mixed[0] + d_mixed[1] * mixed[1] + d_mixed[2] * mixed[2]
        d_dist = (
            jnp.sum(along * weight_t + back[0:width] * latent_t, axis=0, keepdims=True)
            + score * scale_t
        )
        d_env = jnp.where(blocks, ENV * d_env, 0.0)
        d_env = jnp.concatenate([d_env, jnp.zeros((lines, width), jnp.float32)], axis=1)
        d_env = d_env[:, 0:LANES] + d_env[:, LANES:]
        d_env_h, d_env_l = halves(d_env + pltpu.roll(d_env, width, 1))
        d_env = jnp.concatenate([d_env_h, d_env_l[:, 0:width]], axis=1)
        d_rows = d_rows + raw(d_env, weight_s, NN)
        slanted = raw(d_env, slant_s, NN)
        yield
        turned = [d_rows[m * per : (m + 1) * per] for m in range(9)]
        dux = s3 * turned[1] + s15 * (uy * turned[4] + uz * turned[7] + ux * turned[8])
        duy = s3 * turned[2] + s15 * (ux * turned[4] + uz * turned[5] - uy * turned[8])
        duz = (
            s3 * turned[3]
            + s15 * (uy * turned[5] + ux * turned[7])
            + 3.0 * s5 * uz * turned[6]
        )
        dux, duy, duz = [
            jnp.sum(d * member, axis=0, keepdims=True) for d in (dux, duy, duz)
        ]
        d_dist = d_dist + jnp.sum(rows * slanted, axis=0, keepdims=True)
        radial = d_dist - (ux * dux + uy * duy + uz * duz) * inv
        yield [d * inv + u * radial for d, u in ((dux, ux), (duy, uy), (duz, uz))] + [
            pair_energy
        ]

    runs = [network(at) for at in range(0, pairs, wide)]
    found = [None] * len(runs)
    while found[0] is None:
        found = [next(run) for run in runs]
    *grad, pair_energy = [jnp.concatenate(v, axis=1) for v in zip(*found)]
    back_mail[...] = jnp.concatenate(grad + [pair_energy], axis=0)
    reply = remote(back_mail, back_inbox, send_b.at[1], recv_b.at[1], swapped)
    reply.start()
    partial = mm_exact_a(hot_j, placed(there, [-g for g in grad]))
    early = max(at + rows for (_, dy, _), at, rows in plan if dy)

    def give(entries):
        for step, at, rows in entries:
            span = pl.ds(at, rows)
            copy = remote(
                part.at[span], got.at[span], send_b.at[0], recv_b.at[0], holder(step)
            )
            unless_mine(step, copy.start)

    ranked = by_reach(plan)
    first_rows = -(-early // 8) * 8
    part[pl.ds(0, first_rows), :] = partial[0:first_rows]
    give([entry for entry in ranked if entry[0][1]])
    part[pl.ds(first_rows, halo_rows - first_rows), :] = partial[first_rows:]
    give([entry for entry in ranked if not entry[0][1]])

    reply.wait_recv()
    answer = back_inbox[...]
    moves = [answer[c : c + 1] for c in range(3)]
    settled = mm_exact_a(
        hot_own,
        jnp.concatenate(
            [placed(place[:, 0:pairs], [-m for m in moves]), placed(place[:, pairs:], moves)],
            axis=1,
        ),
    )
    energies = mm_exact_b(jnp.broadcast_to(answer[3:4], (8, pairs)), mine16, NT)
    result[pl.ds(own, 8), 0:centre_total] = energies
    below = lax.broadcasted_iota(jnp.int32, (CELLS, LANES), 0)
    upper_lanes = high((CELLS, LANES))
    returns = every(got, send_b.at[0], recv_b.at[0])
    returns.wait_recv()

    slabs = [settled[CELLS * x : CELLS * (x + 1)] for x in range(CELLS)]
    columns = {y: [[] for x in range(CELLS)] for y in (0, 1, CELLS - 2, CELLS - 1)}

    def low_part(value):
        return jnp.where(upper_lanes[0 : value.shape[0]], 0.0, value)

    def high_part(value):
        kept = jnp.where(upper_lanes[0 : value.shape[0]], value, 0.0)
        return pltpu.roll(kept, LANES - KEPT, 1)

    for (dx, dy, dz), at, rows in plan:
        x, y = (CELLS - 1) * (dx < 0), (CELLS - 1) * (dy < 0)
        if own_corner((dx, dy, dz)):
            value = jnp.where(
                mine_too((dx, dy, dz)), part[pl.ds(at, 1), :], got[pl.ds(at, 1), :]
            )
            columns[y][x].append(value)
        elif dx and dy:
            value = got[pl.ds(at, 1), :]
            columns[y][x].append(high_part(value) if dx < 0 else low_part(value))
        elif dz and dy:
            value = got[pl.ds(at, rows), :]
            for part_of, base in ((low_part(value), 0), (high_part(value), rows)):
                for r in range(rows):
                    columns[y][base + r].append(part_of[r : r + 1])
        elif dz and dx:
            value = got[pl.ds(at, rows), :]
            slabs[x] = slabs[x] + (high_part(value) if dx < 0 else low_part(value))
        elif dz:
            for r in range(CELLS // 2):
                value = got[pl.ds(at + CELLS * r, CELLS), :]
                slabs[r] = slabs[r] + low_part(value)
                slabs[CELLS // 2 + r] = slabs[CELLS // 2 + r] + high_part(value)
        elif dy:
            for t in range(2):
                for r in range(CELLS):
                    columns[origin(dy, 2) + t][r].append(got[pl.ds(at + 8 * t + r, 1), :])
        else:
            for t in range(2):
                x = origin(dx, 2) + t
                slabs[x] = slabs[x] + got[pl.ds(at + CELLS * t, CELLS), :]
    for x in range(CELLS):
        side = jnp.zeros((CELLS, LANES), jnp.float32)
        for y, lists in columns.items():
            value = sum(lists[x][1:], lists[x][0])
            side = jnp.where(below == y, value, side)
        total[pl.ds(CELLS * x, CELLS), :] = slabs[x] + side
    for copy in (post, parcel, arrivals, reply, returns):
        copy.wait_send()


def unpack_body(result, energy, forces):
    energy[0] = result[pl.ds(CELLS * CELLS, 1), 0 : energy.shape[2]]
    final = jnp.concatenate(
        [result[pl.ds(j, 4, stride=16), :][:, 0:ZROWS] for j in range(16)], axis=1
    )
    wide = 16 * ZROWS
    for q in range(4):
        forces[0, :, wide * q : wide * (q + 1)] = final[q : q + 1, :]


def solution(mesh):
    sizes = tuple(mesh.shape[a] for a in AXES)
    plan, line_total = slot_plan(sizes[2])

    def local(displacement, species, centres, neighbours, neighbour_count, live_centres,
              w_two, w_lat, w_env, w_out, readout):
        pairs = neighbours.shape[2]
        vmem = pl.BlockSpec(memory_space=pltpu.VMEM)
        rows = -(-line_total // 8) * 8
        args = [
            displacement, species, centres, neighbours, neighbour_count, live_centres,
            w_two, w_lat, w_env, w_out.T, readout.reshape(1, -1),
        ]

        def body(*refs):
            pl.run_scoped(
                lambda load: kernel_body(sizes, plan, *refs, load),
                pltpu.SemaphoreType.DMA((len(args),)),
            )

        sizes_vmem = [
            (CELLS * CELLS, LANES), (4 * CELLS, LANES), (HALF, LANES), (CELLS, LANES),
            (4, pairs), (4, pairs), (4, pairs), (4, pairs), (4, pairs), (4, pairs),
            (rows, LANES), (rows, LANES), (rows, LANES),
        ]
        result = pl.pallas_call(
            body,
            out_shape=pltpu.VMEM((CELLS * CELLS + 8, LANES), jnp.float32),
            in_specs=[pl.BlockSpec(memory_space=pltpu.HBM)] * len(args),
            out_specs=vmem,
            scratch_shapes=[pltpu.VMEM(x.shape, x.dtype) for x in args]
            + [pltpu.VMEM(shape, jnp.float32) for shape in sizes_vmem]
            + [pltpu.SemaphoreType.DMA((3,))] * 2
            + [pltpu.SemaphoreType.DMA((2,))] * 2,
            compiler_params=pltpu.CompilerParams(collective_id=0, has_side_effects=True),
        )(*args)
        result = pltpu.with_memory_space_constraint(result, pltpu.VMEM)
        return pl.pallas_call(
            unpack_body,
            out_shape=(
                jax.ShapeDtypeStruct(centres.shape, jnp.float32),
                jax.ShapeDtypeStruct(displacement.shape, jnp.float32),
            ),
            in_specs=[vmem],
            out_specs=(vmem, vmem),
        )(result)

    split = P(*AXES)
    return jax.shard_map(
        local,
        mesh=mesh,
        in_specs=(split,) * 6 + (P(),) * 5,
        out_specs=(split, split),
        check_vma=False,
    )
```

```python
import math

import jax
import jax.numpy as jnp
from jax import lax
from jax.experimental import pallas as pl
from jax.experimental.pallas import tpu as pltpu
from jax.sharding import PartitionSpec as P

CELLS = 8
NBASIS = 8
CUTOFF = 6.0
SIDE = 3.1
ENV = 0.2
LANES = 128
ZROWS = CELLS * 9
KINDS = CELLS * 3
KEPT = 18
KIND_AT = ZROWS + KEPT
HALF = CELLS * CELLS // 2
AXES = ("gx", "gy", "gz")

NN = (((1,), (0,)), ((), ()))
NT = (((1,), (1,)), ((), ()))


def halves(x):
    hi = x.astype(jnp.bfloat16)
    lo = (x - hi.astype(jnp.float32)).astype(jnp.bfloat16)
    return hi, lo


def raw(a, b, dims):
    return lax.dot_general(a, b, dims, preferred_element_type=jnp.float32)


def thrice(a):
    high, low = halves(a)
    return jnp.concatenate([high, high, low], axis=1)


def stacked(b):
    high, low = halves(b)
    return jnp.concatenate([high, low, high], axis=0)


def doubled(b):
    return jnp.concatenate(halves(b), axis=0)


def by_parts(a, bh, bl, dims=NN):
    n = a.shape[0] // 2
    both = raw(a, bh, dims)
    return both[:n] + (both[n:] + raw(a[:n], bl, dims))


def mm_exact_b(a, b, dims=NN):
    ah, al = halves(a)
    return raw(ah, b, dims) + raw(al, b, dims)


def mm_exact_a(a, b):
    n = b.shape[0]
    both = raw(a, jnp.concatenate(halves(b), axis=0), NT)
    return both[:, :n] + both[:, n:]


def slot_plan(depth):
    sides = [1] if depth == 2 else [1, -1]
    ends = (-1, 1)
    groups = [
        [((0, dy, dz), CELLS // 2) for dz in sides for dy in ends],
        [((dx, dy, 0), 1) for dx in ends for dy in ends],
        [((dx, dy, dz), 1) for dz in sides for dx in ends for dy in ends],
        [((0, dy, 0), 2 * CELLS) for dy in ends],
        [((dx, 0, dz), CELLS) for dz in sides for dx in ends],
        [((dx, 0, 0), 2 * CELLS) for dx in ends],
        [((0, 0, dz), HALF) for dz in sides],
    ]
    plan, at = [], 0
    for step, rows in [entry for group in groups for entry in group]:
        plan.append((step, at, rows))
        at += rows
    return plan, at


def origin(step, tiles):
    return 0 if step >= 0 else CELLS - tiles


def by_reach(plan):
    def rank(entry):
        (dx, dy, dz), _, rows = entry
        return dy == 0, dy < 0, rows > CELLS, dz, rows

    return sorted(plan, key=rank)


def own_corner(step):
    return step[2] == 0 and step[0] != 0 and step[1] != 0


def wave(turns):
    f = turns - jnp.floor(turns + 0.5)
    f = jnp.where(f > 0.25, 0.5 - f, jnp.where(f < -0.25, -0.5 - f, f))
    x = f * (2.0 * math.pi)
    s = x * x
    p = -1.0 / 39916800.0
    for c in (1.0 / 362880.0, -1.0 / 5040.0, 1.0 / 120.0, -1.0 / 6.0):
        p = p * s + c
    return x + x * s * p


def divided(value, by):
    return jnp.floor((value + 0.5) * (1.0 / by))


def silu_pair(x):
    s = 0.5 + 0.5 * jnp.tanh(0.5 * x)
    return x * s, s * (1.0 + x * (1.0 - s))


def kernel_body(sizes, plan, disp_hbm, spec_hbm, cen_hbm, nbr_hbm, cnt_hbm, alive_hbm, two_hbm,
                lat_hbm, env_hbm, out_hbm, readout_hbm, result,
                disp, spec, cen, nbr, cnt, alive, w_two, w_lat, w_env, w_out_t, readout,
                table, pack, ztable, zpack, note, inbox, mail, mail_in, back_mail, back_inbox, halo, part, got,
                recv_a, recv_b, load, send_a, send_b):
    loads = [
        pltpu.make_async_copy(src, dst, load.at[at])
        for at, (src, dst) in enumerate(
            (
                (disp_hbm, disp),
                (spec_hbm, spec),
                (cen_hbm, cen),
                (nbr_hbm, nbr),
                (cnt_hbm, cnt),
                (alive_hbm, alive),
                (two_hbm, w_two),
                (lat_hbm, w_lat),
                (env_hbm, w_env),
                (out_hbm, w_out_t),
                (readout_hbm, readout),
            )
        )
    ]
    for copy in loads:
        copy.start()
    disp, spec, cen, nbr, cnt, alive = (
        ref.at[0] for ref in (disp, spec, cen, nbr, cnt, alive)
    )
    total = result.at[pl.ds(0, CELLS * CELLS)]
    me = tuple(lax.axis_index(a) for a in AXES)
    odd = [lax.rem(i, 2) for i in me[:2]]
    swapped = tuple(i + 1 - 2 * o for i, o in zip(me, odd)) + me[2:]

    def moved(place, step, sign):
        return tuple(
            lax.rem(i + (sign * d + n), n) if d else i for i, d, n in zip(place, step, sizes)
        )

    def holder(step):
        return moved(swapped, step, 1)

    def worker(step):
        x, y, z = moved(me, step, -1)
        return x + 1 - 2 * lax.rem(x, 2), y + 1 - 2 * lax.rem(y, 2), z

    def mine_too(step):
        return (odd[0] == (1 if step[0] > 0 else 0)) & (odd[1] == (1 if step[1] > 0 else 0))

    barrier = pltpu.get_barrier_semaphore()

    def greet(device):
        pl.semaphore_signal(
            barrier, inc=1, device_id=device, device_id_type=pl.DeviceIdType.MESH
        )

    def unless_mine(step, action):
        if own_corner(step):
            pl.when(jnp.logical_not(mine_too(step)))(action)
        else:
            action()

    for step, at, rows in by_reach(plan):
        unless_mine(step, lambda step=step: greet(holder(step)))
    greet(swapped)

    for copy in loads[:6]:
        copy.wait()
    dwide, swide = 16 * ZROWS, 16 * KINDS
    dline = jnp.concatenate([disp[:, dwide * q : dwide * (q + 1)] for q in range(4)], axis=0)
    sline = jnp.concatenate([spec[:, swide * q : swide * (q + 1)] for q in range(4)], axis=0)
    sline = sline.astype(jnp.float32)
    gap = jnp.zeros((4, KEPT), jnp.float32)
    blank = jnp.zeros((4, LANES - KIND_AT - KINDS), jnp.float32)
    for j in range(16):
        kinds = sline[:, KINDS * j : KINDS * (j + 1)]
        table[pl.ds(j, 4, stride=16), :] = jnp.concatenate(
            [
                dline[:, ZROWS * j : ZROWS * (j + 1)],
                gap,
                kinds[:, KINDS - 6 : KINDS],
                kinds[:, 0 : KINDS - 6],
                blank,
            ],
            axis=1,
        )
    lane_row = lax.broadcasted_iota(jnp.int32, (1, LANES), 1)

    def high(shape):
        ids = lax.broadcasted_iota(jnp.int32, shape, 1)
        return (
            ((ids >= KEPT) & (ids < 2 * KEPT))
            | ((ids >= ZROWS) & (ids < KIND_AT))
            | ((ids >= KIND_AT + KEPT) & (ids < KIND_AT + KEPT + 12))
        )

    ztable[...] = jnp.where(
        high((HALF, LANES)),
        pltpu.roll(table[pl.ds(HALF, HALF), :], KEPT, 1),
        table[pl.ds(0, HALF), :],
    )
    for t, y in enumerate((0, 1, CELLS - 2, CELLS - 1)):
        pack[pl.ds(8 * t, 8), :] = table[pl.ds(y, 8, stride=8), :]
    for t, y in enumerate((0, CELLS - 1)):
        zpack[pl.ds(4 * t, 4), :] = ztable[pl.ds(y, 4, stride=8), :]

    def source(step, rows):
        dx, dy, dz = step
        if dx and dy:
            if dz:
                return ztable.at[pl.ds((HALF - CELLS) * (dx < 0) + (CELLS - 1) * (dy < 0), 1)]
            return table.at[pl.ds(CELLS * (CELLS - 1) * (dx < 0) + (CELLS - 1) * (dy < 0), 1)]
        if dy:
            return (zpack if dz else pack).at[pl.ds(0 if dy > 0 else rows, rows)]
        if dz:
            return ztable.at[pl.ds(HALF - rows if dx < 0 else 0, rows)]
        return table.at[pl.ds(CELLS * origin(dx, 2), rows)]

    def remote(src, dst, send, recv, device):
        return pltpu.make_async_remote_copy(
            src_ref=src,
            dst_ref=dst,
            send_sem=send,
            recv_sem=recv,
            device_id=device,
            device_id_type=pl.DeviceIdType.MESH,
        )


    pairs = nbr.shape[1]
    centre_total = cen.shape[1]
    slots = pairs // centre_total
    lane = lax.broadcasted_iota(jnp.int32, (centre_total, pairs), 1)
    row = lax.broadcasted_iota(jnp.int32, (centre_total, pairs), 0)
    mine = ((lane >= row * slots) & (lane < (row + 1) * slots)).astype(jnp.float32)
    mine16 = mine.astype(jnp.bfloat16)
    own = CELLS * CELLS

    def site(atom):
        one, two = atom == 1.0, atom == 2.0
        return (
            jnp.where(one, 0.75, 0.25),
            jnp.where(one | two, 0.75, 0.25),
            jnp.where(two, 0.75, 0.25),
        )

    def kind_lane(z, atom):
        turned = jnp.where(z >= CELLS - 2, z - (CELLS - 2), z + 2.0)
        return KIND_AT + 3.0 * turned + atom

    first = cen[...].astype(jnp.float32)
    cell_i = divided(first, 3.0)
    atom_i = first - 3.0 * cell_i
    col_i = divided(cell_i, CELLS)
    z_i = cell_i - CELLS * col_i
    x_i = divided(col_i, CELLS)
    y_i = col_i - CELLS * x_i
    spot_i = [a + b for a, b in zip((x_i, y_i, z_i), site(atom_i))]
    alive_lane = lax.broadcasted_iota(jnp.int32, (1, centre_total), 1)
    count = jnp.where(alive_lane < alive[...], cnt[...], 0).astype(jnp.float32)
    spread = raw(
        jnp.concatenate(
            spot_i + [count, col_i, 3.0 * z_i + atom_i, kind_lane(z_i, atom_i)]
            + [jnp.zeros((1, centre_total), jnp.float32)],
            axis=0,
        ).astype(jnp.bfloat16),
        mine16,
        NN,
    )
    lanef = lax.broadcasted_iota(jnp.int32, (1, pairs), 1).astype(jnp.float32)
    slot_id = lanef - slots * divided(lanef, slots)
    live = jnp.where(slot_id < spread[3:4], 1.0, 0.0).astype(jnp.float32)

    second = nbr[...].astype(jnp.float32)
    ext = CELLS + 4
    cell_j = divided(second, 3.0)
    atom_j = second - 3.0 * cell_j
    col_j = divided(cell_j, ext)
    z_j = cell_j - ext * col_j - 2.0
    x_j = divided(col_j, ext)
    y_j = col_j - ext * x_j - 2.0
    x_j = x_j - 2.0

    def side(v):
        return jnp.where(v < 0.0, -1.0, jnp.where(v >= CELLS, 1.0, 0.0))

    sx, sy, sz = side(x_j), side(y_j), side(z_j)
    x_in, y_in, z_in = x_j - CELLS * sx, y_j - CELLS * sy, z_j - CELLS * sz
    if sizes[2] == 2:
        sz = jnp.abs(sz)
    code = sx * 9.0 + sy * 3.0 + sz
    upper = jnp.where(x_in >= CELLS // 2, 1.0, 0.0)
    across, along = x_in * CELLS + y_in, y_in * CELLS + x_in
    line = jnp.full_like(code, -1.0)
    for (dx, dy, dz), at, rows in plan:
        if dx and dy:
            value = float(at)
        elif dz and dy:
            value = x_in - (CELLS // 2) * upper + float(at)
        elif dz and dx:
            value = y_in + float(at)
        elif dz:
            value = across - HALF * upper + float(at)
        elif dy:
            value = along + float(at - CELLS * origin(dy, 2))
        else:
            value = across + float(at - CELLS * origin(dx, 2))
        line = jnp.where(code == float(dx * 9 + dy * 3 + dz), value, line)
    raised = jnp.where(sz != 0.0, upper, 0.0)
    place_j = 3.0 * z_in + atom_j + (KEPT // 3) * raised
    kind_at_j = kind_lane(z_in, atom_j) + KEPT * raised
    inner = jnp.where(code == 0.0, across, -1.0)

    place = jnp.concatenate(
        [jnp.where(code == 0.0, place_j, -8.0), spread[5:6]], axis=1
    ).astype(jnp.int32)
    kind_at = jnp.concatenate([kind_at_j, spread[6:7]], axis=1).astype(jnp.int32)
    column = jnp.concatenate([inner, spread[4:5]], axis=1).astype(jnp.int32)

    def hot(index, length):
        ids = lax.broadcasted_iota(jnp.int32, (length, index.shape[1]), 0)
        return jnp.where(ids == index, 1.0, 0.0).astype(jnp.bfloat16)

    def third(rows, width):
        ids = lax.broadcasted_iota(jnp.int32, (rows, width), 0).astype(jnp.float32)
        group = divided(ids, 3.0)
        return group.astype(jnp.int32), (ids - 3.0 * group).astype(jnp.int32)

    def picked(stack, at, kind_at):
        width = stack.shape[1]
        group, _ = third(96, width)
        _, turn = third(24, width)
        kept = jnp.where(group == at, stack[0:96], 0.0)
        folded = (kept[0:24] + kept[24:48]) + (kept[48:72] + kept[72:96])
        out = [
            jnp.sum(jnp.where(turn == c, folded, 0.0), axis=0, keepdims=True) for c in range(3)
        ]
        ids = lax.broadcasted_iota(jnp.int32, (32, width), 0) + 88
        kind = jnp.sum(jnp.where(ids == kind_at, stack[88:120], 0.0), axis=0, keepdims=True)
        return out, kind

    def placed(at, values):
        width = at.shape[1]
        group, _ = third(96, width)
        _, turn = third(24, width)
        cycle = jnp.where(
            turn == 0, values[0], jnp.where(turn == 1, values[1], values[2])
        )
        out = jnp.where(group == at, jnp.concatenate([cycle] * 4, axis=0), 0.0)
        return jnp.concatenate([out, jnp.zeros((LANES - 96, width), jnp.float32)], axis=0)

    def fetch(block, onehot):
        return raw(
            jnp.concatenate(halves(block.T), axis=1),
            jnp.concatenate([onehot, onehot], axis=0),
            NN,
        )

    hot_own = hot(column, own)
    note[...] = jnp.concatenate([line, place_j, kind_at_j, live], axis=0)
    spot_j = [a + b for a, b in zip((x_j, y_j, z_j), site(atom_j))]
    apart = [spot_j[c] - spread[c : c + 1] for c in range(3)]

    pl.semaphore_wait(barrier, len(plan))
    post = None
    for step, at, rows in by_reach(plan):
        if step[1] == 0 and post is None:
            post = remote(note, inbox, send_a.at[1], recv_a.at[1], worker((0, 0, 0)))
            post.start()
        copy = remote(
            source(step, rows), halo.at[pl.ds(at, rows)], send_a.at[0], recv_a.at[0], worker(step)
        )
        unless_mine(step, copy.start)


    shift, kind = picked(fetch(table[...], hot_own), place, kind_at)
    mail[...] = jnp.concatenate(
        [(apart[c] + (shift[c][:, 0:pairs] - shift[c][:, pairs:])) * SIDE for c in range(3)]
        + [kind[:, pairs:] + 2.0 * jnp.where(code == 0.0, kind[:, 0:pairs], 0.0)],
        axis=0,
    )
    parcel = remote(mail, mail_in, send_a.at[2], recv_a.at[2], worker((0, 0, 0)))
    parcel.start()

    for copy in loads[6:]:
        copy.wait()
    two = w_two[...]
    two = jnp.concatenate([two[4:12], two[0:4], jnp.zeros_like(two[0:4])], axis=0)
    out_t = w_out_t[...]
    width = w_lat.shape[0]
    two_3, lat_3, env_3 = thrice(two.T), thrice(w_lat[...].T), thrice(w_env[...].T)
    out_a, out_b = thrice(out_t[:, 0:width]), doubled(out_t[:, width:])
    back_3 = thrice(out_t.T)
    gain = jnp.broadcast_to(readout[...], (8, width)).T[:, 0:1]

    crossing = plan[-1][1] + plan[-1][2] - 1
    halo_rows = halo.shape[0]

    def every(ref, send, recv):
        span = pl.ds(0, crossing)
        return remote(ref.at[span], ref.at[span], send, recv, swapped)

    ids = lax.broadcasted_iota(jnp.int32, (8, LANES), 0)

    def with_mine(block, row_of):
        corner = [(step, at) for step, at, rows in plan if own_corner(step)]
        base = corner[0][1] // 8 * 8
        tile = block[base : base + 8]
        for step, at in corner:
            tile = jnp.where((ids == at - base) & mine_too(step), row_of(step, at), tile)
        pieces = [block[0:base]] if base else []
        pieces.append(tile)
        if base + 8 < block.shape[0]:
            pieces.append(block[base + 8 :])
        return jnp.concatenate(pieces, axis=0)

    arrivals = every(halo, send_a.at[0], recv_a.at[0])
    wide = 2 * LANES
    per = wide // slots
    lines = -(-9 * per // 16) * 16
    member = (
        lax.broadcasted_iota(jnp.int32, (per, wide), 1)
        - slots * lax.broadcasted_iota(jnp.int32, (per, wide), 0)
    )
    member = ((member >= 0) & (member < slots)).astype(jnp.float32)
    unused = jnp.zeros((lines - 9 * per, wide), jnp.float32)
    spot = lax.broadcasted_iota(jnp.int32, (width, 3 * lines), 1)
    term = jnp.where(spot >= 2 * lines, 2, jnp.where(spot >= lines, 1, 0))
    inner_spot = spot - lines * term
    groups = [
        (inner_spot >= a * per) & (inner_spot < b * per) for a, b in ((0, 1), (1, 4), (4, 9))
    ]
    block_row = lax.broadcasted_iota(jnp.int32, (lines, 3 * width), 0)
    block_lane = lax.broadcasted_iota(jnp.int32, (lines, 3 * width), 1)
    blocks = [
        (block_row >= a * per) & (block_row < b * per) & (block_lane >= k * width)
        & (block_lane < (k + 1) * width)
        for k, (a, b) in enumerate(((0, 1), (1, 4), (4, 9)))
    ]
    blocks = blocks[0] | blocks[1] | blocks[2]
    order = (lax.broadcasted_iota(jnp.int32, (NBASIS, wide), 0) + 1).astype(jnp.float32)
    s3, s5, s15 = math.sqrt(3.0), math.sqrt(5.0), math.sqrt(15.0)
    norm = math.sqrt(2.0 / CUTOFF)

    def split(a):
        high = a.astype(jnp.bfloat16).astype(jnp.float32)
        return jnp.where(term == 2, a - high, high)

    post.wait_recv()
    letter = inbox[...]
    hot_j = hot(letter[0:1].astype(jnp.int32), halo_rows)
    twice_j = jnp.concatenate([hot_j, hot_j], axis=0)
    there = letter[1:2].astype(jnp.int32)
    kind_there = letter[2:3].astype(jnp.int32)
    arrivals.wait_recv()

    block = with_mine(halo[...], lambda step, at: source(step, 1)[...])
    total_rows = plan[-1][1] + plan[-1][2]
    if total_rows < halo_rows:
        every_id = lax.broadcasted_iota(jnp.int32, (halo_rows, LANES), 0)
        block = jnp.where(every_id < total_rows, block, 0.0)

    block = jnp.concatenate([v.T for v in halves(block)], axis=1)

    stacks = [raw(block, twice_j[:, at : at + wide], NN) for at in range(0, pairs, wide)]
    parcel.wait_recv()
    sheet = mail_in[...]

    def network(at):
        span = slice(at, at + wide)
        shift_j, kind_j = picked(stacks[at // wide], there[:, span], kind_there[:, span])
        yield
        rx, ry, rz = [sheet[c : c + 1, span] + SIDE * shift_j[c] for c in range(3)]
        live = letter[3:4, span]
        own_j = jnp.where(sheet[3:4, span] > 1.5, 1.0, 0.0)
        kind_i = sheet[3:4, span] - 2.0 * own_j
        kind_j = own_j + kind_j
        square = rx * rx + ry * ry + rz * rz
        inv = lax.rsqrt(square)
        dist = square * inv
        ux, uy, uz = rx * inv, ry * inv, rz * inv
        ratio = dist * (1.0 / CUTOFF)
        r2 = ratio * ratio
        r5 = r2 * r2 * ratio
        inside = ratio < 1.0
        bell = jnp.where(
            inside, 1.0 + r5 * ratio * (-28.0 + ratio * (48.0 - 21.0 * ratio)), 0.0
        )
        slope = jnp.where(
            inside, r5 * (1.0 - ratio) * (1.0 - ratio) * (-168.0 / CUTOFF), 0.0
        )
        turns = order * (dist * (0.5 / CUTOFF))
        sines, cosines = wave(turns), wave(turns + 0.25)
        basis = norm * sines * (inv * bell)
        basis_d = norm * (
            cosines * order * (inv * bell * (math.pi / CUTOFF))
            + sines * (inv * (slope - bell * inv))
        )
        kinds = [1.0 - kind_i, kind_i, 1.0 - kind_j, kind_j]
        inputs = jnp.concatenate(
            [basis] + kinds + [jnp.zeros((4, wide), jnp.float32)], axis=0
        )
        inputs_t = jnp.concatenate([basis_d, jnp.zeros((8, wide), jnp.float32)], axis=0)

        hidden = raw(two_3, stacked(inputs), NN)
        hidden_t = raw(two_3, stacked(inputs_t), NN)
        yield
        hidden, hidden_d = silu_pair(hidden)
        latent = raw(lat_3, stacked(hidden), NN)
        latent_t = raw(lat_3, stacked(hidden_t * hidden_d), NN)
        yield
        latent, latent_d = silu_pair(latent)
        latent_t = latent_t * latent_d
        lat_h, lat_l = halves(latent)
        scale = bell * live
        scale_t = slope * live
        harm = [
            jnp.ones_like(ux),
            s3 * ux,
            s3 * uy,
            s3 * uz,
            s15 * ux * uy,
            s15 * uy * uz,
            0.5 * s5 * (3.0 * uz * uz - 1.0),
            s15 * ux * uz,
            0.5 * s15 * (ux * ux - uy * uy),
        ]
        rows = jnp.concatenate([h * member for h in harm] + [unused], axis=0)
        rows_h, rows_l = halves(rows)
        rows_3 = jnp.concatenate([rows_h, rows_l, rows_h], axis=0)
        scaled_h, scaled_l = [
            jnp.concatenate([v] * 3, axis=0) for v in halves(rows * scale)
        ]
        gathered = by_parts(jnp.concatenate([lat_h, lat_l], axis=0), scaled_h, scaled_l, NT)
        yield
        environ = ENV * raw(env_3, stacked(gathered), NN)
        lat_s = jnp.concatenate([lat_h, lat_l, lat_h], axis=0)
        plain = raw(env_3, lat_s, NN)
        yield
        environ_s = split(environ)
        chosen = jnp.concatenate(
            [jnp.where(g, environ_s, 0.0) for g in groups], axis=0
        ).astype(jnp.bfloat16)
        mixed = raw(chosen, rows_3, NN)
        partly = raw(out_a, lat_s, NN)
        plain_t = raw(env_3, stacked(latent_t), NN)
        weight = plain * scale
        yield
        mixed = [mixed[width * k : width * (k + 1)] for k in range(3)]
        joined_h, joined_l = halves(jnp.concatenate([weight * a for a in mixed], axis=0))
        updated = by_parts(out_b, joined_h, joined_l) + partly
        yield
        weight_t = plain_t * scale + plain * scale_t
        near = jnp.concatenate([jnp.where(g, environ, 0.0)[:, 0:LANES] for g in groups], axis=0)
        near = doubled(near.T[0:lines])
        weight_s, slant_s = stacked(weight), stacked(weight_t)
        updated, updated_d = silu_pair(updated)
        d_out = (gain * scale) * updated_d
        back = raw(back_3, stacked(d_out), NN)
        score = jnp.sum(gain * updated, axis=0, keepdims=True)
        pair_energy = score * scale
        yield
        d_mixed = [back[width * (k + 1) : width * (k + 2)] for k in range(3)]
        pass_h, pass_l = halves(jnp.concatenate([q * weight for q in d_mixed], axis=0))
        d_env = by_parts(jnp.concatenate([rows_h, rows_l], axis=0), pass_h, pass_l, NT)
        d_rows = by_parts(near, pass_h, pass_l)
        yield
        along = d_mixed[0] * mixed[0] + d_mixed[1] * mixed[1] + d_mixed[2] * mixed[2]
        d_dist = (
            jnp.sum(along * weight_t + back[0:width] * latent_t, axis=0, keepdims=True)
            + score * scale_t
        )
        d_env = jnp.where(blocks, ENV * d_env, 0.0)
        d_env = jnp.concatenate([d_env, jnp.zeros((lines, width), jnp.float32)], axis=1)
        d_env = d_env[:, 0:LANES] + d_env[:, LANES:]
        d_env_h, d_env_l = halves(d_env + pltpu.roll(d_env, width, 1))
        d_env = jnp.concatenate([d_env_h, d_env_l[:, 0:width]], axis=1)
        d_rows = d_rows + raw(d_env, weight_s, NN)
        slanted = raw(d_env, slant_s, NN)
        yield
        turned = [d_rows[m * per : (m + 1) * per] for m in range(9)]
        dux = s3 * turned[1] + s15 * (uy * turned[4] + uz * turned[7] + ux * turned[8])
        duy = s3 * turned[2] + s15 * (ux * turned[4] + uz * turned[5] - uy * turned[8])
        duz = (
            s3 * turned[3]
            + s15 * (uy * turned[5] + ux * turned[7])
            + 3.0 * s5 * uz * turned[6]
        )
        dux, duy, duz = [
            jnp.sum(d * member, axis=0, keepdims=True) for d in (dux, duy, duz)
        ]
        d_dist = d_dist + jnp.sum(rows * slanted, axis=0, keepdims=True)
        radial = d_dist - (ux * dux + uy * duy + uz * duz) * inv
        yield [d * inv + u * radial for d, u in ((dux, ux), (duy, uy), (duz, uz))] + [
            pair_energy
        ]

    runs = [network(at) for at in range(0, pairs, wide)]
    found = [None] * len(runs)
    while found[0] is None:
        found = [next(run) for run in runs]
    *grad, pair_energy = [jnp.concatenate(v, axis=1) for v in zip(*found)]
    back_mail[...] = jnp.concatenate(grad + [pair_energy], axis=0)
    reply = remote(back_mail, back_inbox, send_b.at[1], recv_b.at[1], swapped)
    reply.start()
    partial = mm_exact_a(hot_j, placed(there, [-g for g in grad]))
    early = max(at + rows for (_, dy, _), at, rows in plan if dy)

    def give(entries):
        for step, at, rows in entries:
            span = pl.ds(at, rows)
            copy = remote(
                part.at[span], got.at[span], send_b.at[0], recv_b.at[0], holder(step)
            )
            unless_mine(step, copy.start)

    ranked = by_reach(plan)
    first_rows = -(-early // 8) * 8
    part[pl.ds(0, first_rows), :] = partial[0:first_rows]
    give([entry for entry in ranked if entry[0][1]])
    part[pl.ds(first_rows, halo_rows - first_rows), :] = partial[first_rows:]
    give([entry for entry in ranked if not entry[0][1]])

    reply.wait_recv()
    answer = back_inbox[...]
    moves = [answer[c : c + 1] for c in range(3)]
    settled = mm_exact_a(
        hot_own,
        jnp.concatenate(
            [placed(place[:, 0:pairs], [-m for m in moves]), placed(place[:, pairs:], moves)],
            axis=1,
        ),
    )
    energies = mm_exact_b(jnp.broadcast_to(answer[3:4], (8, pairs)), mine16, NT)
    result[pl.ds(own, 8), 0:centre_total] = energies
    below = lax.broadcasted_iota(jnp.int32, (CELLS, LANES), 0)
    upper_lanes = high((CELLS, LANES))
    returns = every(got, send_b.at[0], recv_b.at[0])
    returns.wait_recv()

    slabs = [settled[CELLS * x : CELLS * (x + 1)] for x in range(CELLS)]
    columns = {y: [[] for x in range(CELLS)] for y in (0, 1, CELLS - 2, CELLS - 1)}

    def low_part(value):
        return jnp.where(upper_lanes[0 : value.shape[0]], 0.0, value)

    def high_part(value):
        kept = jnp.where(upper_lanes[0 : value.shape[0]], value, 0.0)
        return pltpu.roll(kept, LANES - KEPT, 1)

    for (dx, dy, dz), at, rows in plan:
        x, y = (CELLS - 1) * (dx < 0), (CELLS - 1) * (dy < 0)
        if own_corner((dx, dy, dz)):
            value = jnp.where(
                mine_too((dx, dy, dz)), part[pl.ds(at, 1), :], got[pl.ds(at, 1), :]
            )
            columns[y][x].append(value)
        elif dx and dy:
            value = got[pl.ds(at, 1), :]
            columns[y][x].append(high_part(value) if dx < 0 else low_part(value))
        elif dz and dy:
            value = got[pl.ds(at, rows), :]
            for part_of, base in ((low_part(value), 0), (high_part(value), rows)):
                for r in range(rows):
                    columns[y][base + r].append(part_of[r : r + 1])
        elif dz and dx:
            value = got[pl.ds(at, rows), :]
            slabs[x] = slabs[x] + (high_part(value) if dx < 0 else low_part(value))
        elif dz:
            for r in range(CELLS // 2):
                value = got[pl.ds(at + CELLS * r, CELLS), :]
                slabs[r] = slabs[r] + low_part(value)
                slabs[CELLS // 2 + r] = slabs[CELLS // 2 + r] + high_part(value)
        elif dy:
            for t in range(2):
                for r in range(CELLS):
                    columns[origin(dy, 2) + t][r].append(got[pl.ds(at + 8 * t + r, 1), :])
        else:
            for t in range(2):
                x = origin(dx, 2) + t
                slabs[x] = slabs[x] + got[pl.ds(at + CELLS * t, CELLS), :]
    for x in range(CELLS):
        side = jnp.zeros((CELLS, LANES), jnp.float32)
        for y, lists in columns.items():
            value = sum(lists[x][1:], lists[x][0])
            side = jnp.where(below == y, value, side)
        total[pl.ds(CELLS * x, CELLS), :] = slabs[x] + side
    for copy in (post, parcel, arrivals, reply, returns):
        copy.wait_send()


def unpack_body(result, energy, forces):
    energy[0] = result[pl.ds(CELLS * CELLS, 1), 0 : energy.shape[2]]
    final = jnp.concatenate(
        [result[pl.ds(j, 4, stride=16), :][:, 0:ZROWS] for j in range(16)], axis=1
    )
    wide = 16 * ZROWS
    for q in range(4):
        forces[0, :, wide * q : wide * (q + 1)] = final[q : q + 1, :]


def solution(mesh):
    sizes = tuple(mesh.shape[a] for a in AXES)
    plan, line_total = slot_plan(sizes[2])

    def local(displacement, species, centres, neighbours, neighbour_count, live_centres,
              w_two, w_lat, w_env, w_out, readout):
        pairs = neighbours.shape[2]
        vmem = pl.BlockSpec(memory_space=pltpu.VMEM)
        rows = -(-line_total // 8) * 8
        args = [
            displacement, species, centres, neighbours, neighbour_count, live_centres,
            w_two, w_lat, w_env, w_out.T, readout.reshape(1, -1),
        ]

        def body(*refs):
            pl.run_scoped(
                lambda *local_sems: kernel_body(sizes, plan, *refs, *local_sems),
                pltpu.SemaphoreType.DMA((len(args),)),
                pltpu.SemaphoreType.DMA((3,)),
                pltpu.SemaphoreType.DMA((2,)),
            )

        sizes_vmem = [
            (CELLS * CELLS, LANES), (4 * CELLS, LANES), (HALF, LANES), (CELLS, LANES),
            (4, pairs), (4, pairs), (4, pairs), (4, pairs), (4, pairs), (4, pairs),
            (rows, LANES), (rows, LANES), (rows, LANES),
        ]
        result = pl.pallas_call(
            body,
            out_shape=pltpu.VMEM((CELLS * CELLS + 8, LANES), jnp.float32),
            in_specs=[pl.BlockSpec(memory_space=pltpu.HBM)] * len(args),
            out_specs=vmem,
            scratch_shapes=[pltpu.VMEM(x.shape, x.dtype) for x in args]
            + [pltpu.VMEM(shape, jnp.float32) for shape in sizes_vmem]
            + [pltpu.SemaphoreType.DMA((3,)), pltpu.SemaphoreType.DMA((2,))],
            compiler_params=pltpu.CompilerParams(collective_id=0, has_side_effects=True),
        )(*args)
        result = pltpu.with_memory_space_constraint(result, pltpu.VMEM)
        return pl.pallas_call(
            unpack_body,
            out_shape=(
                jax.ShapeDtypeStruct(centres.shape, jnp.float32),
                jax.ShapeDtypeStruct(displacement.shape, jnp.float32),
            ),
            in_specs=[vmem],
            out_specs=(vmem, vmem),
        )(result)

    split = P(*AXES)
    return jax.shard_map(
        local,
        mesh=mesh,
        in_specs=(split,) * 6 + (P(),) * 5,
        out_specs=(split, split),
        check_vma=False,
    )
```
